1024 devices in a mesh: node: 32 (over y, x), local: 32 (over z, core).
Axes of the slice: x: 4, y: 8, z: 16, core: 2. Of those that a mesh axis runs over, the one named last changes fastest.
Arguments:
- tokens: bfloat16 [1024, 7168], P(('node', 'local')), may hold values from -6 to 6
- w_gate: bfloat16 [64, 1024, 7168], P('node', 'local'), may hold values from -0.0625 to 0.0625
- w_up: bfloat16 [64, 1024, 7168], P('node', 'local'), may hold values from -0.0625 to 0.0625
- w_down: bfloat16 [64, 1024, 7168], P('node', 'local'), may hold values from -0.1875 to 0.1875
- expert_ids: int32 [1024, 8], P(('node', 'local')), may hold values from 0 to 63, all different within a row
- gate_ints: int32 [1024, 8], P(('node', 'local')), may hold values from 1 to 8
Outputs:
- mixed: bfloat16 [1024, 7168], P(('node', 'local'))
The draws below stay inside these ranges and needn't reach their ends.
Inputs may be any that keep to these rules, and one draw needn't show every extreme that they name: `expert_ids`: each row names 8 different experts.
All inputs are finite; a program needn't handle non-finite values.
Results may differ from the reference program's by a relative error of at most 0.025.
Values may be sent and summed in bfloat16 or wider, within the bound.
A program may use at most 32 MiB of HBM per device.

```python
import jax
import jax.numpy as jnp
from jax import lax

D = 7168
FF = 1024
TOP = 8
EXP_NODE = 2
CAP = 8
TOK_DEV = 1
EXPERTS = 64
TOKENS = 1024
FFL = 32
N_NODE = 32
N_LOCAL = 32


def touch_ends(values, own_key, smallest, high):
    place = [jax.random.randint(jax.random.fold_in(own_key, axis), (), 0, length) for axis, length in enumerate(values.shape)]
    widest = values.shape.index(max(values.shape))
    neighbour = place[:widest] + [(place[widest] + 1) % values.shape[widest]] + place[widest + 1:]
    return values.at[tuple(place)].set(smallest).at[tuple(neighbour)].set(high)


def block_levels(rng, extent, pieces, least, top_value):
    loudness = 1.0
    for axis_at, parts in pieces:
        steps = jax.random.uniform(jax.random.fold_in(jax.random.fold_in(rng, 6), axis_at), (parts,), jnp.float32, least / len(pieces), top_value / len(pieces))
        loudness = loudness * jnp.repeat(jnp.exp(steps), extent[axis_at] // parts).reshape((-1,) + (1,) * (len(extent) - 1 - axis_at))
    return loudness


def distinct(stream_key, rows, count, top, lift):
    ranking = jax.random.permutation(jax.random.fold_in(stream_key, 1), count)
    boost = ranking
    for power in range(3):
        boost = boost * boost // count
    boost = boost * lift // count
    lots = jax.random.randint(jax.random.fold_in(stream_key, 2), (rows, count), 0, 4096) + boost
    fixed_rows = jax.random.permutation(jax.random.fold_in(stream_key, 3), rows)[jnp.arange(count) % rows]
    lots = jnp.where(jnp.arange(rows)[:, None] == fixed_rows[None, :], 1 << 14, lots)
    score = lots * count + jnp.arange(count)
    return lax.top_k(score.astype(jnp.int32), top)[1].astype(jnp.int32)


def normal_values(stream_key, shape, width, limit, shards=(), held_as=jnp.bfloat16):
    loudness = block_levels(stream_key, shape, shards, -0.22, 0.18) if shards else 1.0
    entries = jax.random.normal(stream_key, shape, jnp.float32) * width * loudness
    return jnp.minimum(jnp.maximum(entries, -limit), limit).astype(held_as)


def setup_inputs(seed: int = 0) -> dict:
    splits = jax.random.split(jax.random.key(seed), 7)
    tokens = normal_values(splits[0], (TOKENS, D), 1.0, 6.0, ((0, 1024),))
    w_gate = normal_values(splits[1], (EXPERTS, FF, D), D ** -0.5, 0.0625, ((0, 32), (1, 32)))
    w_up = normal_values(splits[2], (EXPERTS, FF, D), D ** -0.5, 0.0625, ((0, 32), (1, 32)))
    w_down = normal_values(splits[3], (EXPERTS, FF, D), FF ** -0.5, 0.1875, ((0, 32), (1, 32)))
    expert_ids = distinct(splits[4], TOKENS, EXPERTS, TOP, 2048)
    gate_ints = touch_ends(jax.random.randint(splits[5], (TOKENS, TOP), 1, 9), jax.random.fold_in(splits[5], 1), 1, 8).astype(jnp.int32)
    return dict(tokens=tokens, w_gate=w_gate, w_up=w_up, w_down=w_down, expert_ids=expert_ids, gate_ints=gate_ints)


def reference(tokens, w_gate, w_up, w_down, expert_ids, gate_ints):
    slot_count = N_NODE * TOK_DEV
    by_column = tokens.reshape(N_NODE, N_LOCAL, TOK_DEV, D).transpose(1, 0, 2, 3).reshape(N_LOCAL, slot_count, D)
    ids_column = expert_ids.reshape(N_NODE, N_LOCAL, TOK_DEV, TOP).transpose(1, 0, 2, 3).reshape(N_LOCAL, slot_count, TOP)
    gates_column = gate_ints.reshape(N_NODE, N_LOCAL, TOK_DEV, TOP).transpose(1, 0, 2, 3).reshape(N_LOCAL, slot_count, TOP)
    slot_iota = jnp.arange(CAP, dtype=jnp.int32)
    row_count = N_LOCAL * CAP
    rows_f32 = by_column.astype(jnp.float32)

    def per_node(total, group):
        wanted = group * EXP_NODE + jnp.arange(EXP_NODE, dtype=jnp.int32)
        matched = ids_column[..., None] == wanted
        gate_sums = jnp.sum(jnp.where(matched, gates_column[..., None], 0), axis=2).astype(jnp.int32)
        is_hit = (jnp.sum(gate_sums, axis=-1) > 0).astype(jnp.int32)
        slot_rank = jnp.cumsum(is_hit, axis=1).astype(jnp.int32) - is_hit
        keep_flag = (is_hit > 0) & (slot_rank < CAP)
        picker = (keep_flag[:, None, :] & (slot_rank[:, None, :] == slot_iota[None, :, None])).astype(jnp.float32)
        packed = jnp.einsum('lcs,lsd->lcd', picker, rows_f32).astype(jnp.bfloat16).reshape(row_count, D)
        packed_gates = jnp.einsum('lcs,lse->lce', picker, gate_sums.astype(jnp.float32)).reshape(row_count, EXP_NODE) / 8.0
        first = (group * EXP_NODE).astype(jnp.int32)
        gate_w = lax.dynamic_slice_in_dim(w_gate, first, EXP_NODE, 0).astype(jnp.float32)
        up_w = lax.dynamic_slice_in_dim(w_up, first, EXP_NODE, 0).astype(jnp.float32)
        down_w = lax.dynamic_slice_in_dim(w_down, first, EXP_NODE, 0)
        packed_f32 = packed.astype(jnp.float32)
        gate_act = jnp.einsum('rd,efd->ref', packed_f32, gate_w)
        up_act = jnp.einsum('rd,efd->ref', packed_f32, up_w)
        hidden = (jax.nn.silu(gate_act) * up_act * packed_gates[:, :, None]).astype(jnp.bfloat16)
        hidden_blocks = hidden.reshape(row_count, EXP_NODE, N_LOCAL, FFL).transpose(2, 0, 1, 3).reshape(N_LOCAL, row_count, EXP_NODE * FFL)
        down_blocks = down_w.reshape(EXP_NODE, N_LOCAL, FFL, D).transpose(1, 0, 2, 3).reshape(N_LOCAL, EXP_NODE * FFL, D)

        def add_block(acc, block_pair):
            part = jnp.dot(block_pair[0], block_pair[1], preferred_element_type=jnp.float32)
            rounded = lax.optimization_barrier(part.astype(jnp.bfloat16))
            return acc + rounded.astype(jnp.float32), None

        summed, _ = lax.scan(add_block, jnp.zeros((row_count, D), jnp.float32), (hidden_blocks, down_blocks))
        group_out = summed.astype(jnp.bfloat16).reshape(N_LOCAL, CAP, D).astype(jnp.float32)
        placed = jnp.einsum('lcs,lcd->lsd', picker, group_out)
        return total + placed, None

    start = jnp.zeros((N_LOCAL, slot_count, D), jnp.float32)
    total, _ = lax.scan(per_node, start, jnp.arange(N_NODE, dtype=jnp.int32))
    mixed = total.astype(jnp.bfloat16).reshape(N_LOCAL, N_NODE, TOK_DEV, D).transpose(1, 0, 2, 3).reshape(N_NODE * N_LOCAL * TOK_DEV, D)
    return mixed
```

```python
import functools

import jax
import jax.numpy as jnp
from jax import lax
from jax.experimental import pallas as pl
from jax.experimental.pallas import tpu as pltpu
from jax.sharding import PartitionSpec as P

CAP = 8
NX = 4
CHUNKS = 4
META = 128
BF16 = jnp.bfloat16
F32 = jnp.float32
MESH_ID = pl.DeviceIdType.MESH


def layer_kernel(
    nx, ny, nz,
    tok_ref, wg_ref, wu_ref, wd_ref, ids_ref, gates_ref,
    out_ref,
    t1, t2, xbuf, wgu, wdn, zbuf, hbuf, pbuf, rsend, rrecv, ysend, yrecv, fsend, frecv,
    wl_sem, ws_sem, wr_sem, s1, r1, s2, r2, sa, ra, ss, rs, s3, r3, s4, r4,
):
    half = wgu.shape[-1]
    width = half // CHUNKS
    offs = [0] + [META + q * width for q in range(1, CHUNKS)]
    lens = [META + width] + [width] * (CHUNKS - 1)
    d_off = [META + q * width for q in range(CHUNKS)]
    hz = nz // 2
    n = lax.axis_index("node")
    l = lax.axis_index("local")
    x, y = lax.rem(n, nx), n // nx
    z, c = l // 2, lax.rem(l, 2)

    def at_x(v):
        return (y * nx + v, l)

    def at_y(v):
        return (v * nx + x, l)

    def at_z(v):
        return (n, v * 2 + c)

    up, down = lax.rem(z + 1, nz), lax.rem(z + nz - 1, nz)
    partner = (n, z * 2 + 1 - c)
    xs = [lax.rem(x + d, nx) for d in range(1, nx)]
    ys = [lax.rem(y + d, ny) for d in range(1, ny)]

    def push(src, dst, send, recv, device):
        pltpu.make_async_remote_copy(
            src_ref=src, dst_ref=dst, send_sem=send, recv_sem=recv,
            device_id=device, device_id_type=MESH_ID,
        ).start()

    def await_bytes(ref, sem):
        pltpu.make_async_copy(ref, ref, sem).wait()

    local = []
    for h in range(2):
        cols = pl.ds(h * half, half)
        local.append(pltpu.make_async_copy(wg_ref.at[:, :, cols], wgu.at[h, 0, 0], wl_sem.at[0, h]))
        local.append(pltpu.make_async_copy(wu_ref.at[:, :, cols], wgu.at[h, 1, 0], wl_sem.at[1, h]))
        local.append(pltpu.make_async_copy(wd_ref.at[:, :, cols], wdn.at[h, 0], wl_sem.at[2, h]))
    for copy in local:
        copy.start()

    barrier = pltpu.get_barrier_semaphore()
    greeted = [partner, at_z(up), at_z(down)] + [at_x(v) for v in xs] + [at_y(v) for v in ys]
    for device in greeted:
        pl.semaphore_signal(barrier, 1, device_id=device, device_id_type=MESH_ID)

    lane = lax.broadcasted_iota(jnp.int32, (2, META), 1)
    row = lax.broadcasted_iota(jnp.int32, (2, META), 0)
    gates = jnp.zeros((2, META), jnp.int32)
    for k in range(ids_ref.shape[1]):
        gates += jnp.where((lane == ids_ref[0, k]) & (row == 0), gates_ref[0, k], 0)
    t1[y, :, 0:META] = gates.astype(F32).astype(BF16)
    tok = tok_ref[...].astype(F32)
    pair = jnp.concatenate([tok[:, :half], tok[:, half:]], axis=0)
    t1[y, :, META:] = pair.astype(BF16)

    pl.semaphore_wait(barrier, len(greeted))

    def part(q):
        return pl.ds(offs[q], lens[q])

    for q in range(CHUNKS):
        for v in ys:
            own = t1.at[y, :, part(q)]
            push(own, own, s1.at[q], r1.at[q], at_y(v))
    for h in range(2):
        cols = pl.ds(h * half, half)
        push(wg_ref.at[:, :, cols], wgu.at[h, 0, 1], ws_sem.at[0, h], wr_sem.at[0, h], partner)
        push(wu_ref.at[:, :, cols], wgu.at[h, 1, 1], ws_sem.at[1, h], wr_sem.at[1, h], partner)
        push(wd_ref.at[:, :, cols], wdn.at[h, 1], ws_sem.at[2, h], wr_sem.at[2, h], partner)

    for q in range(CHUNKS):
        await_bytes(t1.at[pl.ds(0, ny - 1), :, part(q)], r1.at[q])
        for v in range(ny):
            t2[x, 2 * v : 2 * v + 2, part(q)] = t1[v, :, part(q)]
        for v in xs:
            own = t2.at[x, :, part(q)]
            push(own, own, s2.at[q], r2.at[q], at_x(v))

    cells = nx * ny * 2
    rows = CAP * 2

    def order(i):
        return ((i // 2) % ny) * nx + i // (2 * ny)

    i0 = lax.broadcasted_iota(jnp.int32, (cells, cells), 0)
    i1 = lax.broadcasted_iota(jnp.int32, (cells, cells), 1)
    same = (i0 // 2 == i1 // 2).astype(F32).astype(BF16)
    before = (order(i0) < order(i1)).astype(F32).astype(BF16)
    after = (order(i1) < order(i0)).astype(F32).astype(BF16)
    mine = lax.broadcasted_iota(jnp.int32, (rows, META), 1)
    mine = ((mine // 2) == n).astype(F32).astype(BF16)

    picker = None
    picker_t = None
    for q in range(CHUNKS):
        await_bytes(t2.at[pl.ds(0, nx - 1), :, part(q)], r2.at[q])
        if q == 0:
            meta = t2[:, :, 0:META].reshape(cells, META)
            nt = (((1,), (1,)), ((), ()))
            total = lax.dot_general(mine, meta, nt, preferred_element_type=F32)
            hit = (total > 0).astype(F32).astype(BF16)
            rank = jnp.dot(hit, before, preferred_element_type=F32)
            hit = jnp.dot(hit, same, preferred_element_type=F32)
            r = lax.broadcasted_iota(jnp.int32, (rows, cells), 0)
            i = lax.broadcasted_iota(jnp.int32, (rows, cells), 1)
            picks = (hit > 0) & (rank == (r // 2).astype(F32)) & (r % 2 == i % 2)
            picker = picks.astype(F32).astype(BF16)
            total = lax.dot_general(meta, mine, nt, preferred_element_type=F32)
            hit = (total > 0).astype(F32).astype(BF16)
            rank = jnp.dot(after, hit, preferred_element_type=F32)
            hit = jnp.dot(same, hit, preferred_element_type=F32)
            r = lax.broadcasted_iota(jnp.int32, (cells, rows), 1)
            i = lax.broadcasted_iota(jnp.int32, (cells, rows), 0)
            picks = (hit > 0) & (rank == (r // 2).astype(F32)) & (r % 2 == i % 2)
            picker_t = picks.astype(F32).astype(BF16)
        field = t2[:, :, part(q)].reshape(cells, lens[q])
        xbuf[z, :, part(q)] = jnp.dot(picker, field, preferred_element_type=F32).astype(BF16)
        own = xbuf.at[z, :, part(q)]
        push(own, own, sa.at[q], ra.at[0, 1, q], at_z(up))
        push(own, own, sa.at[q], ra.at[1, 1, q], at_z(down))

    def hop(s, carry):
        below = lax.rem(z + nz - s, nz)
        above = lax.rem(z + s, nz)
        for q in range(CHUNKS):
            block = xbuf.at[below, :, part(q)]
            await_bytes(block, ra.at[0, s, q])
            push(block, block, sa.at[q], ra.at[0, s + 1, q], at_z(up))
            block = xbuf.at[above, :, part(q)]
            await_bytes(block, ra.at[1, s, q])
            @pl.when(s < hz - 1)
            def _():
                push(block, block, sa.at[q], ra.at[1, s + 1, q], at_z(down))
        return carry

    lax.fori_loop(1, hz, hop, 0)
    for q in range(CHUNKS):
        await_bytes(xbuf.at[lax.rem(z + hz, nz), :, part(q)], ra.at[0, hz, q])

    for copy in local:
        copy.wait()
    for h in range(2):
        await_bytes(wgu.at[h, 0, 1], wr_sem.at[0, h])
        await_bytes(wgu.at[h, 1, 1], wr_sem.at[1, h])
        await_bytes(wdn.at[h, 1], wr_sem.at[2, h])
    pair_rows = nz * rows
    tokens = pair_rows // 2
    units = wdn.shape[1] * wdn.shape[2] * wdn.shape[3]
    for q in range(CHUNKS):
        piece = xbuf[:, :, pl.ds(d_off[q], width)].reshape(pair_rows, width)
        for h in range(2):
            w = wgu[h, :, :, :, :, pl.ds(q * width, width)].reshape(2 * units, width)
            nt = (((1,), (1,)), ((), ()))
            v = lax.dot_general(piece, w, nt, preferred_element_type=F32)
            for k in range(2):
                if q == 0:
                    zbuf[h, k] = v[:, k * units : (k + 1) * units]
                else:
                    zbuf[h, k] += v[:, k * units : (k + 1) * units]
    lane = lax.broadcasted_iota(jnp.int32, (META, units), 0)
    unit = lax.broadcasted_iota(jnp.int32, (META, units), 1)
    ffl = wdn.shape[3]
    chosen = (lane == 2 * n + (unit // ffl) % 2).astype(F32).astype(BF16)
    gate_rows = xbuf[:, :, 0:META].reshape(pair_rows, META)
    hbuf[0] = jnp.dot(gate_rows, chosen, preferred_element_type=F32)
    even, odd = pl.ds(0, tokens, 2), pl.ds(1, tokens, 2)
    gate_act = zbuf[0, 0, even, :] + zbuf[1, 0, odd, :]
    up_act = zbuf[0, 1, even, :] + zbuf[1, 1, odd, :]
    scale = hbuf[0, even, :] / 8.0
    hidden = gate_act / (1.0 + jnp.exp(-gate_act)) * up_act * scale
    none = jnp.zeros_like(hidden)
    hbuf[0, even, :] = hidden
    hbuf[1, even, :] = none
    hbuf[0, odd, :] = none
    hbuf[1, odd, :] = hidden
    hidden = jnp.concatenate([hbuf[0], hbuf[1]], axis=1).astype(BF16)
    for q in range(CHUNKS):
        w = wdn[:, :, :, :, pl.ds(q * width, width)].reshape(2 * units, width)
        v = jnp.dot(hidden, w, preferred_element_type=F32)
        pbuf[:, :, pl.ds(q * width, width)] = v.reshape(nz, rows, width)

    def slot(direction, step):
        return direction * hz + step - 1

    def cols(q):
        return pl.ds(q * width, width)

    for q in range(CHUNKS):
        far = lax.rem(z + hz, nz)
        rsend[slot(0, 1), :, cols(q)] = pbuf[far, :, cols(q)].astype(BF16)
        push(rsend.at[slot(0, 1), :, cols(q)], rrecv.at[slot(0, 1), :, cols(q)], ss.at[q], rs.at[0, 1, q], at_z(up))
        far = lax.rem(z + hz + 1, nz)
        rsend[slot(1, 1), :, cols(q)] = pbuf[far, :, cols(q)].astype(BF16)
        push(rsend.at[slot(1, 1), :, cols(q)], rrecv.at[slot(1, 1), :, cols(q)], ss.at[q], rs.at[1, 1, q], at_z(down))

    def back(s, carry):
        above = lax.rem(z + hz + 1 - s, nz)
        below = lax.rem(z + hz + s, nz)
        for q in range(CHUNKS):
            got = rrecv.at[slot(0, s - 1), :, cols(q)]
            await_bytes(got, rs.at[0, s - 1, q])
            rsend[slot(0, s), :, cols(q)] = (got[...].astype(F32) + pbuf[above, :, cols(q)]).astype(BF16)
            push(rsend.at[slot(0, s), :, cols(q)], rrecv.at[slot(0, s), :, cols(q)], ss.at[q], rs.at[0, s, q], at_z(up))
            @pl.when(s < hz)
            def _():
                got = rrecv.at[slot(1, s - 1), :, cols(q)]
                await_bytes(got, rs.at[1, s - 1, q])
                rsend[slot(1, s), :, cols(q)] = (got[...].astype(F32) + pbuf[below, :, cols(q)]).astype(BF16)
                push(rsend.at[slot(1, s), :, cols(q)], rrecv.at[slot(1, s), :, cols(q)], ss.at[q], rs.at[1, s, q], at_z(down))
        return carry

    lax.fori_loop(2, hz + 1, back, 0)

    for q in range(CHUNKS):
        await_bytes(rrecv.at[slot(1, hz - 1), :, cols(q)], rs.at[1, hz - 1, q])
        await_bytes(rrecv.at[slot(0, hz), :, cols(q)], rs.at[0, hz, q])
        total = pbuf[z, :, cols(q)] + rrecv[slot(0, hz), :, cols(q)].astype(F32) + rrecv[slot(1, hz - 1), :, cols(q)].astype(F32)
        placed = jnp.dot(picker_t, total.astype(BF16), preferred_element_type=F32)
        ysend[:, :, cols(q)] = placed.astype(BF16).reshape(nx, 2 * ny, width)
        for v in xs:
            push(ysend.at[v, :, cols(q)], yrecv.at[x, :, cols(q)], s3.at[q], r3.at[q], at_x(v))
    for q in range(CHUNKS):
        await_bytes(yrecv.at[pl.ds(0, nx - 1), :, cols(q)], r3.at[q])
        total = ysend[x, :, cols(q)].astype(F32)
        for v in xs:
            total += yrecv[v, :, cols(q)].astype(F32)
        total = total.astype(BF16)
        for v in range(ny):
            fsend[v, :, cols(q)] = total[2 * v : 2 * v + 2, :]
        for v in ys:
            push(fsend.at[v, :, cols(q)], frecv.at[y, :, cols(q)], s4.at[q], r4.at[q], at_y(v))
    for q in range(CHUNKS):
        await_bytes(frecv.at[pl.ds(0, ny - 1), :, cols(q)], r4.at[q])
        total = fsend[y, :, cols(q)].astype(F32)
        for v in ys:
            total += frecv[v, :, cols(q)].astype(F32)
        total = total.astype(BF16)
        out_ref[0:1, pl.ds(q * width, width)] = total[0:1, :]
        out_ref[0:1, pl.ds(half + q * width, width)] = total[1:2, :]

    for q in range(CHUNKS):
        await_bytes(t1.at[pl.ds(0, ny - 1), :, part(q)], s1.at[q])
        await_bytes(t2.at[pl.ds(0, nx - 1), :, part(q)], s2.at[q])
        await_bytes(xbuf.at[pl.ds(0, nz - 1), :, part(q)], sa.at[q])
        await_bytes(rrecv.at[pl.ds(0, nz - 1), :, cols(q)], ss.at[q])
        await_bytes(yrecv.at[pl.ds(0, nx - 1), :, cols(q)], s3.at[q])
        await_bytes(frecv.at[pl.ds(0, ny - 1), :, cols(q)], s4.at[q])
    for h in range(2):
        await_bytes(wgu.at[h, 0, 1], ws_sem.at[0, h])
        await_bytes(wgu.at[h, 1, 1], ws_sem.at[1, h])
        await_bytes(wdn.at[h, 1], ws_sem.at[2, h])


def solution(mesh):
    nodes, locals_ = mesh.shape["node"], mesh.shape["local"]
    nx = min(NX, nodes)
    ny, nz = nodes // nx, locals_ // 2
    hz = nz // 2

    def on_device(tokens, w_gate, w_up, w_down, expert_ids, gate_ints):
        model_width = tokens.shape[1]
        half = model_width // 2
        exp_node, ffl = w_gate.shape[0], w_gate.shape[1]
        units = 2 * exp_node * ffl
        rows = 2 * CAP
        sem = pltpu.SemaphoreType.DMA
        any_space = pl.BlockSpec(memory_space=pl.ANY)
        vmem = pl.BlockSpec(memory_space=pltpu.VMEM)
        smem = pl.BlockSpec(memory_space=pltpu.SMEM)
        return pl.pallas_call(
            functools.partial(layer_kernel, nx, ny, nz),
            out_shape=jax.ShapeDtypeStruct((1, model_width), BF16),
            in_specs=[vmem, any_space, any_space, any_space, smem, smem],
            out_specs=vmem,
            scratch_shapes=[
                pltpu.VMEM((ny, 2, META + half), BF16),
                pltpu.VMEM((nx, 2 * ny, META + half), BF16),
                pltpu.VMEM((nz, rows, META + half), BF16),
                pltpu.VMEM((2, 2, 2, exp_node, ffl, half), BF16),
                pltpu.VMEM((2, 2, exp_node, ffl, half), BF16),
                pltpu.VMEM((2, 2, nz * rows, units), F32),
                pltpu.VMEM((2, nz * rows, units), F32),
                pltpu.VMEM((nz, rows, half), F32),
                pltpu.VMEM((nz, rows, half), BF16),
                pltpu.VMEM((nz, rows, half), BF16),
                pltpu.VMEM((nx, 2 * ny, half), BF16),
                pltpu.VMEM((nx, 2 * ny, half), BF16),
                pltpu.VMEM((ny, 2, half), BF16),
                pltpu.VMEM((ny, 2, half), BF16),
                sem((3, 2)), sem((3, 2)), sem((3, 2)),
                sem((CHUNKS,)), sem((CHUNKS,)), sem((CHUNKS,)), sem((CHUNKS,)),
                sem((CHUNKS,)), sem((2, hz + 1, CHUNKS)),
                sem((CHUNKS,)), sem((2, hz + 1, CHUNKS)),
                sem((CHUNKS,)), sem((CHUNKS,)), sem((CHUNKS,)), sem((CHUNKS,)),
            ],
            compiler_params=pltpu.CompilerParams(
                collective_id=0, has_side_effects=True, vmem_limit_bytes=60 * 1024 * 1024
            ),
            name="layer",
        )(tokens, w_gate, w_up, w_down, expert_ids, gate_ints)

    both = P(("node", "local"), None)
    weights = P("node", "local", None)
    return jax.shard_map(
        on_device, mesh=mesh,
        in_specs=(both, weights, weights, weights, both, both),
        out_specs=both, check_vma=False,
    )
```

```python
import functools

import jax
import jax.numpy as jnp
from jax import lax
from jax.experimental import pallas as pl
from jax.experimental.pallas import tpu as pltpu
from jax.sharding import PartitionSpec as P

CAP = 8
NX = 4
CHUNKS = 7
META = 128
BF16 = jnp.bfloat16
F32 = jnp.float32
MESH_ID = pl.DeviceIdType.MESH
NT = (((1,), (1,)), ((), ()))
scope = jax.named_scope


def ones(mask):
    return mask.astype(F32).astype(BF16)


def layer_kernel(
    nx, ny, nz,
    tok_ref, wg_ref, wu_ref, wd_ref, ids_ref, gates_ref,
    out_ref,
    tokv, idsv, gatesv, tsend, t1, t2, xbuf, wgu, wdn, zbuf, hbuf, pfar, pnear, rsend, rrecv,
    ysend, yrecv, fsend, frecv,
    in_sem, wl_sem, ws_sem, wr_sem, s0, s1, r1, s2, r2, sa, ra, sx, rx, sp, rp, ss, rs, s3, r3, s4, r4,
):
    half = wgu.shape[-1]
    width = half // CHUNKS
    offs = [0] + [META + q * width for q in range(1, CHUNKS)]
    lens = [META + width] + [width] * (CHUNKS - 1)
    d_off = [META + q * width for q in range(CHUNKS)]
    hz = nz // 2
    rows = CAP * 2
    ffl = wdn.shape[3]
    units = wdn.shape[1] * wdn.shape[2] * ffl
    n = lax.axis_index("node")
    l = lax.axis_index("local")
    x, y = lax.rem(n, nx), n // nx
    z, c = l // 2, lax.rem(l, 2)
    lead = c == 1

    def at_x(v):
        return (y * nx + v, z * 2 + 1)

    def at_y(v, core):
        return (v * nx + x, z * 2 + core)

    up = (n, lax.rem(z + 1, nz) * 2 + 1)
    down = (n, lax.rem(z + nz - 1, nz) * 2 + 1)
    partner = (n, z * 2 + 1 - c)
    xs = [lax.rem(x + d, nx) for d in range(1, nx)]
    ys = [lax.rem(y + d, ny) for d in range(1, ny)]

    near = 1 + 2 * (hz - 2)
    far = 3

    def going_up(s):
        return s if s <= hz - 2 else near + s - (hz - 1)

    def going_down(s):
        return hz - 2 + s if s <= hz - 2 else near + 2

    def push(src, dst, send, recv, device):
        pltpu.make_async_remote_copy(
            src_ref=src, dst_ref=dst, send_sem=send, recv_sem=recv,
            device_id=device, device_id_type=MESH_ID,
        ).start()

    def await_bytes(ref, sem):
        pltpu.make_async_copy(ref, ref, sem).wait()

    def signal(sem, device):
        pl.semaphore_signal(sem, 1, device_id=device, device_id_type=MESH_ID)

    def part(q):
        return pl.ds(offs[q], lens[q])

    def cols(q):
        return pl.ds(q * width, width)

    barrier = pltpu.get_barrier_semaphore()
    with scope("entry"):
        signal(barrier, partner)
        for v in ys:
            signal(barrier, at_y(v, 1))

        @pl.when(lead)
        def _():
            for v in ys:
                signal(barrier, at_y(v, 0))
            for v in xs:
                signal(barrier, at_x(v))
            signal(barrier, up)
            signal(barrier, down)

        inputs = [
            pltpu.make_async_copy(tok_ref, tokv, in_sem.at[0]),
            pltpu.make_async_copy(ids_ref, idsv, in_sem.at[1]),
            pltpu.make_async_copy(gates_ref, gatesv, in_sem.at[2]),
        ]
        for copy in inputs:
            copy.start()
        for h in range(2):
            wcols = pl.ds(h * half, half)
            pltpu.make_async_copy(wg_ref.at[:, :, wcols], wgu.at[h, 0, 0], wl_sem.at[0]).start()
            pltpu.make_async_copy(wu_ref.at[:, :, wcols], wgu.at[h, 1, 0], wl_sem.at[0]).start()
            pltpu.make_async_copy(wd_ref.at[:, :, wcols], wdn.at[h, 0], wl_sem.at[1]).start()

        for copy in inputs:
            copy.wait()
        lane = lax.broadcasted_iota(jnp.int32, (2, META), 1)
        row = lax.broadcasted_iota(jnp.int32, (2, META), 0)
        gates = jnp.zeros((2, META), jnp.int32)
        for k in range(ids_ref.shape[1]):
            gates += jnp.where((lane == idsv[0, k]) & (row == 0), gatesv[0, k], 0)
        tsend[:, 0:META] = gates.astype(F32).astype(BF16)
        tok = tokv[...].astype(F32)
        tsend[:, META:] = jnp.concatenate([tok[:, :half], tok[:, half:]], axis=0).astype(BF16)

        @pl.when(lead)
        def _():
            t1[y * 2 + 1] = tsend[...]

    with scope("bar"):
        pl.semaphore_wait(barrier, ny + jnp.where(lead, ny - 1 + nx - 1 + 2, 0))

    with scope("ypush"):
        for q in range(CHUNKS):
            for v in ys:
                push(tsend.at[:, part(q)], t1.at[y * 2 + c, :, part(q)], s1, r1.at[q], at_y(v, 1))

            @pl.when(jnp.logical_not(lead))
            def _():
                push(tsend.at[:, part(q)], t1.at[y * 2 + c, :, part(q)], s0, r1.at[q], partner)

        for h in range(2):
            wcols = pl.ds(h * half, half)
            push(wg_ref.at[:, :, wcols], wgu.at[h, 0, 1], ws_sem.at[0], wr_sem.at[0], partner)
            push(wu_ref.at[:, :, wcols], wgu.at[h, 1, 1], ws_sem.at[0], wr_sem.at[0], partner)
            push(wd_ref.at[:, :, wcols], wdn.at[h, 1], ws_sem.at[1], wr_sem.at[1], partner)

    cells = nx * ny * 2

    def order(i):
        return ((i // 2) % ny) * nx + i // (2 * ny)

    def picker(col, side):
        i0 = lax.broadcasted_iota(jnp.int32, (cells, cells), 0)
        i1 = lax.broadcasted_iota(jnp.int32, (cells, cells), 1)
        same = ones(i0 // 2 == i1 // 2)
        own = ones(lax.broadcasted_iota(jnp.int32, (rows, META), 1) // 2 == n)
        meta = t2[:, col, :, 0:META].reshape(cells, META)
        if side == 0:
            total = lax.dot_general(own, meta, NT, preferred_element_type=F32)
            hit = ones(total > 0)
            rank = jnp.dot(hit, ones(order(i0) < order(i1)), preferred_element_type=F32)
            hit = jnp.dot(hit, same, preferred_element_type=F32)
            shape = (rows, cells)
        else:
            total = lax.dot_general(meta, own, NT, preferred_element_type=F32)
            hit = ones(total > 0)
            rank = jnp.dot(ones(order(i1) < order(i0)), hit, preferred_element_type=F32)
            hit = jnp.dot(same, hit, preferred_element_type=F32)
            shape = (cells, rows)
        r = lax.broadcasted_iota(jnp.int32, shape, side)
        i = lax.broadcasted_iota(jnp.int32, shape, 1 - side)
        return ones((hit > 0) & (rank == (r // 2).astype(F32)) & (r % 2 == i % 2))

    def weights_here():
        await_bytes(wgu.at[:, :, 0], wl_sem.at[0])
        await_bytes(wdn.at[:, 0], wl_sem.at[1])
        await_bytes(wgu.at[:, :, 1], wr_sem.at[0])
        await_bytes(wdn.at[:, 1], wr_sem.at[1])

    def gate_up(start, blocks, q):
        count = blocks * 2 * rows
        piece = xbuf[start : start + blocks, :, :, pl.ds(d_off[q], width)].reshape(count, width)
        for h in range(2):
            w = wgu[h, :, :, :, :, cols(q)].reshape(2 * units, width)
            v = lax.dot_general(piece, w, NT, preferred_element_type=F32)
            for k in range(2):
                if q == 0:
                    zbuf[h, k, 0:count] = v[:, k * units : (k + 1) * units]
                else:
                    zbuf[h, k, 0:count] += v[:, k * units : (k + 1) * units]

    def activations(start, blocks):
        count = blocks * 2 * rows
        lane = lax.broadcasted_iota(jnp.int32, (META, units), 0)
        unit = lax.broadcasted_iota(jnp.int32, (META, units), 1)
        chosen = ones(lane == 2 * n + (unit // ffl) % 2)
        gate_rows = xbuf[start : start + blocks, :, :, 0:META].reshape(count, META)
        hbuf[0, 0:count] = jnp.dot(gate_rows, chosen, preferred_element_type=F32)
        even, odd = pl.ds(0, count // 2, 2), pl.ds(1, count // 2, 2)
        gate_act = zbuf[0, 0, even, :] + zbuf[1, 0, odd, :]
        up_act = zbuf[0, 1, even, :] + zbuf[1, 1, odd, :]
        scale = hbuf[0, even, :] / 8.0
        hidden = gate_act / (1.0 + jnp.exp(-gate_act)) * up_act * scale
        none = jnp.zeros_like(hidden)
        hbuf[0, even, :] = hidden
        hbuf[1, even, :] = none
        hbuf[0, odd, :] = none
        hbuf[1, odd, :] = hidden
        return jnp.concatenate([hbuf[0, 0:count], hbuf[1, 0:count]], axis=1).astype(BF16)

    def project(hidden, q):
        w = wdn[:, :, :, :, cols(q)].reshape(2 * units, width)
        return jnp.dot(hidden, w, preferred_element_type=F32)

    def slot(direction, step):
        return direction * hz + step - 1

    @pl.when(jnp.logical_not(lead))
    def _():
        with scope("s_wait"):
            weights_here()
            await_bytes(xbuf.at[0:near], rx)
        with scope("s_gateup"):
            for q in range(CHUNKS):
                gate_up(0, near, q)
        with scope("s_act"):
            hidden = activations(0, near)
        with scope("s_down"):
            for q in range(CHUNKS):
                v = project(hidden, q)
                pnear[:, :, :, cols(q)] = v.reshape(near, 2, rows, width).astype(BF16)
            for s in range(hz - 2, 0, -1):
                for b in (going_down(s), going_up(s)):
                    push(pnear.at[b], pnear.at[b], sp, rp.at[s], partner)
            push(pnear.at[0], pnear.at[0], sp, rp.at[0], partner)

    @pl.when(lead)
    def _():
        with scope("xstage"):
            for q in range(CHUNKS):
                await_bytes(t1.at[pl.ds(0, 2 * ny - 1), :, part(q)], r1.at[q])
                for v in range(ny):
                    for col in range(2):
                        t2[x, col, 2 * v : 2 * v + 2, part(q)] = t1[2 * v + col, :, part(q)]
                for v in xs:
                    own = t2.at[x, :, :, part(q)]
                    push(own, own, s2, r2.at[q], at_x(v))

        with scope("pack"):
            pickers = None
            for q in range(CHUNKS):
                await_bytes(t2.at[pl.ds(0, nx - 1), :, :, part(q)], r2.at[q])
                if q == 0:
                    pickers = [picker(col, 0) for col in range(2)]
                for col in range(2):
                    field = t2[:, col, :, part(q)].reshape(cells, lens[q])
                    picked = jnp.dot(pickers[col], field, preferred_element_type=F32)
                    xbuf[0, col, :, part(q)] = picked.astype(BF16)
                own = xbuf.at[0, :, :, part(q)]
                push(own, xbuf.at[going_up(1), :, :, part(q)], sa, ra.at[slot(0, 1), q], up)
                push(own, xbuf.at[going_down(1), :, :, part(q)], sa, ra.at[slot(1, 1), q], down)
                push(own, own, sx, rx, partner)
            weights_here()

        with scope("ring"):
            for s in range(1, hz + 1):
                for q in range(CHUNKS):
                    b = going_up(s)
                    block = xbuf.at[b, :, :, part(q)]
                    await_bytes(block, ra.at[slot(0, s), q])
                    if s < hz:
                        push(block, xbuf.at[going_up(s + 1), :, :, part(q)], sa, ra.at[slot(0, s + 1), q], up)
                    if b < near:
                        push(block, block, sx, rx, partner)
                    if s < hz:
                        b = going_down(s)
                        block = xbuf.at[b, :, :, part(q)]
                        await_bytes(block, ra.at[slot(1, s), q])
                        if s < hz - 1:
                            push(block, xbuf.at[going_down(s + 1), :, :, part(q)], sa, ra.at[slot(1, s + 1), q], down)
                        if b < near:
                            push(block, block, sx, rx, partner)
                    else:
                        gate_up(near, far, q)
        with scope("act"):
            hidden = activations(near, far)

        def onward(direction, s, q, value, device):
            i = slot(direction, s)
            if s > 1:
                await_bytes(rrecv.at[i - 1, :, :, cols(q)], rs.at[i - 1, q])
                value = value.astype(F32) + rrecv[i - 1, :, :, cols(q)].astype(F32)
            rsend[i, :, :, cols(q)] = value.astype(BF16)
            push(rsend.at[i, :, :, cols(q)], rrecv.at[i, :, :, cols(q)], ss, rs.at[i, q], device)

        with scope("rs1"):
            for q in range(CHUNKS):
                v = project(hidden, q).reshape(far, 2, rows, width)
                pfar[:, :, cols(q)] = v[2]
                onward(0, 1, q, v[1], up)
                onward(1, 1, q, v[0], down)
        with scope("rs"):
            for s in range(2, hz + 1):
                above, below = hz + 1 - s, hz - s
                if s < hz:
                    await_bytes(pnear.at[0:2], rp.at[below])
                for q in range(CHUNKS):
                    value = pfar[:, :, cols(q)] if s == 2 else pnear[going_down(above), :, :, cols(q)]
                    onward(0, s, q, value, up)
                    if s < hz:
                        onward(1, s, q, pnear[going_up(below), :, :, cols(q)], down)

        with scope("retx"):
            pickers = [picker(col, 1) for col in range(2)]
            await_bytes(pnear.at[0], rp.at[0])
            for q in range(CHUNKS):
                one, two = slot(0, hz), slot(1, hz - 1)
                await_bytes(rrecv.at[two, :, :, cols(q)], rs.at[two, q])
                await_bytes(rrecv.at[one, :, :, cols(q)], rs.at[one, q])
                total = pnear[0, :, :, cols(q)].astype(F32) + rrecv[one, :, :, cols(q)].astype(F32)
                total = (total + rrecv[two, :, :, cols(q)].astype(F32)).astype(BF16)
                for col in range(2):
                    placed = jnp.dot(pickers[col], total[col], preferred_element_type=F32)
                    ysend[:, col, :, cols(q)] = placed.astype(BF16).reshape(nx, 2 * ny, width)
                for v in xs:
                    push(ysend.at[v, :, :, cols(q)], yrecv.at[x, :, :, cols(q)], s3, r3.at[q], at_x(v))
        with scope("rety"):
            for q in range(CHUNKS):
                await_bytes(yrecv.at[pl.ds(0, nx - 1), :, :, cols(q)], r3.at[q])
                total = ysend[x, :, :, cols(q)].astype(F32)
                for v in xs:
                    total += yrecv[v, :, :, cols(q)].astype(F32)
                total = total.astype(BF16)
                for v in range(ny):
                    for col in range(2):
                        fsend[v, col, :, cols(q)] = total[col, 2 * v : 2 * v + 2, :]
                for v in ys:
                    for col in range(2):
                        push(fsend.at[v, col, :, cols(q)], frecv.at[y, :, cols(q)], s4, r4.at[q], at_y(v, col))
                push(fsend.at[y, 0, :, cols(q)], frecv.at[y, :, cols(q)], s0, r4.at[q], partner)
                frecv[y, :, cols(q)] = fsend[y, 1, :, cols(q)]

    with scope("final"):
        for q in range(CHUNKS):
            @pl.when(lead)
            def _():
                await_bytes(frecv.at[0 : ny - 1, :, cols(q)], r4.at[q])

            @pl.when(jnp.logical_not(lead))
            def _():
                await_bytes(frecv.at[:, :, cols(q)], r4.at[q])

            total = frecv[0, :, cols(q)].astype(F32)
            for v in range(1, ny):
                total += frecv[v, :, cols(q)].astype(F32)
            total = total.astype(BF16)
            out_ref[0:1, cols(q)] = total[0:1, :]
            out_ref[0:1, pl.ds(half + q * width, width)] = total[1:2, :]

    with scope("drain"):
        await_bytes(t1.at[0 : ny - 1], s1)
        await_bytes(wgu.at[:, :, 1], ws_sem.at[0])
        await_bytes(wdn.at[:, 1], ws_sem.at[1])

        @pl.when(jnp.logical_not(lead))
        def _():
            await_bytes(tsend, s0)
            await_bytes(pnear, sp)

        @pl.when(lead)
        def _():
            await_bytes(t2.at[0 : nx - 1], s2)
            await_bytes(xbuf.at[0 : nz - 1], sa)
            await_bytes(xbuf.at[0:near], sx)
            await_bytes(rsend, ss)
            await_bytes(yrecv.at[0 : nx - 1], s3)
            await_bytes(fsend.at[0 : ny - 1], s4)
            await_bytes(frecv.at[0], s0)


def solution(mesh):
    nodes, locals_ = mesh.shape["node"], mesh.shape["local"]
    nx = min(NX, nodes)
    ny, nz = nodes // nx, locals_ // 2
    hz = nz // 2
    near = 1 + 2 * (hz - 2)

    def on_device(tokens, w_gate, w_up, w_down, expert_ids, gate_ints):
        model_width = tokens.shape[1]
        half = model_width // 2
        exp_node, ffl = w_gate.shape[0], w_gate.shape[1]
        units = 2 * exp_node * ffl
        rows = 2 * CAP
        sem = pltpu.SemaphoreType.DMA
        one = sem(())
        any_space = pl.BlockSpec(memory_space=pl.ANY)
        vmem = pl.BlockSpec(memory_space=pltpu.VMEM)
        return pl.pallas_call(
            functools.partial(layer_kernel, nx, ny, nz),
            out_shape=jax.ShapeDtypeStruct((1, model_width), BF16),
            in_specs=[any_space] * 6,
            out_specs=vmem,
            scratch_shapes=[
                pltpu.VMEM((1, model_width), BF16),
                pltpu.SMEM(expert_ids.shape, jnp.int32),
                pltpu.SMEM(gate_ints.shape, jnp.int32),
                pltpu.VMEM((2, META + half), BF16),
                pltpu.VMEM((2 * ny, 2, META + half), BF16),
                pltpu.VMEM((nx, 2, 2 * ny, META + half), BF16),
                pltpu.VMEM((nz, 2, rows, META + half), BF16),
                pltpu.VMEM((2, 2, 2, exp_node, ffl, half), BF16),
                pltpu.VMEM((2, 2, exp_node, ffl, half), BF16),
                pltpu.VMEM((2, 2, near * 2 * rows, units), F32),
                pltpu.VMEM((2, near * 2 * rows, units), F32),
                pltpu.VMEM((2, rows, half), F32),
                pltpu.VMEM((near, 2, rows, half), BF16),
                pltpu.VMEM((nz - 1, 2, rows, half), BF16),
                pltpu.VMEM((nz - 1, 2, rows, half), BF16),
                pltpu.VMEM((nx, 2, 2 * ny, half), BF16),
                pltpu.VMEM((nx, 2, 2 * ny, half), BF16),
                pltpu.VMEM((ny, 2, 2, half), BF16),
                pltpu.VMEM((ny, 2, half), BF16),
                sem((3,)), sem((2,)), sem((2,)), sem((2,)),
                one, one, sem((CHUNKS,)), one, sem((CHUNKS,)),
                one, sem((nz - 1, CHUNKS)), one, one, one, sem((hz - 1,)),
                one, sem((nz - 1, CHUNKS)), one, sem((CHUNKS,)), one, sem((CHUNKS,)),
            ],
            compiler_params=pltpu.CompilerParams(
                collective_id=0, has_side_effects=True, vmem_limit_bytes=60 * 1024 * 1024
            ),
            name="layer",
        )(tokens, w_gate, w_up, w_down, expert_ids, gate_ints)

    both = P(("node", "local"), None)
    weights = P("node", "local", None)
    return jax.shard_map(
        on_device, mesh=mesh,
        in_specs=(both, weights, weights, weights, both, both),
        out_specs=both, check_vma=False,
    )
```

```python
import functools

import jax
import jax.numpy as jnp
from jax import lax
from jax.experimental import pallas as pl
from jax.experimental.pallas import tpu as pltpu
from jax.sharding import PartitionSpec as P

CAP = 8
NX = 4
CHUNKS = 7
META = 128
BF16 = jnp.bfloat16
F32 = jnp.float32
MESH_ID = pl.DeviceIdType.MESH
NT = (((1,), (1,)), ((), ()))
scope = jax.named_scope


def ones(mask):
    return mask.astype(F32).astype(BF16)


def layer_kernel(
    nx, ny, nz,
    tok_ref, wg_ref, wu_ref, wd_ref, ids_ref, gates_ref,
    out_ref,
    tokv, idsv, gatesv, tsend, t1, t2, xbuf, wgu, wdn, zbuf, hbuf, pnear, rsend, rrecv,
    ysend, yrecv, fsend, frecv, ftok, ft1, ft2, fxs, fxr, fys, fyr, fzs, fin,
    in_sem, wl_sem, ws_sem, wr_sem, s0, s1, r1, s2, r2, sa, ra, sx, rx, sp, rp, ss, rs, s3, r3, s4, r4,
    fs, fr, ready,
):
    half = wgu.shape[-1]
    width = half // CHUNKS
    offs = [0] + [META + q * width for q in range(1, CHUNKS)]
    lens = [META + width] + [width] * (CHUNKS - 1)
    d_off = [META + q * width for q in range(CHUNKS)]
    hz = nz // 2
    rows = CAP * 2
    ffl = wdn.shape[3]
    units = wdn.shape[1] * wdn.shape[2] * ffl
    n = lax.axis_index("node")
    l = lax.axis_index("local")
    x, y = lax.rem(n, nx), n // nx
    z, c = l // 2, lax.rem(l, 2)
    lead = c == 1

    def at_x(v, core=1):
        return (y * nx + v, z * 2 + core)

    def at_y(v, core):
        return (v * nx + x, z * 2 + core)

    up = (n, lax.rem(z + 1, nz) * 2 + 1)
    down = (n, lax.rem(z + nz - 1, nz) * 2 + 1)
    partner = (n, z * 2 + 1 - c)
    xs = [lax.rem(x + d, nx) for d in range(1, nx)]
    ys = [lax.rem(y + d, ny) for d in range(1, ny)]

    steps = hz - 1
    near = 2 * steps - 1
    opposite = near + 2

    def going_up(s):
        return s if s < steps else near

    def going_down(s):
        return steps - 1 + s if s < steps else near + 1

    early = z < hz

    def across(core):
        return (n, lax.rem(z + hz, nz) * 2 + core)

    def push(src, dst, send, recv, device):
        pltpu.make_async_remote_copy(
            src_ref=src, dst_ref=dst, send_sem=send, recv_sem=recv,
            device_id=device, device_id_type=MESH_ID,
        ).start()

    def await_bytes(ref, sem):
        pltpu.make_async_copy(ref, ref, sem).wait()

    def signal(sem, device):
        pl.semaphore_signal(sem, 1, device_id=device, device_id_type=MESH_ID)

    def part(q):
        return pl.ds(offs[q], lens[q])

    def cols(q):
        return pl.ds(q * width, width)

    barrier = pltpu.get_barrier_semaphore()
    with scope("entry"):
        signal(barrier, partner)
        for v in ys:
            signal(barrier, at_y(v, 1))
            signal(barrier, at_y(v, 0))
        for v in xs:
            signal(barrier, at_x(v, c))

        @pl.when(lead)
        def _():
            signal(barrier, up)
            signal(barrier, down)

        @pl.when(early)
        def _():
            signal(barrier, across(0))

            @pl.when(jnp.logical_not(lead))
            def _():
                signal(barrier, across(1))

        inputs = [
            pltpu.make_async_copy(tok_ref, tokv, in_sem.at[0]),
            pltpu.make_async_copy(ids_ref, idsv, in_sem.at[1]),
            pltpu.make_async_copy(gates_ref, gatesv, in_sem.at[2]),
        ]
        for copy in inputs:
            copy.start()
        for h in range(2):
            wcols = pl.ds(h * half, half)
            pltpu.make_async_copy(wg_ref.at[:, :, wcols], wgu.at[h, 0, 0], wl_sem.at[0]).start()
            pltpu.make_async_copy(wu_ref.at[:, :, wcols], wgu.at[h, 1, 0], wl_sem.at[0]).start()
            pltpu.make_async_copy(wd_ref.at[:, :, wcols], wdn.at[h, 0], wl_sem.at[1]).start()

        for copy in inputs:
            copy.wait()
        lane = lax.broadcasted_iota(jnp.int32, (2, META), 1)
        row = lax.broadcasted_iota(jnp.int32, (2, META), 0)
        gates = jnp.zeros((2, META), jnp.int32)
        for k in range(ids_ref.shape[1]):
            gates += jnp.where((lane == idsv[0, k]) & (row == 0), gatesv[0, k], 0)
        tsend[:, 0:META] = gates.astype(F32).astype(BF16)
        tok = tokv[...].astype(F32)
        tsend[:, META:] = jnp.concatenate([tok[:, :half], tok[:, half:]], axis=0).astype(BF16)

        @pl.when(lead)
        def _():
            t1[y * 2 + 1] = tsend[...]

        @pl.when(jnp.logical_not(lead))
        def _():
            ftok[0] = tsend[...]

    with scope("bar"):
        count = 1 + 2 * (ny - 1) + nx - 1 + 2 * c + (z // hz) * (2 - c)
        pl.semaphore_wait(barrier, count)

        @pl.when(jnp.logical_not(early))
        def _():
            signal(ready, across(0))

    with scope("ypush"):
        for q in range(CHUNKS):
            for v in ys:
                push(tsend.at[:, part(q)], t1.at[y * 2 + c, :, part(q)], s1, r1.at[q], at_y(v, 1))

            @pl.when(jnp.logical_not(lead))
            def _():
                push(tsend.at[:, part(q)], t1.at[y * 2 + c, :, part(q)], s0, r1.at[q], partner)

        @pl.when(lead)
        def _():
            push(tsend, ftok.at[1], fs.at[0], fr.at[6], partner)

        for h in range(2):
            wcols = pl.ds(h * half, half)
            push(wg_ref.at[:, :, wcols], wgu.at[h, 0, 1], ws_sem.at[0], wr_sem.at[0], partner)
            push(wu_ref.at[:, :, wcols], wgu.at[h, 1, 1], ws_sem.at[0], wr_sem.at[0], partner)
            push(wd_ref.at[:, :, wcols], wdn.at[h, 1], ws_sem.at[1], wr_sem.at[1], partner)

    cells = nx * ny * 2

    def order(i):
        return ((i // 2) % ny) * nx + i // (2 * ny)

    def picker(field, col, side):
        i0 = lax.broadcasted_iota(jnp.int32, (cells, cells), 0)
        i1 = lax.broadcasted_iota(jnp.int32, (cells, cells), 1)
        same = ones(i0 // 2 == i1 // 2)
        own = ones(lax.broadcasted_iota(jnp.int32, (rows, META), 1) // 2 == n)
        meta = field[:, col, :, 0:META].reshape(cells, META)
        if side == 0:
            total = lax.dot_general(own, meta, NT, preferred_element_type=F32)
            hit = ones(total > 0)
            rank = jnp.dot(hit, ones(order(i0) < order(i1)), preferred_element_type=F32)
            hit = jnp.dot(hit, same, preferred_element_type=F32)
            shape = (rows, cells)
        else:
            total = lax.dot_general(meta, own, NT, preferred_element_type=F32)
            hit = ones(total > 0)
            rank = jnp.dot(ones(order(i1) < order(i0)), hit, preferred_element_type=F32)
            hit = jnp.dot(same, hit, preferred_element_type=F32)
            shape = (cells, rows)
        r = lax.broadcasted_iota(jnp.int32, shape, side)
        i = lax.broadcasted_iota(jnp.int32, shape, 1 - side)
        return ones((hit > 0) & (rank == (r // 2).astype(F32)) & (r % 2 == i % 2))

    def weights_here():
        await_bytes(wgu.at[:, :, 0], wl_sem.at[0])
        await_bytes(wdn.at[:, 0], wl_sem.at[1])
        await_bytes(wgu.at[:, :, 1], wr_sem.at[0])
        await_bytes(wdn.at[:, 1], wr_sem.at[1])

    def gate_up(start, blocks, q):
        count = blocks * 2 * rows
        piece = xbuf[start : start + blocks, :, :, pl.ds(d_off[q], width)].reshape(count, width)
        for h in range(2):
            w = wgu[h, :, :, :, :, cols(q)].reshape(2 * units, width)
            v = lax.dot_general(piece, w, NT, preferred_element_type=F32)
            for k in range(2):
                if q == 0:
                    zbuf[h, k, 0:count] = v[:, k * units : (k + 1) * units]
                else:
                    zbuf[h, k, 0:count] += v[:, k * units : (k + 1) * units]

    def activations(start, blocks):
        count = blocks * 2 * rows
        lane = lax.broadcasted_iota(jnp.int32, (META, units), 0)
        unit = lax.broadcasted_iota(jnp.int32, (META, units), 1)
        chosen = ones(lane == 2 * n + (unit // ffl) % 2)
        gate_rows = xbuf[start : start + blocks, :, :, 0:META].reshape(count, META)
        hbuf[0, 0:count] = jnp.dot(gate_rows, chosen, preferred_element_type=F32)
        even, odd = pl.ds(0, count // 2, 2), pl.ds(1, count // 2, 2)
        gate_act = zbuf[0, 0, even, :] + zbuf[1, 0, odd, :]
        up_act = zbuf[0, 1, even, :] + zbuf[1, 1, odd, :]
        scale = hbuf[0, even, :] / 8.0
        hidden = gate_act / (1.0 + jnp.exp(-gate_act)) * up_act * scale
        none = jnp.zeros_like(hidden)
        hbuf[0, even, :] = hidden
        hbuf[1, even, :] = none
        hbuf[0, odd, :] = none
        hbuf[1, odd, :] = hidden
        return jnp.concatenate([hbuf[0, 0:count], hbuf[1, 0:count]], axis=1).astype(BF16)

    def project(hidden, q):
        w = wdn[:, :, :, :, cols(q)].reshape(2 * units, width)
        return jnp.dot(hidden, w, preferred_element_type=F32)

    def slot(direction, step):
        return direction * steps + step - 1

    @pl.when(jnp.logical_not(lead))
    def _():
        with scope("f_token"):
            @pl.when(early)
            def _():
                pl.semaphore_wait(ready, 2)

            await_bytes(ftok.at[1], fr.at[6])
            push(ftok, ft1.at[y], fs.at[0], fr.at[0], across(0))
        with scope("f_y"):
            await_bytes(ft1.at[y], fr.at[0])
            for v in ys:
                push(ft1.at[y], ft1.at[y], fs.at[1], fr.at[1], at_y(v, 0))
        with scope("f_x"):
            await_bytes(ft1.at[0 : ny - 1], fr.at[1])
            for v in range(ny):
                for col in range(2):
                    ft2[x, col, 2 * v : 2 * v + 2] = ft1[v, col]
            for v in xs:
                push(ft2.at[x], ft2.at[x], fs.at[2], fr.at[2], at_x(v, 0))
        with scope("s_wait"):
            weights_here()
            await_bytes(xbuf.at[0:near], rx)
        with scope("s_gateup"):
            for q in range(CHUNKS):
                gate_up(0, near, q)
        with scope("s_act"):
            hidden = activations(0, near)
        with scope("s_down"):
            for q in range(CHUNKS):
                v = project(hidden, q)
                pnear[:, :, :, cols(q)] = v.reshape(near, 2, rows, width).astype(BF16)
            for s in range(steps - 1, 0, -1):
                for b in (going_down(s), going_up(s)):
                    push(pnear.at[b], pnear.at[b], sp, rp.at[s], partner)
            push(pnear.at[0], pnear.at[0], sp, rp.at[0], partner)
        with scope("f_pack"):
            await_bytes(ft2.at[0 : nx - 1], fr.at[2])
            pickers = [picker(ft2, col, 0) for col in range(2)]
            for col in range(2):
                for q in range(CHUNKS):
                    field = ft2[:, col, :, part(q)].reshape(cells, lens[q])
                    picked = jnp.dot(pickers[col], field, preferred_element_type=F32)
                    xbuf[opposite, col, :, part(q)] = picked.astype(BF16)
            for q in range(CHUNKS):
                gate_up(opposite, 1, q)
            hidden = activations(opposite, 1)
        with scope("f_retx"):
            pickers = [picker(ft2, col, 1) for col in range(2)]
            for q in range(CHUNKS):
                v = project(hidden, q).astype(BF16).reshape(2, rows, width)
                for col in range(2):
                    placed = jnp.dot(pickers[col], v[col], preferred_element_type=F32)
                    fxs[:, col, :, cols(q)] = placed.astype(BF16).reshape(nx, 2 * ny, width)
            for v in xs:
                push(fxs.at[v], fxr.at[x], fs.at[3], fr.at[3], at_x(v, 0))
        with scope("f_rety"):
            await_bytes(fxr.at[0 : nx - 1], fr.at[3])
            for q in range(CHUNKS):
                total = fxs[x, :, :, cols(q)].astype(F32)
                for v in xs:
                    total += fxr[v, :, :, cols(q)].astype(F32)
                total = total.astype(BF16)
                for v in range(ny):
                    for col in range(2):
                        fys[v, col, :, cols(q)] = total[col, 2 * v : 2 * v + 2, :]
            for v in ys:
                push(fys.at[v], fyr.at[y], fs.at[4], fr.at[4], at_y(v, 0))
        with scope("f_retz"):
            await_bytes(fyr.at[0 : ny - 1], fr.at[4])
            for q in range(CHUNKS):
                total = fys[y, :, :, cols(q)].astype(F32)
                for v in ys:
                    total += fyr[v, :, :, cols(q)].astype(F32)
                fzs[:, :, cols(q)] = total.astype(BF16)
            for core in range(2):
                push(fzs.at[core], fin, fs.at[5], fr.at[5], across(core))

    @pl.when(lead)
    def _():
        with scope("xstage"):
            for q in range(CHUNKS):
                await_bytes(t1.at[pl.ds(0, 2 * ny - 1), :, part(q)], r1.at[q])
                for v in range(ny):
                    for col in range(2):
                        t2[x, col, 2 * v : 2 * v + 2, part(q)] = t1[2 * v + col, :, part(q)]
                for v in xs:
                    own = t2.at[x, :, :, part(q)]
                    push(own, own, s2, r2.at[q], at_x(v))

        with scope("pack"):
            pickers = None
            for q in range(CHUNKS):
                await_bytes(t2.at[pl.ds(0, nx - 1), :, :, part(q)], r2.at[q])
                if q == 0:
                    pickers = [picker(t2, col, 0) for col in range(2)]
                for col in range(2):
                    field = t2[:, col, :, part(q)].reshape(cells, lens[q])
                    picked = jnp.dot(pickers[col], field, preferred_element_type=F32)
                    xbuf[0, col, :, part(q)] = picked.astype(BF16)
                own = xbuf.at[0, :, :, part(q)]
                push(own, xbuf.at[going_up(1), :, :, part(q)], sa, ra.at[slot(0, 1), q], up)
                push(own, xbuf.at[going_down(1), :, :, part(q)], sa, ra.at[slot(1, 1), q], down)
                push(own, own, sx, rx, partner)
            weights_here()

        with scope("ring"):
            for s in range(1, steps + 1):
                for q in range(CHUNKS):
                    for direction, b, later, device in (
                        (0, going_up(s), going_up(s + 1), up),
                        (1, going_down(s), going_down(s + 1), down),
                    ):
                        block = xbuf.at[b, :, :, part(q)]
                        await_bytes(block, ra.at[slot(direction, s), q])
                        if s < steps:
                            push(block, xbuf.at[later, :, :, part(q)], sa, ra.at[slot(direction, s + 1), q], device)
                            push(block, block, sx, rx, partner)
                    if s == steps:
                        gate_up(near, 2, q)
        with scope("act"):
            hidden = activations(near, 2)

        def onward(direction, s, q, value, device):
            i = slot(direction, s)
            if s > 1:
                await_bytes(rrecv.at[i - 1, :, :, cols(q)], rs.at[i - 1, q])
                value = value + rrecv[i - 1, :, :, cols(q)]
            rsend[i, :, :, cols(q)] = value
            push(rsend.at[i, :, :, cols(q)], rrecv.at[i, :, :, cols(q)], ss, rs.at[i, q], device)

        with scope("rs1"):
            for q in range(CHUNKS):
                v = project(hidden, q).astype(BF16).reshape(2, 2, rows, width)
                onward(0, 1, q, v[1], up)
                onward(1, 1, q, v[0], down)
        with scope("rs"):
            pickers = [picker(t2, col, 1) for col in range(2)]
            for s in range(2, steps + 1):
                at = steps + 1 - s
                await_bytes(pnear.at[0:2], rp.at[at])
                for q in range(CHUNKS):
                    onward(0, s, q, pnear[going_down(at), :, :, cols(q)], up)
                    onward(1, s, q, pnear[going_up(at), :, :, cols(q)], down)

        with scope("retx"):
            await_bytes(pnear.at[0], rp.at[0])
            for q in range(CHUNKS):
                one, two = slot(0, steps), slot(1, steps)
                await_bytes(rrecv.at[two, :, :, cols(q)], rs.at[two, q])
                await_bytes(rrecv.at[one, :, :, cols(q)], rs.at[one, q])
                total = pnear[0, :, :, cols(q)].astype(F32) + rrecv[one, :, :, cols(q)].astype(F32)
                total = (total + rrecv[two, :, :, cols(q)].astype(F32)).astype(BF16)
                for col in range(2):
                    placed = jnp.dot(pickers[col], total[col], preferred_element_type=F32)
                    ysend[:, col, :, cols(q)] = placed.astype(BF16).reshape(nx, 2 * ny, width)
                for v in xs:
                    push(ysend.at[v, :, :, cols(q)], yrecv.at[x, :, :, cols(q)], s3, r3.at[q], at_x(v))
        with scope("rety"):
            for q in range(CHUNKS):
                await_bytes(yrecv.at[pl.ds(0, nx - 1), :, :, cols(q)], r3.at[q])
                total = ysend[x, :, :, cols(q)].astype(F32)
                for v in xs:
                    total += yrecv[v, :, :, cols(q)].astype(F32)
                total = total.astype(BF16)
                for v in range(ny):
                    for col in range(2):
                        fsend[v, col, :, cols(q)] = total[col, 2 * v : 2 * v + 2, :]
                for v in ys:
                    for col in range(2):
                        push(fsend.at[v, col, :, cols(q)], frecv.at[y, :, cols(q)], s4, r4.at[q], at_y(v, col))
                push(fsend.at[y, 0, :, cols(q)], frecv.at[y, :, cols(q)], s0, r4.at[q], partner)
                frecv[y, :, cols(q)] = fsend[y, 1, :, cols(q)]

    with scope("final"):
        for q in range(CHUNKS):
            @pl.when(lead)
            def _():
                await_bytes(frecv.at[0 : ny - 1, :, cols(q)], r4.at[q])

            @pl.when(jnp.logical_not(lead))
            def _():
                await_bytes(frecv.at[:, :, cols(q)], r4.at[q])

            if q == 0:
                await_bytes(fin, fr.at[5])
            total = fin[:, cols(q)].astype(F32)
            for v in range(ny):
                total += frecv[v, :, cols(q)].astype(F32)
            total = total.astype(BF16)
            out_ref[0:1, cols(q)] = total[0:1, :]
            out_ref[0:1, pl.ds(half + q * width, width)] = total[1:2, :]

    with scope("drain"):
        await_bytes(t1.at[0 : ny - 1], s1)
        await_bytes(wgu.at[:, :, 1], ws_sem.at[0])
        await_bytes(wdn.at[:, 1], ws_sem.at[1])

        @pl.when(jnp.logical_not(lead))
        def _():
            await_bytes(tsend, s0)
            await_bytes(pnear, sp)
            await_bytes(ftok, fs.at[0])
            await_bytes(ft1.at[0 : ny - 1], fs.at[1])
            await_bytes(ft2.at[0 : nx - 1], fs.at[2])
            await_bytes(fxs.at[0 : nx - 1], fs.at[3])
            await_bytes(fys.at[0 : ny - 1], fs.at[4])
            await_bytes(fzs, fs.at[5])

        @pl.when(lead)
        def _():
            await_bytes(t2.at[0 : nx - 1], s2)
            await_bytes(xbuf.at[0 : 2 * steps], sa)
            await_bytes(xbuf.at[0:near], sx)
            await_bytes(rsend, ss)
            await_bytes(yrecv.at[0 : nx - 1], s3)
            await_bytes(fsend.at[0 : ny - 1], s4)
            await_bytes(frecv.at[0], s0)
            await_bytes(tsend, fs.at[0])


def solution(mesh):
    nodes, locals_ = mesh.shape["node"], mesh.shape["local"]
    nx = min(NX, nodes)
    ny, nz = nodes // nx, locals_ // 2
    hz = nz // 2
    steps = hz - 1
    near = 2 * steps - 1

    def on_device(tokens, w_gate, w_up, w_down, expert_ids, gate_ints):
        model_width = tokens.shape[1]
        half = model_width // 2
        exp_node, ffl = w_gate.shape[0], w_gate.shape[1]
        units = 2 * exp_node * ffl
        rows = 2 * CAP
        sem = pltpu.SemaphoreType.DMA
        one = sem(())
        any_space = pl.BlockSpec(memory_space=pl.ANY)
        vmem = pl.BlockSpec(memory_space=pltpu.VMEM)
        return pl.pallas_call(
            functools.partial(layer_kernel, nx, ny, nz),
            out_shape=jax.ShapeDtypeStruct((1, model_width), BF16),
            in_specs=[any_space] * 6,
            out_specs=vmem,
            scratch_shapes=[
                pltpu.VMEM((1, model_width), BF16),
                pltpu.SMEM(expert_ids.shape, jnp.int32),
                pltpu.SMEM(gate_ints.shape, jnp.int32),
                pltpu.VMEM((2, META + half), BF16),
                pltpu.VMEM((2 * ny, 2, META + half), BF16),
                pltpu.VMEM((nx, 2, 2 * ny, META + half), BF16),
                pltpu.VMEM((nz, 2, rows, META + half), BF16),
                pltpu.VMEM((2, 2, 2, exp_node, ffl, half), BF16),
                pltpu.VMEM((2, 2, exp_node, ffl, half), BF16),
                pltpu.VMEM((2, 2, near * 2 * rows, units), F32),
                pltpu.VMEM((2, near * 2 * rows, units), F32),
                pltpu.VMEM((near, 2, rows, half), BF16),
                pltpu.VMEM((2 * steps, 2, rows, half), BF16),
                pltpu.VMEM((2 * steps, 2, rows, half), BF16),
                pltpu.VMEM((nx, 2, 2 * ny, half), BF16),
                pltpu.VMEM((nx, 2, 2 * ny, half), BF16),
                pltpu.VMEM((ny, 2, 2, half), BF16),
                pltpu.VMEM((ny, 2, half), BF16),
                pltpu.VMEM((2, 2, META + half), BF16),
                pltpu.VMEM((ny, 2, 2, META + half), BF16),
                pltpu.VMEM((nx, 2, 2 * ny, META + half), BF16),
                pltpu.VMEM((nx, 2, 2 * ny, half), BF16),
                pltpu.VMEM((nx, 2, 2 * ny, half), BF16),
                pltpu.VMEM((ny, 2, 2, half), BF16),
                pltpu.VMEM((ny, 2, 2, half), BF16),
                pltpu.VMEM((2, 2, half), BF16),
                pltpu.VMEM((2, half), BF16),
                sem((3,)), sem((2,)), sem((2,)), sem((2,)),
                one, one, sem((CHUNKS,)), one, sem((CHUNKS,)),
                one, sem((2 * steps, CHUNKS)), one, one, one, sem((steps,)),
                one, sem((2 * steps, CHUNKS)), one, sem((CHUNKS,)), one, sem((CHUNKS,)),
                sem((6,)), sem((7,)), pltpu.SemaphoreType.REGULAR,
            ],
            compiler_params=pltpu.CompilerParams(
                collective_id=0, has_side_effects=True, vmem_limit_bytes=60 * 1024 * 1024
            ),
            name="layer",
        )(tokens, w_gate, w_up, w_down, expert_ids, gate_ints)

    both = P(("node", "local"), None)
    weights = P("node", "local", None)
    return jax.shard_map(
        on_device, mesh=mesh,
        in_specs=(both, weights, weights, weights, both, both),
        out_specs=both, check_vma=False,
    )
```

```python
import functools

import jax
import jax.numpy as jnp
from jax import lax
from jax.experimental import pallas as pl
from jax.experimental.pallas import tpu as pltpu
from jax.sharding import PartitionSpec as P

CAP = 8
NX = 4
CHUNKS = 7
OTHER = 2
META = 128
BF16 = jnp.bfloat16
F32 = jnp.float32
MESH_ID = pl.DeviceIdType.MESH
NT = (((1,), (1,)), ((), ()))
scope = jax.named_scope


def ones(mask):
    return mask.astype(F32).astype(BF16)


def layer_kernel(
    nx, ny, nz,
    tok_ref, wg_ref, wu_ref, wd_ref, ids_ref, gates_ref,
    out_ref,
    tokv, idsv, gatesv, tsend, t1, t2, xbuf, wgu, wdn, zbuf, hbuf, pnear, rsend, rrecv,
    ysend, yrecv, fsend, frecv, ftok, ft1, ft2, fxs, fxr, fys, fyr, fzs, fin, a1, b1, c1, c2, e1, e2,
    in_sem, wl_sem, ws_sem, wr_sem, s0, s1, r1, s2, r2, sa, ra, sx, rx, sp, rp, ss, s3, r3, s4, r4,
    fs, fr, ready, so,
):
    half = wgu.shape[-1]
    width = half // CHUNKS
    offs = [0] + [META + q * width for q in range(1, CHUNKS)]
    lens = [META + width] + [width] * (CHUNKS - 1)
    d_off = [META + q * width for q in range(CHUNKS)]
    hz = nz // 2
    rows = CAP * 2
    ffl = wdn.shape[3]
    units = wdn.shape[1] * wdn.shape[2] * ffl
    n = lax.axis_index("node")
    l = lax.axis_index("local")
    x, y = lax.rem(n, nx), n // nx
    z, c = l // 2, lax.rem(l, 2)
    lead = c == 1

    def at_x(v, core=1):
        return (y * nx + v, z * 2 + core)

    def at_y(v, core):
        return (v * nx + x, z * 2 + core)

    up = (n, lax.rem(z + 1, nz) * 2 + 1)
    down = (n, lax.rem(z + nz - 1, nz) * 2 + 1)
    partner = (n, z * 2 + 1 - c)
    xs = [lax.rem(x + d, nx) for d in range(1, nx)]
    ys = [lax.rem(y + d, ny) for d in range(1, ny)]

    steps = hz - 1
    near = 2 * steps - 1
    opposite = near + 2

    def going_up(s):
        return 2 * s - 1

    def going_down(s):
        return 2 * s

    early = z < hz

    def across(core):
        return (n, lax.rem(z + hz, nz) * 2 + core)

    def push(src, dst, send, recv, device):
        pltpu.make_async_remote_copy(
            src_ref=src, dst_ref=dst, send_sem=send, recv_sem=recv,
            device_id=device, device_id_type=MESH_ID,
        ).start()

    def await_bytes(ref, sem):
        pltpu.make_async_copy(ref, ref, sem).wait()

    def signal(sem, device):
        pl.semaphore_signal(sem, 1, device_id=device, device_id_type=MESH_ID)

    def part(q):
        return pl.ds(offs[q], lens[q])

    def cols(q):
        return pl.ds(q * width, width)

    main, other = range(CHUNKS - OTHER), range(CHUNKS - OTHER, CHUNKS)
    main_part, main_cols = pl.ds(0, META + len(main) * width), pl.ds(0, len(main) * width)
    other_part = pl.ds(META + len(main) * width, OTHER * width)
    ring_order = list(main[:1]) + [q for pair in zip(other, main[1:]) for q in pair] + list(main[1 + OTHER :])
    back_order = list(other) + list(main)

    def own(q):
        return pl.ds((q - len(main)) * width, width)

    barrier = pltpu.get_barrier_semaphore()
    with scope("entry"):
        signal(barrier, partner)
        for v in ys:
            signal(barrier, at_y(v, 1))
            signal(barrier, at_y(v, 0))
        for v in xs:
            signal(barrier, at_x(v, 0))
            signal(barrier, at_x(v, 1))

        @pl.when(lead)
        def _():
            signal(barrier, up)
            signal(barrier, down)

        @pl.when(early)
        def _():
            signal(barrier, across(0))

            @pl.when(jnp.logical_not(lead))
            def _():
                signal(barrier, across(1))

        inputs = [
            pltpu.make_async_copy(tok_ref, tokv, in_sem.at[0]),
            pltpu.make_async_copy(ids_ref, idsv, in_sem.at[1]),
            pltpu.make_async_copy(gates_ref, gatesv, in_sem.at[2]),
        ]
        for copy in inputs:
            copy.start()
        for h in range(2):
            wcols = pl.ds(h * half, half)
            pltpu.make_async_copy(wg_ref.at[:, :, wcols], wgu.at[h, 0, 0], wl_sem.at[0]).start()
            pltpu.make_async_copy(wu_ref.at[:, :, wcols], wgu.at[h, 1, 0], wl_sem.at[0]).start()
            pltpu.make_async_copy(wd_ref.at[:, :, wcols], wdn.at[h, 0], wl_sem.at[1]).start()

        for copy in inputs:
            copy.wait()
        lane = lax.broadcasted_iota(jnp.int32, (2, META), 1)
        row = lax.broadcasted_iota(jnp.int32, (2, META), 0)
        gates = jnp.zeros((2, META), jnp.int32)
        for k in range(ids_ref.shape[1]):
            gates += jnp.where((lane == idsv[0, k]) & (row == 0), gatesv[0, k], 0)
        tsend[:, 0:META] = gates.astype(F32).astype(BF16)
        tok = tokv[...].astype(F32)
        tsend[:, META:] = jnp.concatenate([tok[:, :half], tok[:, half:]], axis=0).astype(BF16)

        @pl.when(lead)
        def _():
            t1[y * 2 + 1] = tsend[...]
            a1[x * 2 + 1] = tsend[:, other_part]

        @pl.when(jnp.logical_not(lead))
        def _():
            ftok[0] = tsend[...]

    with scope("bar"):
        count = 1 + 2 * (ny - 1) + 2 * (nx - 1) + 2 * c + (z // hz) * (2 - c)
        pl.semaphore_wait(barrier, count)

        @pl.when(jnp.logical_not(early))
        def _():
            signal(ready, across(0))

    with scope("ypush"):
        for q in other:
            for v in xs:
                push(tsend.at[:, part(q)], a1.at[x * 2 + c, :, own(q)], so.at[0], r1.at[q], at_x(v))

            @pl.when(jnp.logical_not(lead))
            def _():
                push(tsend.at[:, part(q)], a1.at[x * 2 + c, :, own(q)], s0, r1.at[q], partner)

        for q in main:
            for v in ys:
                push(tsend.at[:, part(q)], t1.at[y * 2 + c, :, part(q)], s1, r1.at[q], at_y(v, 1))

            @pl.when(jnp.logical_not(lead))
            def _():
                push(tsend.at[:, part(q)], t1.at[y * 2 + c, :, part(q)], s0, r1.at[q], partner)

        @pl.when(lead)
        def _():
            push(tsend, ftok.at[1], fs.at[0], fr.at[6], partner)

        for h in range(2):
            wcols = pl.ds(h * half, half)
            push(wg_ref.at[:, :, wcols], wgu.at[h, 0, 1], ws_sem.at[0], wr_sem.at[0], partner)
            push(wu_ref.at[:, :, wcols], wgu.at[h, 1, 1], ws_sem.at[0], wr_sem.at[0], partner)
            push(wd_ref.at[:, :, wcols], wdn.at[h, 1], ws_sem.at[1], wr_sem.at[1], partner)

    cells = nx * ny * 2

    def order(i):
        return ((i // 2) % ny) * nx + i // (2 * ny)

    def picker(field, col, side):
        i0 = lax.broadcasted_iota(jnp.int32, (cells, cells), 0)
        i1 = lax.broadcasted_iota(jnp.int32, (cells, cells), 1)
        same = ones(i0 // 2 == i1 // 2)
        own = ones(lax.broadcasted_iota(jnp.int32, (rows, META), 1) // 2 == n)
        meta = field[:, col, :, 0:META].reshape(cells, META)
        if side == 0:
            total = lax.dot_general(own, meta, NT, preferred_element_type=F32)
            hit = ones(total > 0)
            rank = jnp.dot(hit, ones(order(i0) < order(i1)), preferred_element_type=F32)
            hit = jnp.dot(hit, same, preferred_element_type=F32)
            shape = (rows, cells)
        else:
            total = lax.dot_general(meta, own, NT, preferred_element_type=F32)
            hit = ones(total > 0)
            rank = jnp.dot(ones(order(i1) < order(i0)), hit, preferred_element_type=F32)
            hit = jnp.dot(same, hit, preferred_element_type=F32)
            shape = (cells, rows)
        r = lax.broadcasted_iota(jnp.int32, shape, side)
        i = lax.broadcasted_iota(jnp.int32, shape, 1 - side)
        return ones((hit > 0) & (rank == (r // 2).astype(F32)) & (r % 2 == i % 2))

    def weights_here():
        await_bytes(wgu.at[:, :, 0], wl_sem.at[0])
        await_bytes(wdn.at[:, 0], wl_sem.at[1])
        await_bytes(wgu.at[:, :, 1], wr_sem.at[0])
        await_bytes(wdn.at[:, 1], wr_sem.at[1])

    def gate_up(start, blocks, q):
        count = blocks * 2 * rows
        piece = xbuf[start : start + blocks, :, :, pl.ds(d_off[q], width)].reshape(count, width)
        for h in range(2):
            w = wgu[h, :, :, :, :, cols(q)].reshape(2 * units, width)
            v = lax.dot_general(piece, w, NT, preferred_element_type=F32)
            for k in range(2):
                if q == 0:
                    zbuf[h, k, 0:count] = v[:, k * units : (k + 1) * units]
                else:
                    zbuf[h, k, 0:count] += v[:, k * units : (k + 1) * units]

    def activations(start, blocks):
        count = blocks * 2 * rows
        lane = lax.broadcasted_iota(jnp.int32, (META, units), 0)
        unit = lax.broadcasted_iota(jnp.int32, (META, units), 1)
        chosen = ones(lane == 2 * n + (unit // ffl) % 2)
        gate_rows = xbuf[start : start + blocks, :, :, 0:META].reshape(count, META)
        hbuf[0, 0:count] = jnp.dot(gate_rows, chosen, preferred_element_type=F32)
        even, odd = pl.ds(0, count // 2, 2), pl.ds(1, count // 2, 2)
        gate_act = zbuf[0, 0, even, :] + zbuf[1, 0, odd, :]
        up_act = zbuf[0, 1, even, :] + zbuf[1, 1, odd, :]
        scale = hbuf[0, even, :] / 8.0
        hidden = gate_act / (1.0 + jnp.exp(-gate_act)) * up_act * scale
        none = jnp.zeros_like(hidden)
        hbuf[0, even, :] = hidden
        hbuf[1, even, :] = none
        hbuf[0, odd, :] = none
        hbuf[1, odd, :] = hidden
        return jnp.concatenate([hbuf[0, 0:count], hbuf[1, 0:count]], axis=1).astype(BF16)

    def project(hidden, q):
        w = wdn[:, :, :, :, cols(q)].reshape(2 * units, width)
        return jnp.dot(hidden, w, preferred_element_type=F32)

    def arrival(k):
        return k % 4

    def slot(direction, step):
        return direction * steps + step - 1

    @pl.when(jnp.logical_not(lead))
    def _():
        with scope("f_token"):
            @pl.when(early)
            def _():
                pl.semaphore_wait(ready, 2)

            await_bytes(ftok.at[1], fr.at[6])
            push(ftok, ft1.at[y], fs.at[0], fr.at[0], across(0))
        with scope("f_y"):
            await_bytes(ft1.at[y], fr.at[0])
            for v in ys:
                push(ft1.at[y], ft1.at[y], fs.at[1], fr.at[1], at_y(v, 0))
        with scope("f_x"):
            await_bytes(ft1.at[0 : ny - 1], fr.at[1])
            for v in range(ny):
                for col in range(2):
                    ft2[x, col, 2 * v : 2 * v + 2] = ft1[v, col]
            for v in xs:
                push(ft2.at[x], ft2.at[x], fs.at[2], fr.at[2], at_x(v, 0))
        with scope("s_wait"):
            weights_here()
        for batch, (start, blocks) in enumerate(((0, near - 2), (near - 2, 2))):
            with scope(f"s_wait{batch}"):
                await_bytes(xbuf.at[start : start + blocks], rx.at[batch])
            with scope(f"s_comp{batch}"):
                for q in range(CHUNKS):
                    gate_up(start, blocks, q)
                hidden = activations(start, blocks)
                for q in range(CHUNKS):
                    v = project(hidden, q).astype(BF16).reshape(blocks, 2, rows, width)
                    pnear[start : start + blocks, :, :, cols(q)] = v
        for b in range(near - 1, -1, -1):
            push(pnear.at[b], pnear.at[b], sp, rp.at[(b + 1) // 2], partner)
        with scope("f_pack"):
            await_bytes(ft2.at[0 : nx - 1], fr.at[2])
            pickers = [picker(ft2, col, 0) for col in range(2)]
            for col in range(2):
                for q in range(CHUNKS):
                    field = ft2[:, col, :, part(q)].reshape(cells, lens[q])
                    picked = jnp.dot(pickers[col], field, preferred_element_type=F32)
                    xbuf[opposite, col, :, part(q)] = picked.astype(BF16)
            for q in range(CHUNKS):
                gate_up(opposite, 1, q)
            hidden = activations(opposite, 1)
        with scope("f_retx"):
            pickers = [picker(ft2, col, 1) for col in range(2)]
            for q in range(CHUNKS):
                v = project(hidden, q).astype(BF16).reshape(2, rows, width)
                for col in range(2):
                    placed = jnp.dot(pickers[col], v[col], preferred_element_type=F32)
                    fxs[:, col, :, cols(q)] = placed.astype(BF16).reshape(nx, 2 * ny, width)
            for v in xs:
                push(fxs.at[v], fxr.at[x], fs.at[3], fr.at[3], at_x(v, 0))
        with scope("f_rety"):
            await_bytes(fxr.at[0 : nx - 1], fr.at[3])
            for q in range(CHUNKS):
                total = fxs[x, :, :, cols(q)].astype(F32)
                for v in xs:
                    total += fxr[v, :, :, cols(q)].astype(F32)
                total = total.astype(BF16)
                for v in range(ny):
                    for col in range(2):
                        fys[v, col, :, cols(q)] = total[col, 2 * v : 2 * v + 2, :]
            for v in ys:
                push(fys.at[v], fyr.at[y], fs.at[4], fr.at[4], at_y(v, 0))
        with scope("f_retz"):
            await_bytes(fyr.at[0 : ny - 1], fr.at[4])
            for q in range(CHUNKS):
                total = fys[y, :, :, cols(q)].astype(F32)
                for v in ys:
                    total += fyr[v, :, :, cols(q)].astype(F32)
                fzs[:, :, cols(q)] = total.astype(BF16)
            for core in range(2):
                push(fzs.at[core], fin, fs.at[5], fr.at[5], across(core))

    def hop(s, q):
        for direction, b, later, device in (
            (0, going_up(s), going_up(s + 1), up),
            (1, going_down(s), going_down(s + 1), down),
        ):
            block = xbuf.at[b, :, :, part(q)]
            await_bytes(block, ra.at[arrival(s), direction, q])
            if s < steps:
                push(block, xbuf.at[later, :, :, part(q)], sa, ra.at[arrival(s + 1), direction, q], device)
                push(block, block, sx, rx.at[1 if s == steps - 1 else 0], partner)

    @pl.when(lead)
    def _():
        with scope("xstage"):
            for q in other:
                await_bytes(a1.at[0 : 2 * nx - 1, :, own(q)], r1.at[q])
                for v in ys:
                    push(a1.at[:, :, own(q)], b1.at[y, :, :, own(q)], so.at[1], r2.at[q], at_y(v, 1))
                b1[y, :, :, own(q)] = a1[:, :, own(q)]
            for q in main:
                await_bytes(t1.at[0 : 2 * ny - 1, :, part(q)], r1.at[q])
                for v in range(ny):
                    for col in range(2):
                        t2[x, col, 2 * v : 2 * v + 2, part(q)] = t1[2 * v + col, :, part(q)]
                for v in xs:
                    block = t2.at[x, :, :, part(q)]
                    push(block, block, s2, r2.at[q], at_x(v))

        with scope("pack"):
            pickers = None
            for q in ring_order:
                if q in main:
                    await_bytes(t2.at[0 : nx - 1, :, :, part(q)], r2.at[q])
                else:
                    await_bytes(b1.at[0 : ny - 1, :, :, own(q)], r2.at[q])
                    for v in range(ny):
                        for j in range(2 * nx):
                            t2[j // 2, j % 2, 2 * v : 2 * v + 2, part(q)] = b1[v, j, :, own(q)]
                if q == 0:
                    pickers = [picker(t2, col, 0) for col in range(2)]
                for col in range(2):
                    field = t2[:, col, :, part(q)].reshape(cells, lens[q])
                    picked = jnp.dot(pickers[col], field, preferred_element_type=F32)
                    xbuf[0, col, :, part(q)] = picked.astype(BF16)
                block = xbuf.at[0, :, :, part(q)]
                push(block, xbuf.at[going_up(1), :, :, part(q)], sa, ra.at[arrival(1), 0, q], up)
                push(block, xbuf.at[going_down(1), :, :, part(q)], sa, ra.at[arrival(1), 1, q], down)
                push(block, block, sx, rx.at[0], partner)
            weights_here()

        with scope("ring"):
            for s in range(1, steps + 1):
                for q in ring_order:
                    hop(s, q)
                    if s == steps:
                        gate_up(near, 2, q)
        with scope("act"):
            hidden = activations(near, 2)

        def onward(direction, s, q, value, device):
            i = slot(direction, s)
            if s > 1:
                await_bytes(rrecv.at[i - 1, :, :, cols(q)], ra.at[arrival(steps + s - 1), direction, q])
                value = value + rrecv[i - 1, :, :, cols(q)]
            rsend[i, :, :, cols(q)] = value
            push(rsend.at[i, :, :, cols(q)], rrecv.at[i, :, :, cols(q)], ss, ra.at[arrival(steps + s), direction, q], device)

        with scope("rs1"):
            for q in back_order:
                v = project(hidden, q).astype(BF16).reshape(2, 2, rows, width)
                onward(0, 1, q, v[1], up)
                onward(1, 1, q, v[0], down)
        with scope("rs"):
            pickers = [picker(t2, col, 1) for col in range(2)]
            for s in range(2, steps + 1):
                at = steps + 1 - s
                await_bytes(pnear.at[0:2], rp.at[at])
                for q in back_order:
                    onward(0, s, q, pnear[going_down(at), :, :, cols(q)], up)
                    onward(1, s, q, pnear[going_up(at), :, :, cols(q)], down)

        with scope("retx"):
            await_bytes(pnear.at[0], rp.at[0])
            for q in back_order:
                one, two = slot(0, steps), slot(1, steps)
                await_bytes(rrecv.at[two, :, :, cols(q)], ra.at[arrival(2 * steps), 1, q])
                await_bytes(rrecv.at[one, :, :, cols(q)], ra.at[arrival(2 * steps), 0, q])
                total = pnear[0, :, :, cols(q)].astype(F32) + rrecv[one, :, :, cols(q)].astype(F32)
                total = (total + rrecv[two, :, :, cols(q)].astype(F32)).astype(BF16)
                for col in range(2):
                    placed = jnp.dot(pickers[col], total[col], preferred_element_type=F32).astype(BF16)
                    if q in main:
                        ysend[:, col, :, cols(q)] = placed.reshape(nx, 2 * ny, width)
                    else:
                        for i in range(nx * ny):
                            c1[i % ny, 2 * (i // ny) + col, :, own(q)] = placed[2 * i : 2 * i + 2, :]
                if q in main:
                    for v in xs:
                        push(ysend.at[v, :, :, cols(q)], yrecv.at[x, :, :, cols(q)], s3, r3.at[q], at_x(v))
                else:
                    for v in ys:
                        push(c1.at[v, :, :, own(q)], c2.at[y, :, :, own(q)], so.at[2], r3.at[q], at_y(v, 1))
        with scope("rety"):
            for q in main:
                await_bytes(yrecv.at[0 : nx - 1, :, :, cols(q)], r3.at[q])
                total = ysend[x, :, :, cols(q)].astype(F32)
                for v in xs:
                    total += yrecv[v, :, :, cols(q)].astype(F32)
                total = total.astype(BF16)
                for v in range(ny):
                    for col in range(2):
                        fsend[v, col, :, cols(q)] = total[col, 2 * v : 2 * v + 2, :]
                for v in ys:
                    for col in range(2):
                        push(fsend.at[v, col, :, cols(q)], frecv.at[y, :, cols(q)], s4, r4.at[q], at_y(v, col))
                push(fsend.at[y, 0, :, cols(q)], frecv.at[y, :, cols(q)], s0, r4.at[q], partner)
                frecv[y, :, cols(q)] = fsend[y, 1, :, cols(q)]
            for q in other:
                await_bytes(c2.at[0 : ny - 1, :, :, own(q)], r3.at[q])
                total = c1[y, :, :, own(q)].astype(F32)
                for v in ys:
                    total += c2[v, :, :, own(q)].astype(F32)
                e1[:, :, own(q)] = total.astype(BF16)
                for v in xs:
                    for col in range(2):
                        push(e1.at[2 * v + col, :, own(q)], e2.at[x, :, own(q)], so.at[3], r4.at[q], at_x(v, col))
                push(e1.at[2 * x, :, own(q)], e2.at[x, :, own(q)], so.at[4], r4.at[q], partner)
                e2[x, :, own(q)] = e1[2 * x + 1, :, own(q)]

    with scope("final"):
        await_bytes(fin, fr.at[5])
        for q in range(CHUNKS):
            parts, mine, count = (frecv, cols(q), ny) if q in main else (e2, own(q), nx)

            @pl.when(lead)
            def _():
                await_bytes(parts.at[0 : count - 1, :, mine], r4.at[q])

            @pl.when(jnp.logical_not(lead))
            def _():
                await_bytes(parts.at[:, :, mine], r4.at[q])

            total = fin[:, cols(q)].astype(F32)
            for v in range(count):
                total += parts[v, :, mine].astype(F32)
            total = total.astype(BF16)
            out_ref[0:1, cols(q)] = total[0:1, :]
            out_ref[0:1, pl.ds(half + q * width, width)] = total[1:2, :]

    with scope("drain"):
        await_bytes(t1.at[0 : ny - 1, :, main_part], s1)
        await_bytes(a1.at[0 : nx - 1], so.at[0])
        await_bytes(wgu.at[:, :, 1], ws_sem.at[0])
        await_bytes(wdn.at[:, 1], ws_sem.at[1])

        @pl.when(jnp.logical_not(lead))
        def _():
            await_bytes(tsend, s0)
            await_bytes(pnear, sp)
            await_bytes(ftok, fs.at[0])
            await_bytes(ft1.at[0 : ny - 1], fs.at[1])
            await_bytes(ft2.at[0 : nx - 1], fs.at[2])
            await_bytes(fxs.at[0 : nx - 1], fs.at[3])
            await_bytes(fys.at[0 : ny - 1], fs.at[4])
            await_bytes(fzs, fs.at[5])

        @pl.when(lead)
        def _():
            await_bytes(t2.at[0 : nx - 1, :, :, main_part], s2)
            await_bytes(b1.at[0 : ny - 1], so.at[1])
            await_bytes(c2.at[0 : ny - 1], so.at[2])
            await_bytes(e1.at[0 : 2 * (nx - 1)], so.at[3])
            await_bytes(e1.at[0], so.at[4])
            await_bytes(xbuf.at[0 : 2 * steps], sa)
            await_bytes(xbuf.at[0:near], sx)
            await_bytes(rsend, ss)
            await_bytes(yrecv.at[0 : nx - 1, :, :, main_cols], s3)
            await_bytes(fsend.at[0 : ny - 1, :, :, main_cols], s4)
            await_bytes(frecv.at[0, :, main_cols], s0)
            await_bytes(tsend, fs.at[0])


def solution(mesh):
    nodes, locals_ = mesh.shape["node"], mesh.shape["local"]
    nx = min(NX, nodes)
    ny, nz = nodes // nx, locals_ // 2
    hz = nz // 2
    steps = hz - 1
    near = 2 * steps - 1

    def on_device(tokens, w_gate, w_up, w_down, expert_ids, gate_ints):
        model_width = tokens.shape[1]
        half = model_width // 2
        exp_node, ffl = w_gate.shape[0], w_gate.shape[1]
        units = 2 * exp_node * ffl
        rows = 2 * CAP
        lanes = OTHER * (half // CHUNKS)
        sem = pltpu.SemaphoreType.DMA
        one = sem(())
        any_space = pl.BlockSpec(memory_space=pl.ANY)
        vmem = pl.BlockSpec(memory_space=pltpu.VMEM)
        return pl.pallas_call(
            functools.partial(layer_kernel, nx, ny, nz),
            out_shape=jax.ShapeDtypeStruct((1, model_width), BF16),
            in_specs=[any_space] * 6,
            out_specs=vmem,
            scratch_shapes=[
                pltpu.VMEM((1, model_width), BF16),
                pltpu.SMEM(expert_ids.shape, jnp.int32),
                pltpu.SMEM(gate_ints.shape, jnp.int32),
                pltpu.VMEM((2, META + half), BF16),
                pltpu.VMEM((2 * ny, 2, META + half), BF16),
                pltpu.VMEM((nx, 2, 2 * ny, META + half), BF16),
                pltpu.VMEM((nz, 2, rows, META + half), BF16),
                pltpu.VMEM((2, 2, 2, exp_node, ffl, half), BF16),
                pltpu.VMEM((2, 2, exp_node, ffl, half), BF16),
                pltpu.VMEM((2, 2, near * 2 * rows, units), F32),
                pltpu.VMEM((2, near * 2 * rows, units), F32),
                pltpu.VMEM((near, 2, rows, half), BF16),
                pltpu.VMEM((2 * steps, 2, rows, half), BF16),
                pltpu.VMEM((2 * steps, 2, rows, half), BF16),
                pltpu.VMEM((nx, 2, 2 * ny, half), BF16),
                pltpu.VMEM((nx, 2, 2 * ny, half), BF16),
                pltpu.VMEM((ny, 2, 2, half), BF16),
                pltpu.VMEM((ny, 2, half), BF16),
                pltpu.VMEM((2, 2, META + half), BF16),
                pltpu.VMEM((ny, 2, 2, META + half), BF16),
                pltpu.VMEM((nx, 2, 2 * ny, META + half), BF16),
                pltpu.VMEM((nx, 2, 2 * ny, half), BF16),
                pltpu.VMEM((nx, 2, 2 * ny, half), BF16),
                pltpu.VMEM((ny, 2, 2, half), BF16),
                pltpu.VMEM((ny, 2, 2, half), BF16),
                pltpu.VMEM((2, 2, half), BF16),
                pltpu.VMEM((2, half), BF16),
                pltpu.VMEM((2 * nx, 2, lanes), BF16),
                pltpu.VMEM((ny, 2 * nx, 2, lanes), BF16),
                pltpu.VMEM((ny, 2 * nx, 2, lanes), BF16),
                pltpu.VMEM((ny, 2 * nx, 2, lanes), BF16),
                pltpu.VMEM((2 * nx, 2, lanes), BF16),
                pltpu.VMEM((nx, 2, lanes), BF16),
                sem((3,)), sem((2,)), sem((2,)), sem((2,)),
                one, one, sem((CHUNKS,)), one, sem((CHUNKS,)),
                one, sem((4, 2, CHUNKS)), one, sem((2,)), one, sem((steps,)),
                one, one, sem((CHUNKS,)), one, sem((CHUNKS,)),
                sem((6,)), sem((7,)), pltpu.SemaphoreType.REGULAR, sem((5,)),
            ],
            compiler_params=pltpu.CompilerParams(
                collective_id=0, has_side_effects=True, vmem_limit_bytes=60 * 1024 * 1024
            ),
            name="layer",
        )(tokens, w_gate, w_up, w_down, expert_ids, gate_ints)

    both = P(("node", "local"), None)
    weights = P("node", "local", None)
    return jax.shard_map(
        on_device, mesh=mesh,
        in_specs=(both, weights, weights, weights, both, both),
        out_specs=both, check_vma=False,
    )
```

```python
import functools

import jax
import jax.numpy as jnp
from jax import lax
from jax.experimental import pallas as pl
from jax.experimental.pallas import tpu as pltpu
from jax.sharding import PartitionSpec as P

CAP = 8
NX = 4
CHUNKS = 7
OTHER = 2
META = 128
BF16 = jnp.bfloat16
F32 = jnp.float32
MESH_ID = pl.DeviceIdType.MESH
NT = (((1,), (1,)), ((), ()))
scope = jax.named_scope


def ones(mask):
    return mask.astype(F32).astype(BF16)


def layer_kernel(
    nx, ny, nz,
    tok_ref, wg_ref, wu_ref, wd_ref, ids_ref, gates_ref,
    out_ref,
    tokv, idsv, gatesv, tsend, t1, t2, xbuf, wgu, wdn, zbuf, hbuf, pnear, rsend, rrecv,
    ysend, yrecv, fsend, frecv, ftok, ft1, ft2, fxs, fxr, fys, fyr, fzs, fin, a1, b1, c1, c2, e1, e2,
    in_sem, wl_sem, ws_sem, wr_sem, s0, s1, r1, s2, r2, sa, ra, sx, rx, sp, rp, ss, s3, r3, s4, r4,
    fs, fr, ready, so, outv, out_sem,
):
    half = wgu.shape[-1]
    width = half // CHUNKS
    offs = [0] + [META + q * width for q in range(1, CHUNKS)]
    lens = [META + width] + [width] * (CHUNKS - 1)
    d_off = [META + q * width for q in range(CHUNKS)]
    hz = nz // 2
    rows = CAP * 2
    ffl = wdn.shape[3]
    units = wdn.shape[1] * wdn.shape[2] * ffl
    n = lax.axis_index("node")
    l = lax.axis_index("local")
    x, y = lax.rem(n, nx), n // nx
    z, c = l // 2, lax.rem(l, 2)
    lead = c == 1

    def at_x(v, core=1):
        return (y * nx + v, z * 2 + core)

    def at_y(v, core):
        return (v * nx + x, z * 2 + core)

    up = (n, lax.rem(z + 1, nz) * 2 + 1)
    down = (n, lax.rem(z + nz - 1, nz) * 2 + 1)
    partner = (n, z * 2 + 1 - c)
    xs = [lax.rem(x + d, nx) for d in sorted(range(1, nx), key=lambda d: -min(d, nx - d))]
    ys = [lax.rem(y + d, ny) for d in sorted(range(1, ny), key=lambda d: -min(d, ny - d))]

    steps = hz - 1
    near = 2 * steps - 1
    opposite = near + 2

    def going_up(s):
        return 2 * s - 1

    def going_down(s):
        return 2 * s

    early = z < hz

    def across(core):
        return (n, lax.rem(z + hz, nz) * 2 + core)

    def push(src, dst, send, recv, device):
        pltpu.make_async_remote_copy(
            src_ref=src, dst_ref=dst, send_sem=send, recv_sem=recv,
            device_id=device, device_id_type=MESH_ID,
        ).start()

    def await_bytes(ref, sem):
        pltpu.make_async_copy(ref, ref, sem).wait()

    def signal(sem, device):
        pl.semaphore_signal(sem, 1, device_id=device, device_id_type=MESH_ID)

    def part(q):
        return pl.ds(offs[q], lens[q])

    def cols(q):
        return pl.ds(q * width, width)

    main, other = range(CHUNKS - OTHER), range(CHUNKS - OTHER, CHUNKS)
    main_part, main_cols = pl.ds(0, META + len(main) * width), pl.ds(0, len(main) * width)
    other_part = pl.ds(META + len(main) * width, OTHER * width)
    ring_order = list(main[:1]) + [q for pair in zip(other, main[1:]) for q in pair] + list(main[1 + OTHER :])
    back_order = list(other) + list(main)

    def own(q):
        return pl.ds((q - len(main)) * width, width)

    barrier = pltpu.get_barrier_semaphore()
    with scope("entry"):
        signal(barrier, partner)
        for v in ys:
            signal(barrier, at_y(v, 1))
            signal(barrier, at_y(v, 0))
        for v in xs:
            signal(barrier, at_x(v, 0))
            signal(barrier, at_x(v, 1))

        @pl.when(lead)
        def _():
            signal(barrier, up)
            signal(barrier, down)

        @pl.when(early)
        def _():
            signal(barrier, across(0))

            @pl.when(jnp.logical_not(lead))
            def _():
                signal(barrier, across(1))

        inputs = [
            pltpu.make_async_copy(tok_ref, tokv, in_sem.at[0]),
            pltpu.make_async_copy(ids_ref, idsv, in_sem.at[1]),
            pltpu.make_async_copy(gates_ref, gatesv, in_sem.at[2]),
        ]
        for copy in inputs:
            copy.start()
        for h in range(2):
            wcols = pl.ds(h * half, half)
            pltpu.make_async_copy(wg_ref.at[:, :, wcols], wgu.at[h, 0, 0], wl_sem.at[0]).start()
            pltpu.make_async_copy(wu_ref.at[:, :, wcols], wgu.at[h, 1, 0], wl_sem.at[0]).start()
            pltpu.make_async_copy(wd_ref.at[:, :, wcols], wdn.at[h, 0], wl_sem.at[1]).start()

        for copy in inputs:
            copy.wait()
        lane = lax.broadcasted_iota(jnp.int32, (2, META), 1)
        row = lax.broadcasted_iota(jnp.int32, (2, META), 0)
        gates = jnp.zeros((2, META), jnp.int32)
        for k in range(ids_ref.shape[1]):
            gates += jnp.where((lane == idsv[0, k]) & (row == 0), gatesv[0, k], 0)
        tsend[:, 0:META] = gates.astype(F32).astype(BF16)
        tok = tokv[...].astype(F32)
        tsend[:, META:] = jnp.concatenate([tok[:, :half], tok[:, half:]], axis=0).astype(BF16)

        @pl.when(lead)
        def _():
            t1[y * 2 + 1] = tsend[...]
            a1[x * 2 + 1] = tsend[:, other_part]

        @pl.when(jnp.logical_not(lead))
        def _():
            ftok[0] = tsend[...]

    with scope("bar"):
        count = 1 + 2 * (ny - 1) + 2 * (nx - 1) + 2 * c + (z // hz) * (2 - c)
        pl.semaphore_wait(barrier, count)

        @pl.when(jnp.logical_not(early))
        def _():
            signal(ready, across(0))

    with scope("ypush"):
        for q in other:
            for v in xs:
                push(tsend.at[:, part(q)], a1.at[x * 2 + c, :, own(q)], so.at[0], r1.at[q], at_x(v))

            @pl.when(jnp.logical_not(lead))
            def _():
                push(tsend.at[:, part(q)], a1.at[x * 2 + c, :, own(q)], s0, r1.at[q], partner)

        for q in main:
            for v in ys:
                push(tsend.at[:, part(q)], t1.at[y * 2 + c, :, part(q)], s1, r1.at[q], at_y(v, 1))

            @pl.when(jnp.logical_not(lead))
            def _():
                push(tsend.at[:, part(q)], t1.at[y * 2 + c, :, part(q)], s0, r1.at[q], partner)

        @pl.when(lead)
        def _():
            push(tsend, ftok.at[1], fs.at[0], fr.at[6], partner)

        for h in range(2):
            wcols = pl.ds(h * half, half)
            push(wg_ref.at[:, :, wcols], wgu.at[h, 0, 1], ws_sem.at[0], wr_sem.at[0], partner)
            push(wu_ref.at[:, :, wcols], wgu.at[h, 1, 1], ws_sem.at[0], wr_sem.at[0], partner)
            push(wd_ref.at[:, :, wcols], wdn.at[h, 1], ws_sem.at[1], wr_sem.at[1], partner)

    cells = nx * ny * 2

    def order(i):
        return ((i // 2) % ny) * nx + i // (2 * ny)

    def picker(field, col, side):
        i0 = lax.broadcasted_iota(jnp.int32, (cells, cells), 0)
        i1 = lax.broadcasted_iota(jnp.int32, (cells, cells), 1)
        same = ones(i0 // 2 == i1 // 2)
        own = ones(lax.broadcasted_iota(jnp.int32, (rows, META), 1) // 2 == n)
        meta = field[:, col, :, 0:META].reshape(cells, META)
        if side == 0:
            total = lax.dot_general(own, meta, NT, preferred_element_type=F32)
            hit = ones(total > 0)
            rank = jnp.dot(hit, ones(order(i0) < order(i1)), preferred_element_type=F32)
            hit = jnp.dot(hit, same, preferred_element_type=F32)
            shape = (rows, cells)
        else:
            total = lax.dot_general(meta, own, NT, preferred_element_type=F32)
            hit = ones(total > 0)
            rank = jnp.dot(ones(order(i1) < order(i0)), hit, preferred_element_type=F32)
            hit = jnp.dot(same, hit, preferred_element_type=F32)
            shape = (cells, rows)
        r = lax.broadcasted_iota(jnp.int32, shape, side)
        i = lax.broadcasted_iota(jnp.int32, shape, 1 - side)
        return ones((hit > 0) & (rank == (r // 2).astype(F32)) & (r % 2 == i % 2))

    def weights_here():
        await_bytes(wgu.at[:, :, 0], wl_sem.at[0])
        await_bytes(wdn.at[:, 0], wl_sem.at[1])
        await_bytes(wgu.at[:, :, 1], wr_sem.at[0])
        await_bytes(wdn.at[:, 1], wr_sem.at[1])

    def gate_up(start, blocks, q):
        count = blocks * 2 * rows
        piece = xbuf[start : start + blocks, :, :, pl.ds(d_off[q], width)].reshape(count, width)
        for h in range(2):
            w = wgu[h, :, :, :, :, cols(q)].reshape(2 * units, width)
            v = lax.dot_general(piece, w, NT, preferred_element_type=F32)
            for k in range(2):
                if q == 0:
                    zbuf[h, k, 0:count] = v[:, k * units : (k + 1) * units]
                else:
                    zbuf[h, k, 0:count] += v[:, k * units : (k + 1) * units]

    def activations(start, blocks):
        count = blocks * 2 * rows
        lane = lax.broadcasted_iota(jnp.int32, (META, units), 0)
        unit = lax.broadcasted_iota(jnp.int32, (META, units), 1)
        chosen = ones(lane == 2 * n + (unit // ffl) % 2)
        gate_rows = xbuf[start : start + blocks, :, :, 0:META].reshape(count, META)
        hbuf[0, 0:count] = jnp.dot(gate_rows, chosen, preferred_element_type=F32)
        even, odd = pl.ds(0, count // 2, 2), pl.ds(1, count // 2, 2)
        gate_act = zbuf[0, 0, even, :] + zbuf[1, 0, odd, :]
        up_act = zbuf[0, 1, even, :] + zbuf[1, 1, odd, :]
        scale = hbuf[0, even, :] / 8.0
        hidden = gate_act / (1.0 + jnp.exp(-gate_act)) * up_act * scale
        none = jnp.zeros_like(hidden)
        hbuf[0, even, :] = hidden
        hbuf[1, even, :] = none
        hbuf[0, odd, :] = none
        hbuf[1, odd, :] = hidden
        return jnp.concatenate([hbuf[0, 0:count], hbuf[1, 0:count]], axis=1).astype(BF16)

    def project(hidden, q):
        w = wdn[:, :, :, :, cols(q)].reshape(2 * units, width)
        return jnp.dot(hidden, w, preferred_element_type=F32)

    def arrival(k):
        return k % 4

    def slot(direction, step):
        return direction * steps + step - 1

    @pl.when(jnp.logical_not(lead))
    def _():
        with scope("f_token"):
            @pl.when(early)
            def _():
                pl.semaphore_wait(ready, 2)

            await_bytes(ftok.at[1], fr.at[6])
            push(ftok, ft1.at[y], fs.at[0], fr.at[0], across(0))
        with scope("f_y"):
            await_bytes(ft1.at[y], fr.at[0])
            for v in ys:
                push(ft1.at[y], ft1.at[y], fs.at[1], fr.at[1], at_y(v, 0))
        with scope("f_x"):
            await_bytes(ft1.at[0 : ny - 1], fr.at[1])
            for v in range(ny):
                for col in range(2):
                    ft2[x, col, 2 * v : 2 * v + 2] = ft1[v, col]
            for v in xs:
                push(ft2.at[x], ft2.at[x], fs.at[2], fr.at[2], at_x(v, 0))
        with scope("s_wait"):
            weights_here()
        for batch, (start, blocks) in enumerate(((0, near - 2), (near - 2, 2))):
            with scope(f"s_wait{batch}"):
                await_bytes(xbuf.at[start : start + blocks], rx.at[batch])
            with scope(f"s_comp{batch}"):
                for q in range(CHUNKS):
                    gate_up(start, blocks, q)
                hidden = activations(start, blocks)
                for q in range(CHUNKS):
                    v = project(hidden, q).astype(BF16).reshape(blocks, 2, rows, width)
                    pnear[start : start + blocks, :, :, cols(q)] = v
        for b in range(near - 1, -1, -1):
            push(pnear.at[b], pnear.at[b], sp, rp.at[(b + 1) // 2], partner)
        with scope("f_pack"):
            await_bytes(ft2.at[0 : nx - 1], fr.at[2])
            pickers = [picker(ft2, col, 0) for col in range(2)]
            for col in range(2):
                for q in range(CHUNKS):
                    field = ft2[:, col, :, part(q)].reshape(cells, lens[q])
                    picked = jnp.dot(pickers[col], field, preferred_element_type=F32)
                    xbuf[opposite, col, :, part(q)] = picked.astype(BF16)
            for q in range(CHUNKS):
                gate_up(opposite, 1, q)
            hidden = activations(opposite, 1)
        with scope("f_retx"):
            pickers = [picker(ft2, col, 1) for col in range(2)]
            for q in range(CHUNKS):
                v = project(hidden, q).astype(BF16).reshape(2, rows, width)
                for col in range(2):
                    placed = jnp.dot(pickers[col], v[col], preferred_element_type=F32)
                    fxs[:, col, :, cols(q)] = placed.astype(BF16).reshape(nx, 2 * ny, width)
            for v in xs:
                push(fxs.at[v], fxr.at[x], fs.at[3], fr.at[3], at_x(v, 0))
        with scope("f_rety"):
            await_bytes(fxr.at[0 : nx - 1], fr.at[3])
            for q in range(CHUNKS):
                total = fxs[x, :, :, cols(q)].astype(F32)
                for v in xs:
                    total += fxr[v, :, :, cols(q)].astype(F32)
                total = total.astype(BF16)
                for v in range(ny):
                    for col in range(2):
                        fys[v, col, :, cols(q)] = total[col, 2 * v : 2 * v + 2, :]
            for v in ys:
                push(fys.at[v], fyr.at[y], fs.at[4], fr.at[4], at_y(v, 0))
        with scope("f_retz"):
            await_bytes(fyr.at[0 : ny - 1], fr.at[4])
            for q in range(CHUNKS):
                total = fys[y, :, :, cols(q)].astype(F32)
                for v in ys:
                    total += fyr[v, :, :, cols(q)].astype(F32)
                fzs[:, :, cols(q)] = total.astype(BF16)
            for core in range(2):
                push(fzs.at[core], fin, fs.at[5], fr.at[5], across(core))

    def hop(s, q):
        for direction, b, later, device in (
            (0, going_up(s), going_up(s + 1), up),
            (1, going_down(s), going_down(s + 1), down),
        ):
            block = xbuf.at[b, :, :, part(q)]
            await_bytes(block, ra.at[arrival(s), direction, q])
            if s < steps:
                push(block, xbuf.at[later, :, :, part(q)], sa, ra.at[arrival(s + 1), direction, q], device)
                push(block, block, sx, rx.at[1 if s == steps - 1 else 0], partner)

    @pl.when(lead)
    def _():
        with scope("xstage"):
            for q in other:
                await_bytes(a1.at[0 : 2 * nx - 1, :, own(q)], r1.at[q])
                for v in ys:
                    push(a1.at[:, :, own(q)], b1.at[y, :, :, own(q)], so.at[1], r2.at[q], at_y(v, 1))
                b1[y, :, :, own(q)] = a1[:, :, own(q)]
            for q in main:
                await_bytes(t1.at[0 : 2 * ny - 1, :, part(q)], r1.at[q])
                for v in range(ny):
                    for col in range(2):
                        t2[x, col, 2 * v : 2 * v + 2, part(q)] = t1[2 * v + col, :, part(q)]
                for v in xs:
                    block = t2.at[x, :, :, part(q)]
                    push(block, block, s2, r2.at[q], at_x(v))

        with scope("pack"):
            pickers = None
            for q in ring_order:
                if q in main:
                    await_bytes(t2.at[0 : nx - 1, :, :, part(q)], r2.at[q])
                else:
                    await_bytes(b1.at[0 : ny - 1, :, :, own(q)], r2.at[q])
                    for v in range(ny):
                        for j in range(2 * nx):
                            t2[j // 2, j % 2, 2 * v : 2 * v + 2, part(q)] = b1[v, j, :, own(q)]
                if q == 0:
                    pickers = [picker(t2, col, 0) for col in range(2)]
                for col in range(2):
                    field = t2[:, col, :, part(q)].reshape(cells, lens[q])
                    picked = jnp.dot(pickers[col], field, preferred_element_type=F32)
                    xbuf[0, col, :, part(q)] = picked.astype(BF16)
                block = xbuf.at[0, :, :, part(q)]
                push(block, xbuf.at[going_up(1), :, :, part(q)], sa, ra.at[arrival(1), 0, q], up)
                push(block, xbuf.at[going_down(1), :, :, part(q)], sa, ra.at[arrival(1), 1, q], down)
                push(block, block, sx, rx.at[0], partner)
            weights_here()

        with scope("ring"):
            for s in range(1, steps + 1):
                for q in ring_order:
                    hop(s, q)
                    if s == steps:
                        gate_up(near, 2, q)
        with scope("act"):
            hidden = activations(near, 2)

        def onward(direction, s, q, value, device):
            i = slot(direction, s)
            if s > 1:
                await_bytes(rrecv.at[i - 1, :, :, cols(q)], ra.at[arrival(steps + s - 1), direction, q])
                value = value + rrecv[i - 1, :, :, cols(q)]
            rsend[i, :, :, cols(q)] = value
            push(rsend.at[i, :, :, cols(q)], rrecv.at[i, :, :, cols(q)], ss, ra.at[arrival(steps + s), direction, q], device)

        with scope("rs1"):
            for q in back_order:
                v = project(hidden, q).astype(BF16).reshape(2, 2, rows, width)
                onward(0, 1, q, v[1], up)
                onward(1, 1, q, v[0], down)
        with scope("rs"):
            pickers = [picker(t2, col, 1) for col in range(2)]
            for s in range(2, steps + 1):
                at = steps + 1 - s
                await_bytes(pnear.at[0:2], rp.at[at])
                for q in back_order:
                    onward(0, s, q, pnear[going_down(at), :, :, cols(q)], up)
                    onward(1, s, q, pnear[going_up(at), :, :, cols(q)], down)

        with scope("retx"):
            await_bytes(pnear.at[0], rp.at[0])
            for q in back_order:
                one, two = slot(0, steps), slot(1, steps)
                await_bytes(rrecv.at[two, :, :, cols(q)], ra.at[arrival(2 * steps), 1, q])
                await_bytes(rrecv.at[one, :, :, cols(q)], ra.at[arrival(2 * steps), 0, q])
                total = pnear[0, :, :, cols(q)].astype(F32) + rrecv[one, :, :, cols(q)].astype(F32)
                total = (total + rrecv[two, :, :, cols(q)].astype(F32)).astype(BF16)
                for col in range(2):
                    placed = jnp.dot(pickers[col], total[col], preferred_element_type=F32).astype(BF16)
                    if q in main:
                        ysend[:, col, :, cols(q)] = placed.reshape(nx, 2 * ny, width)
                    else:
                        for i in range(nx * ny):
                            c1[i % ny, 2 * (i // ny) + col, :, own(q)] = placed[2 * i : 2 * i + 2, :]
                if q in main:
                    for v in xs:
                        push(ysend.at[v, :, :, cols(q)], yrecv.at[x, :, :, cols(q)], s3, r3.at[q], at_x(v))
                else:
                    for v in ys:
                        push(c1.at[v, :, :, own(q)], c2.at[y, :, :, own(q)], so.at[2], r3.at[q], at_y(v, 1))
        with scope("rety"):
            for q in main:
                await_bytes(yrecv.at[0 : nx - 1, :, :, cols(q)], r3.at[q])
                total = ysend[x, :, :, cols(q)].astype(F32)
                for v in xs:
                    total += yrecv[v, :, :, cols(q)].astype(F32)
                total = total.astype(BF16)
                for v in range(ny):
                    for col in range(2):
                        fsend[v, col, :, cols(q)] = total[col, 2 * v : 2 * v + 2, :]
                for v in ys:
                    for col in range(2):
                        push(fsend.at[v, col, :, cols(q)], frecv.at[y, :, cols(q)], s4, r4.at[q], at_y(v, col))
                push(fsend.at[y, 0, :, cols(q)], frecv.at[y, :, cols(q)], s0, r4.at[q], partner)
                frecv[y, :, cols(q)] = fsend[y, 1, :, cols(q)]
            for q in other:
                await_bytes(c2.at[0 : ny - 1, :, :, own(q)], r3.at[q])
                total = c1[y, :, :, own(q)].astype(F32)
                for v in ys:
                    total += c2[v, :, :, own(q)].astype(F32)
                e1[:, :, own(q)] = total.astype(BF16)
                for v in xs:
                    for col in range(2):
                        push(e1.at[2 * v + col, :, own(q)], e2.at[x, :, own(q)], so.at[3], r4.at[q], at_x(v, col))
                push(e1.at[2 * x, :, own(q)], e2.at[x, :, own(q)], so.at[4], r4.at[q], partner)
                e2[x, :, own(q)] = e1[2 * x + 1, :, own(q)]

    with scope("final"):
        await_bytes(fin, fr.at[5])
        for q in range(CHUNKS):
            parts, mine, count = (frecv, cols(q), ny) if q in main else (e2, own(q), nx)

            @pl.when(lead)
            def _():
                await_bytes(parts.at[0 : count - 1, :, mine], r4.at[q])

            @pl.when(jnp.logical_not(lead))
            def _():
                await_bytes(parts.at[:, :, mine], r4.at[q])

            total = fin[:, cols(q)].astype(F32)
            for v in range(count):
                total += parts[v, :, mine].astype(F32)
            total = total.astype(BF16)
            outv[0:1, cols(q)] = total[0:1, :]
            outv[0:1, pl.ds(half + q * width, width)] = total[1:2, :]

    result = pltpu.make_async_copy(outv, out_ref, out_sem)
    result.start()

    with scope("drain"):
        await_bytes(t1.at[0 : ny - 1, :, main_part], s1)
        await_bytes(a1.at[0 : nx - 1], so.at[0])
        await_bytes(wgu.at[:, :, 1], ws_sem.at[0])
        await_bytes(wdn.at[:, 1], ws_sem.at[1])

        @pl.when(jnp.logical_not(lead))
        def _():
            await_bytes(tsend, s0)
            await_bytes(pnear, sp)
            await_bytes(ftok, fs.at[0])
            await_bytes(ft1.at[0 : ny - 1], fs.at[1])
            await_bytes(ft2.at[0 : nx - 1], fs.at[2])
            await_bytes(fxs.at[0 : nx - 1], fs.at[3])
            await_bytes(fys.at[0 : ny - 1], fs.at[4])
            await_bytes(fzs, fs.at[5])

        @pl.when(lead)
        def _():
            await_bytes(t2.at[0 : nx - 1, :, :, main_part], s2)
            await_bytes(b1.at[0 : ny - 1], so.at[1])
            await_bytes(c2.at[0 : ny - 1], so.at[2])
            await_bytes(e1.at[0 : 2 * (nx - 1)], so.at[3])
            await_bytes(e1.at[0], so.at[4])
            await_bytes(xbuf.at[0 : 2 * steps], sa)
            await_bytes(xbuf.at[0:near], sx)
            await_bytes(rsend, ss)
            await_bytes(yrecv.at[0 : nx - 1, :, :, main_cols], s3)
            await_bytes(fsend.at[0 : ny - 1, :, :, main_cols], s4)
            await_bytes(frecv.at[0, :, main_cols], s0)
            await_bytes(tsend, fs.at[0])

        result.wait()


def solution(mesh):
    nodes, locals_ = mesh.shape["node"], mesh.shape["local"]
    nx = min(NX, nodes)
    ny, nz = nodes // nx, locals_ // 2
    hz = nz // 2
    steps = hz - 1
    near = 2 * steps - 1

    def on_device(tokens, w_gate, w_up, w_down, expert_ids, gate_ints):
        model_width = tokens.shape[1]
        half = model_width // 2
        exp_node, ffl = w_gate.shape[0], w_gate.shape[1]
        units = 2 * exp_node * ffl
        rows = 2 * CAP
        lanes = OTHER * (half // CHUNKS)
        sem = pltpu.SemaphoreType.DMA
        one = sem(())
        any_space = pl.BlockSpec(memory_space=pl.ANY)
        vmem = pl.BlockSpec(memory_space=pltpu.VMEM)
        return pl.pallas_call(
            functools.partial(layer_kernel, nx, ny, nz),
            out_shape=jax.ShapeDtypeStruct((1, model_width), BF16),
            in_specs=[any_space] * 6,
            out_specs=any_space,
            scratch_shapes=[
                pltpu.VMEM((1, model_width), BF16),
                pltpu.SMEM(expert_ids.shape, jnp.int32),
                pltpu.SMEM(gate_ints.shape, jnp.int32),
                pltpu.VMEM((2, META + half), BF16),
                pltpu.VMEM((2 * ny, 2, META + half), BF16),
                pltpu.VMEM((nx, 2, 2 * ny, META + half), BF16),
                pltpu.VMEM((nz, 2, rows, META + half), BF16),
                pltpu.VMEM((2, 2, 2, exp_node, ffl, half), BF16),
                pltpu.VMEM((2, 2, exp_node, ffl, half), BF16),
                pltpu.VMEM((2, 2, near * 2 * rows, units), F32),
                pltpu.VMEM((2, near * 2 * rows, units), F32),
                pltpu.VMEM((near, 2, rows, half), BF16),
                pltpu.VMEM((2 * steps, 2, rows, half), BF16),
                pltpu.VMEM((2 * steps, 2, rows, half), BF16),
                pltpu.VMEM((nx, 2, 2 * ny, half), BF16),
                pltpu.VMEM((nx, 2, 2 * ny, half), BF16),
                pltpu.VMEM((ny, 2, 2, half), BF16),
                pltpu.VMEM((ny, 2, half), BF16),
                pltpu.VMEM((2, 2, META + half), BF16),
                pltpu.VMEM((ny, 2, 2, META + half), BF16),
                pltpu.VMEM((nx, 2, 2 * ny, META + half), BF16),
                pltpu.VMEM((nx, 2, 2 * ny, half), BF16),
                pltpu.VMEM((nx, 2, 2 * ny, half), BF16),
                pltpu.VMEM((ny, 2, 2, half), BF16),
                pltpu.VMEM((ny, 2, 2, half), BF16),
                pltpu.VMEM((2, 2, half), BF16),
                pltpu.VMEM((2, half), BF16),
                pltpu.VMEM((2 * nx, 2, lanes), BF16),
                pltpu.VMEM((ny, 2 * nx, 2, lanes), BF16),
                pltpu.VMEM((ny, 2 * nx, 2, lanes), BF16),
                pltpu.VMEM((ny, 2 * nx, 2, lanes), BF16),
                pltpu.VMEM((2 * nx, 2, lanes), BF16),
                pltpu.VMEM((nx, 2, lanes), BF16),
                sem((3,)), sem((2,)), sem((2,)), sem((2,)),
                one, one, sem((CHUNKS,)), one, sem((CHUNKS,)),
                one, sem((4, 2, CHUNKS)), one, sem((2,)), one, sem((steps,)),
                one, one, sem((CHUNKS,)), one, sem((CHUNKS,)),
                sem((6,)), sem((7,)), pltpu.SemaphoreType.REGULAR, sem((5,)),
                pltpu.VMEM((1, model_width), BF16), one,
            ],
            compiler_params=pltpu.CompilerParams(
                collective_id=0, has_side_effects=True, vmem_limit_bytes=44 * 1024 * 1024
            ),
            name="layer",
        )(*(pltpu.with_memory_space_constraint(a, pltpu.HBM) for a in (tokens, w_gate, w_up, w_down, expert_ids, gate_ints)))

    both = P(("node", "local"), None)
    weights = P("node", "local", None)
    return jax.shard_map(
        on_device, mesh=mesh,
        in_specs=(both, weights, weights, weights, both, both),
        out_specs=both, check_vma=False,
    )
```

```python
import functools

import jax
import jax.numpy as jnp
from jax import lax
from jax.experimental import pallas as pl
from jax.experimental.pallas import tpu as pltpu
from jax.sharding import PartitionSpec as P

CAP = 8
NX = 4
PARTS = (4, 4, 4, 4, 4, 4, 4)
CHUNKS = len(PARTS)
OTHER = 2
META = 128
BF16 = jnp.bfloat16
F32 = jnp.float32
MESH_ID = pl.DeviceIdType.MESH
NT = (((1,), (1,)), ((), ()))
scope = jax.named_scope


def ones(mask):
    return mask.astype(F32).astype(BF16)


def layer_kernel(
    nx, ny, nz,
    tok_ref, wg_ref, wu_ref, wd_ref, ids_ref, gates_ref,
    out_ref,
    tokv, idsv, gatesv, tsend, t1, t2, xbuf, wgu, wdn, zbuf, hbuf, pnear, rsend, rrecv,
    ysend, yrecv, fsend, frecv, ftok, ft1, ft2, fxs, fxr, fys, fyr, fzs, fin, a1, b1, c1, c2, e1, e2,
    in_sem, wl_sem, ws_sem, wr_sem, s0, s1, r1, s2, r2, sa, ra, sx, rx, sp, rp, ss, s3, s4, r4,
    fs, fr, ready, so, outv, out_sem,
):
    half = wgu.shape[-1]
    widths = [half * part // sum(PARTS) for part in PARTS]
    starts = [sum(widths[:q]) for q in range(CHUNKS + 1)]
    offs = [0] + [META + start for start in starts[1:]]
    lens = [META + widths[0]] + widths[1:]
    hz = nz // 2
    rows = CAP * 2
    ffl = wdn.shape[3]
    units = wdn.shape[1] * wdn.shape[2] * ffl
    n = lax.axis_index("node")
    l = lax.axis_index("local")
    x, y = lax.rem(n, nx), n // nx
    z, c = l // 2, lax.rem(l, 2)
    lead = c == 1

    def at_x(v, core=1):
        return (y * nx + v, z * 2 + core)

    def at_y(v, core):
        return (v * nx + x, z * 2 + core)

    up = (n, lax.rem(z + 1, nz) * 2 + 1)
    down = (n, lax.rem(z + nz - 1, nz) * 2 + 1)
    partner = (n, z * 2 + 1 - c)
    xs = [lax.rem(x + d, nx) for d in sorted(range(1, nx), key=lambda d: -min(d, nx - d))]
    ys = [lax.rem(y + d, ny) for d in sorted(range(1, ny), key=lambda d: -min(d, ny - d))]

    steps = hz - 1
    near = 2 * steps - 1
    opposite = near + 2

    def going_up(s):
        return 2 * s - 1

    def going_down(s):
        return 2 * s

    early = z < hz

    def across(core):
        return (n, lax.rem(z + hz, nz) * 2 + core)

    def push(src, dst, send, recv, device):
        pltpu.make_async_remote_copy(
            src_ref=src, dst_ref=dst, send_sem=send, recv_sem=recv,
            device_id=device, device_id_type=MESH_ID,
        ).start()

    def await_bytes(ref, sem):
        pltpu.make_async_copy(ref, ref, sem).wait()

    def signal(sem, device):
        pl.semaphore_signal(sem, 1, device_id=device, device_id_type=MESH_ID)

    def part(q):
        return pl.ds(offs[q], lens[q])

    def cols(q):
        return pl.ds(starts[q], widths[q])

    main, other = range(CHUNKS - OTHER), range(CHUNKS - OTHER, CHUNKS)
    split = starts[len(main)]
    main_part, main_cols = pl.ds(0, META + split), pl.ds(0, split)
    other_part = pl.ds(META + split, half - split)
    ring_order = list(main[:1]) + [q for pair in zip(other, main[1:]) for q in pair] + list(main[1 + OTHER :])
    back_order = [*main[:2], other[0], main[2], other[1], *main[3:]]

    def own(q):
        return pl.ds(starts[q] - split, widths[q])

    barrier = pltpu.get_barrier_semaphore()
    with scope("entry"):
        signal(barrier, partner)
        for v in ys:
            signal(barrier, at_y(v, 1))
            signal(barrier, at_y(v, 0))
        for v in xs:
            signal(barrier, at_x(v, 0))
            signal(barrier, at_x(v, 1))

        @pl.when(lead)
        def _():
            signal(barrier, up)
            signal(barrier, down)

        @pl.when(early)
        def _():
            signal(barrier, across(0))

            @pl.when(jnp.logical_not(lead))
            def _():
                signal(barrier, across(1))

        inputs = [
            pltpu.make_async_copy(tok_ref, tokv, in_sem.at[0]),
            pltpu.make_async_copy(ids_ref, idsv, in_sem.at[1]),
            pltpu.make_async_copy(gates_ref, gatesv, in_sem.at[2]),
        ]
        for copy in inputs:
            copy.start()
        for h in range(2):
            wcols = pl.ds(h * half, half)
            pltpu.make_async_copy(wg_ref.at[:, :, wcols], wgu.at[h, 0, 0], wl_sem.at[0]).start()
            pltpu.make_async_copy(wu_ref.at[:, :, wcols], wgu.at[h, 1, 0], wl_sem.at[0]).start()
            pltpu.make_async_copy(wd_ref.at[:, :, wcols], wdn.at[h, 0], wl_sem.at[1]).start()

        for copy in inputs:
            copy.wait()
        lane = lax.broadcasted_iota(jnp.int32, (2, META), 1)
        row = lax.broadcasted_iota(jnp.int32, (2, META), 0)
        gates = jnp.zeros((2, META), jnp.int32)
        for k in range(ids_ref.shape[1]):
            gates += jnp.where((lane == idsv[0, k]) & (row == 0), gatesv[0, k], 0)
        tsend[:, 0:META] = gates.astype(F32).astype(BF16)
        tok = tokv[...].astype(F32)
        tsend[:, META:] = jnp.concatenate([tok[:, :half], tok[:, half:]], axis=0).astype(BF16)

        @pl.when(lead)
        def _():
            t1[y * 2 + 1] = tsend[...]
            a1[x * 2 + 1] = tsend[:, other_part]

        @pl.when(jnp.logical_not(lead))
        def _():
            ftok[0] = tsend[...]

    with scope("bar"):
        count = 1 + 2 * (ny - 1) + 2 * (nx - 1) + 2 * c + (z // hz) * (2 - c)
        pl.semaphore_wait(barrier, count)

        @pl.when(jnp.logical_not(early))
        def _():
            signal(ready, across(0))

    with scope("ypush"):
        for q in other:
            for v in xs:
                push(tsend.at[:, part(q)], a1.at[x * 2 + c, :, own(q)], so.at[0], r1.at[q], at_x(v))

            @pl.when(jnp.logical_not(lead))
            def _():
                push(tsend.at[:, part(q)], a1.at[x * 2 + c, :, own(q)], s0, r1.at[q], partner)

        for q in main:
            for v in ys:
                push(tsend.at[:, part(q)], t1.at[y * 2 + c, :, part(q)], s1, r1.at[q], at_y(v, 1))

            @pl.when(jnp.logical_not(lead))
            def _():
                push(tsend.at[:, part(q)], t1.at[y * 2 + c, :, part(q)], s0, r1.at[q], partner)

        @pl.when(lead)
        def _():
            push(tsend, ftok.at[1], fs.at[0], fr.at[6], partner)

        for h in range(2):
            wcols = pl.ds(h * half, half)
            push(wg_ref.at[:, :, wcols], wgu.at[h, 0, 1], ws_sem.at[0], wr_sem.at[0], partner)
            push(wu_ref.at[:, :, wcols], wgu.at[h, 1, 1], ws_sem.at[0], wr_sem.at[0], partner)
            push(wd_ref.at[:, :, wcols], wdn.at[h, 1], ws_sem.at[1], wr_sem.at[1], partner)

    cells = nx * ny * 2

    def order(i):
        return ((i // 2) % ny) * nx + i // (2 * ny)

    def picker(field, col, side):
        i0 = lax.broadcasted_iota(jnp.int32, (cells, cells), 0)
        i1 = lax.broadcasted_iota(jnp.int32, (cells, cells), 1)
        same = ones(i0 // 2 == i1 // 2)
        own = ones(lax.broadcasted_iota(jnp.int32, (rows, META), 1) // 2 == n)
        meta = field[:, col, :, 0:META].reshape(cells, META)
        if side == 0:
            total = lax.dot_general(own, meta, NT, preferred_element_type=F32)
            hit = ones(total > 0)
            rank = jnp.dot(hit, ones(order(i0) < order(i1)), preferred_element_type=F32)
            hit = jnp.dot(hit, same, preferred_element_type=F32)
            shape = (rows, cells)
        else:
            total = lax.dot_general(meta, own, NT, preferred_element_type=F32)
            hit = ones(total > 0)
            rank = jnp.dot(ones(order(i1) < order(i0)), hit, preferred_element_type=F32)
            hit = jnp.dot(same, hit, preferred_element_type=F32)
            shape = (cells, rows)
        r = lax.broadcasted_iota(jnp.int32, shape, side)
        i = lax.broadcasted_iota(jnp.int32, shape, 1 - side)
        return ones((hit > 0) & (rank == (r // 2).astype(F32)) & (r % 2 == i % 2))

    def weights_here():
        await_bytes(wgu.at[:, :, 0], wl_sem.at[0])
        await_bytes(wdn.at[:, 0], wl_sem.at[1])
        await_bytes(wgu.at[:, :, 1], wr_sem.at[0])
        await_bytes(wdn.at[:, 1], wr_sem.at[1])

    def gate_up(start, blocks, q):
        count = blocks * 2 * rows
        piece = xbuf[start : start + blocks, :, :, pl.ds(META + starts[q], widths[q])].reshape(count, widths[q])
        for h in range(2):
            w = wgu[h, :, :, :, :, cols(q)].reshape(2 * units, widths[q])
            v = lax.dot_general(piece, w, NT, preferred_element_type=F32)
            for k in range(2):
                if q == 0:
                    zbuf[h, k, 0:count] = v[:, k * units : (k + 1) * units]
                else:
                    zbuf[h, k, 0:count] += v[:, k * units : (k + 1) * units]

    def activations(start, blocks):
        count = blocks * 2 * rows
        lane = lax.broadcasted_iota(jnp.int32, (META, units), 0)
        unit = lax.broadcasted_iota(jnp.int32, (META, units), 1)
        chosen = ones(lane == 2 * n + (unit // ffl) % 2)
        gate_rows = xbuf[start : start + blocks, :, :, 0:META].reshape(count, META)
        hbuf[0, 0:count] = jnp.dot(gate_rows, chosen, preferred_element_type=F32)
        even, odd = pl.ds(0, count // 2, 2), pl.ds(1, count // 2, 2)
        gate_act = zbuf[0, 0, even, :] + zbuf[1, 0, odd, :]
        up_act = zbuf[0, 1, even, :] + zbuf[1, 1, odd, :]
        scale = hbuf[0, even, :] / 8.0
        hidden = gate_act / (1.0 + jnp.exp(-gate_act)) * up_act * scale
        none = jnp.zeros_like(hidden)
        hbuf[0, even, :] = hidden
        hbuf[1, even, :] = none
        hbuf[0, odd, :] = none
        hbuf[1, odd, :] = hidden
        return jnp.concatenate([hbuf[0, 0:count], hbuf[1, 0:count]], axis=1).astype(BF16)

    def project(hidden, q):
        w = wdn[:, :, :, :, cols(q)].reshape(2 * units, widths[q])
        return jnp.dot(hidden, w, preferred_element_type=F32)

    def arrival(k):
        return k % 3

    def slot(direction, step):
        return direction * steps + step - 1

    @pl.when(jnp.logical_not(lead))
    def _():
        with scope("f_token"):
            @pl.when(early)
            def _():
                pl.semaphore_wait(ready, 2)

            await_bytes(ftok.at[1], fr.at[6])
            push(ftok, ft1.at[y], fs.at[0], fr.at[0], across(0))
        with scope("f_y"):
            await_bytes(ft1.at[y], fr.at[0])
            for v in ys:
                push(ft1.at[y], ft1.at[y], fs.at[1], fr.at[1], at_y(v, 0))
        with scope("f_x"):
            await_bytes(ft1.at[0 : ny - 1], fr.at[1])
            for v in range(ny):
                for col in range(2):
                    ft2[x, col, 2 * v : 2 * v + 2] = ft1[v, col]
            for v in xs:
                push(ft2.at[x], ft2.at[x], fs.at[2], fr.at[2], at_x(v, 0))
        with scope("s_wait"):
            weights_here()
        for batch, (start, blocks) in enumerate(((0, near - 2), (near - 2, 2))):
            with scope(f"s_wait{batch}"):
                await_bytes(xbuf.at[start : start + blocks], rx.at[batch])
            with scope(f"s_comp{batch}"):
                for q in range(CHUNKS):
                    gate_up(start, blocks, q)
                hidden = activations(start, blocks)
                for q in range(CHUNKS):
                    v = project(hidden, q).astype(BF16).reshape(blocks, 2, rows, widths[q])
                    pnear[start : start + blocks, :, :, cols(q)] = v
        for b in range(near - 1, -1, -1):
            push(pnear.at[b], pnear.at[b], sp, rp.at[(b + 1) // 2], partner)
        with scope("f_pack"):
            await_bytes(ft2.at[0 : nx - 1], fr.at[2])
            pickers = [picker(ft2, col, 0) for col in range(2)]
            for col in range(2):
                for q in range(CHUNKS):
                    field = ft2[:, col, :, part(q)].reshape(cells, lens[q])
                    picked = jnp.dot(pickers[col], field, preferred_element_type=F32)
                    xbuf[opposite, col, :, part(q)] = picked.astype(BF16)
            for q in range(CHUNKS):
                gate_up(opposite, 1, q)
            hidden = activations(opposite, 1)
        with scope("f_retx"):
            pickers = [picker(ft2, col, 1) for col in range(2)]
            for q in range(CHUNKS):
                v = project(hidden, q).astype(BF16).reshape(2, rows, widths[q])
                for col in range(2):
                    placed = jnp.dot(pickers[col], v[col], preferred_element_type=F32)
                    fxs[:, col, :, cols(q)] = placed.astype(BF16).reshape(nx, 2 * ny, widths[q])
            for v in xs:
                push(fxs.at[v], fxr.at[x], fs.at[3], fr.at[3], at_x(v, 0))
        with scope("f_rety"):
            await_bytes(fxr.at[0 : nx - 1], fr.at[3])
            for q in range(CHUNKS):
                total = fxs[x, :, :, cols(q)].astype(F32)
                for v in xs:
                    total += fxr[v, :, :, cols(q)].astype(F32)
                total = total.astype(BF16)
                for v in range(ny):
                    for col in range(2):
                        fys[v, col, :, cols(q)] = total[col, 2 * v : 2 * v + 2, :]
            for v in ys:
                push(fys.at[v], fyr.at[y], fs.at[4], fr.at[4], at_y(v, 0))
        with scope("f_retz"):
            await_bytes(fyr.at[0 : ny - 1], fr.at[4])
            for q in range(CHUNKS):
                total = fys[y, :, :, cols(q)].astype(F32)
                for v in ys:
                    total += fyr[v, :, :, cols(q)].astype(F32)
                fzs[:, :, cols(q)] = total.astype(BF16)
            for core in range(2):
                push(fzs.at[core], fin, fs.at[5], fr.at[5], across(core))

    def hop(s, q):
        for direction, b, later, device in (
            (0, going_up(s), going_up(s + 1), up),
            (1, going_down(s), going_down(s + 1), down),
        ):
            block = xbuf.at[b, :, :, part(q)]
            await_bytes(block, ra.at[arrival(s), direction, q])
            if s < steps:
                push(block, xbuf.at[later, :, :, part(q)], sa, ra.at[arrival(s + 1), direction, q], device)
                push(block, block, sx, rx.at[1 if s == steps - 1 else 0], partner)

    @pl.when(lead)
    def _():
        with scope("xstage"):
            for q in other:
                await_bytes(a1.at[0 : 2 * nx - 1, :, own(q)], r1.at[q])
                for v in ys:
                    push(a1.at[:, :, own(q)], b1.at[y, :, :, own(q)], so.at[1], r2.at[q], at_y(v, 1))
                b1[y, :, :, own(q)] = a1[:, :, own(q)]
            for q in main:
                await_bytes(t1.at[0 : 2 * ny - 1, :, part(q)], r1.at[q])
                for v in range(ny):
                    for col in range(2):
                        t2[x, col, 2 * v : 2 * v + 2, part(q)] = t1[2 * v + col, :, part(q)]
                for v in xs:
                    block = t2.at[x, :, :, part(q)]
                    push(block, block, s2, r2.at[q], at_x(v))

        with scope("pack"):
            pickers = None
            for q in ring_order:
                if q in main:
                    await_bytes(t2.at[0 : nx - 1, :, :, part(q)], r2.at[q])
                else:
                    await_bytes(b1.at[0 : ny - 1, :, :, own(q)], r2.at[q])
                    for v in range(ny):
                        for j in range(2 * nx):
                            t2[j // 2, j % 2, 2 * v : 2 * v + 2, part(q)] = b1[v, j, :, own(q)]
                if q == 0:
                    pickers = [picker(t2, col, 0) for col in range(2)]
                for col in range(2):
                    field = t2[:, col, :, part(q)].reshape(cells, lens[q])
                    picked = jnp.dot(pickers[col], field, preferred_element_type=F32)
                    xbuf[0, col, :, part(q)] = picked.astype(BF16)
                block = xbuf.at[0, :, :, part(q)]
                push(block, xbuf.at[going_up(1), :, :, part(q)], sa, ra.at[arrival(1), 0, q], up)
                push(block, xbuf.at[going_down(1), :, :, part(q)], sa, ra.at[arrival(1), 1, q], down)
                push(block, block, sx, rx.at[0], partner)
            weights_here()

        with scope("ring"):
            for s in range(1, steps + 1):
                for q in ring_order:
                    hop(s, q)
                    if s == steps:
                        gate_up(near, 2, q)
        with scope("act"):
            hidden = activations(near, 2)

        def onward(direction, s, q, value, device):
            i = slot(direction, s)
            if s > 1:
                await_bytes(rrecv.at[i - 1, :, :, cols(q)], ra.at[arrival(steps + s - 1), direction, q])
                value = value + rrecv[i - 1, :, :, cols(q)]
            rsend[i, :, :, cols(q)] = value
            push(rsend.at[i, :, :, cols(q)], rrecv.at[i, :, :, cols(q)], ss, ra.at[arrival(steps + s), direction, q], device)

        with scope("rs1"):
            for q in back_order:
                v = project(hidden, q).astype(BF16).reshape(2, 2, rows, widths[q])
                onward(0, 1, q, v[1], up)
                onward(1, 1, q, v[0], down)
        with scope("rs"):
            pickers = [picker(t2, col, 1) for col in range(2)]
            for s in range(2, steps + 1):
                at = steps + 1 - s
                await_bytes(pnear.at[0:2], rp.at[at])
                for q in back_order:
                    onward(0, s, q, pnear[going_down(at), :, :, cols(q)], up)
                    onward(1, s, q, pnear[going_up(at), :, :, cols(q)], down)

        with scope("retx"):
            await_bytes(pnear.at[0], rp.at[0])
            for q in back_order:
                one, two = slot(0, steps), slot(1, steps)
                await_bytes(rrecv.at[two, :, :, cols(q)], ra.at[arrival(2 * steps), 1, q])
                await_bytes(rrecv.at[one, :, :, cols(q)], ra.at[arrival(2 * steps), 0, q])
                total = pnear[0, :, :, cols(q)].astype(F32) + rrecv[one, :, :, cols(q)].astype(F32)
                total = (total + rrecv[two, :, :, cols(q)].astype(F32)).astype(BF16)
                for col in range(2):
                    placed = jnp.dot(pickers[col], total[col], preferred_element_type=F32).astype(BF16)
                    if q in main:
                        ysend[:, col, :, cols(q)] = placed.reshape(nx, 2 * ny, widths[q])
                    else:
                        for i in range(nx * ny):
                            c1[i % ny, 2 * (i // ny) + col, :, own(q)] = placed[2 * i : 2 * i + 2, :]
                if q in main:
                    for v in xs:
                        push(ysend.at[v, :, :, cols(q)], yrecv.at[x, :, :, cols(q)], s3, r1.at[q], at_x(v))
                else:
                    for v in ys:
                        push(c1.at[v, :, :, own(q)], c2.at[y, :, :, own(q)], so.at[2], r1.at[q], at_y(v, 1))
        with scope("rety"):
            for q in main:
                await_bytes(yrecv.at[0 : nx - 1, :, :, cols(q)], r1.at[q])
                total = ysend[x, :, :, cols(q)].astype(F32)
                for v in xs:
                    total += yrecv[v, :, :, cols(q)].astype(F32)
                total = total.astype(BF16)
                for v in range(ny):
                    for col in range(2):
                        fsend[v, col, :, cols(q)] = total[col, 2 * v : 2 * v + 2, :]
                for v in ys:
                    for col in range(2):
                        push(fsend.at[v, col, :, cols(q)], frecv.at[y, :, cols(q)], s4, r4.at[q], at_y(v, col))
                push(fsend.at[y, 0, :, cols(q)], frecv.at[y, :, cols(q)], s0, r4.at[q], partner)
                frecv[y, :, cols(q)] = fsend[y, 1, :, cols(q)]
            for q in other:
                await_bytes(c2.at[0 : ny - 1, :, :, own(q)], r1.at[q])
                total = c1[y, :, :, own(q)].astype(F32)
                for v in ys:
                    total += c2[v, :, :, own(q)].astype(F32)
                e1[:, :, own(q)] = total.astype(BF16)
                for v in xs:
                    for col in range(2):
                        push(e1.at[2 * v + col, :, own(q)], e2.at[x, :, own(q)], so.at[3], r4.at[q], at_x(v, col))
                push(e1.at[2 * x, :, own(q)], e2.at[x, :, own(q)], so.at[4], r4.at[q], partner)
                e2[x, :, own(q)] = e1[2 * x + 1, :, own(q)]

    with scope("final"):
        await_bytes(fin, fr.at[5])
        for q in range(CHUNKS):
            parts, mine, count = (frecv, cols(q), ny) if q in main else (e2, own(q), nx)

            @pl.when(lead)
            def _():
                await_bytes(parts.at[0 : count - 1, :, mine], r4.at[q])

            @pl.when(jnp.logical_not(lead))
            def _():
                await_bytes(parts.at[:, :, mine], r4.at[q])

            total = fin[:, cols(q)].astype(F32)
            for v in range(count):
                total += parts[v, :, mine].astype(F32)
            total = total.astype(BF16)
            outv[0:1, cols(q)] = total[0:1, :]
            outv[0:1, pl.ds(half + starts[q], widths[q])] = total[1:2, :]

    result = pltpu.make_async_copy(outv, out_ref, out_sem)
    result.start()

    with scope("drain"):
        await_bytes(t1.at[0 : ny - 1, :, main_part], s1)
        await_bytes(a1.at[0 : nx - 1], so.at[0])
        await_bytes(wgu.at[:, :, 1], ws_sem.at[0])
        await_bytes(wdn.at[:, 1], ws_sem.at[1])

        @pl.when(jnp.logical_not(lead))
        def _():
            await_bytes(tsend, s0)
            await_bytes(pnear, sp)
            await_bytes(ftok, fs.at[0])
            await_bytes(ft1.at[0 : ny - 1], fs.at[1])
            await_bytes(ft2.at[0 : nx - 1], fs.at[2])
            await_bytes(fxs.at[0 : nx - 1], fs.at[3])
            await_bytes(fys.at[0 : ny - 1], fs.at[4])
            await_bytes(fzs, fs.at[5])

        @pl.when(lead)
        def _():
            await_bytes(t2.at[0 : nx - 1, :, :, main_part], s2)
            await_bytes(b1.at[0 : ny - 1], so.at[1])
            await_bytes(c2.at[0 : ny - 1], so.at[2])
            await_bytes(e1.at[0 : 2 * (nx - 1)], so.at[3])
            await_bytes(e1.at[0], so.at[4])
            await_bytes(xbuf.at[0 : 2 * steps], sa)
            await_bytes(xbuf.at[0:near], sx)
            await_bytes(rsend, ss)
            await_bytes(yrecv.at[0 : nx - 1, :, :, main_cols], s3)
            await_bytes(fsend.at[0 : ny - 1, :, :, main_cols], s4)
            await_bytes(frecv.at[0, :, main_cols], s0)
            await_bytes(tsend, fs.at[0])

        result.wait()


def solution(mesh):
    nodes, locals_ = mesh.shape["node"], mesh.shape["local"]
    nx = min(NX, nodes)
    ny, nz = nodes // nx, locals_ // 2
    hz = nz // 2
    steps = hz - 1
    near = 2 * steps - 1

    def on_device(tokens, w_gate, w_up, w_down, expert_ids, gate_ints):
        model_width = tokens.shape[1]
        half = model_width // 2
        exp_node, ffl = w_gate.shape[0], w_gate.shape[1]
        units = 2 * exp_node * ffl
        rows = 2 * CAP
        lanes = half * sum(PARTS[-OTHER:]) // sum(PARTS)
        sem = pltpu.SemaphoreType.DMA
        one = sem(())
        any_space = pl.BlockSpec(memory_space=pl.ANY)
        vmem = pl.BlockSpec(memory_space=pltpu.VMEM)
        return pl.pallas_call(
            functools.partial(layer_kernel, nx, ny, nz),
            out_shape=jax.ShapeDtypeStruct((1, model_width), BF16),
            in_specs=[any_space] * 6,
            out_specs=any_space,
            scratch_shapes=[
                pltpu.VMEM((1, model_width), BF16),
                pltpu.SMEM(expert_ids.shape, jnp.int32),
                pltpu.SMEM(gate_ints.shape, jnp.int32),
                pltpu.VMEM((2, META + half), BF16),
                pltpu.VMEM((2 * ny, 2, META + half), BF16),
                pltpu.VMEM((nx, 2, 2 * ny, META + half), BF16),
                pltpu.VMEM((nz, 2, rows, META + half), BF16),
                pltpu.VMEM((2, 2, 2, exp_node, ffl, half), BF16),
                pltpu.VMEM((2, 2, exp_node, ffl, half), BF16),
                pltpu.VMEM((2, 2, near * 2 * rows, units), F32),
                pltpu.VMEM((2, near * 2 * rows, units), F32),
                pltpu.VMEM((near, 2, rows, half), BF16),
                pltpu.VMEM((2 * steps, 2, rows, half), BF16),
                pltpu.VMEM((2 * steps, 2, rows, half), BF16),
                pltpu.VMEM((nx, 2, 2 * ny, half), BF16),
                pltpu.VMEM((nx, 2, 2 * ny, half), BF16),
                pltpu.VMEM((ny, 2, 2, half), BF16),
                pltpu.VMEM((ny, 2, half), BF16),
                pltpu.VMEM((2, 2, META + half), BF16),
                pltpu.VMEM((ny, 2, 2, META + half), BF16),
                pltpu.VMEM((nx, 2, 2 * ny, META + half), BF16),
                pltpu.VMEM((nx, 2, 2 * ny, half), BF16),
                pltpu.VMEM((nx, 2, 2 * ny, half), BF16),
                pltpu.VMEM((ny, 2, 2, half), BF16),
                pltpu.VMEM((ny, 2, 2, half), BF16),
                pltpu.VMEM((2, 2, half), BF16),
                pltpu.VMEM((2, half), BF16),
                pltpu.VMEM((2 * nx, 2, lanes), BF16),
                pltpu.VMEM((ny, 2 * nx, 2, lanes), BF16),
                pltpu.VMEM((ny, 2 * nx, 2, lanes), BF16),
                pltpu.VMEM((ny, 2 * nx, 2, lanes), BF16),
                pltpu.VMEM((2 * nx, 2, lanes), BF16),
                pltpu.VMEM((nx, 2, lanes), BF16),
                sem((3,)), sem((2,)), sem((2,)), sem((2,)),
                one, one, sem((CHUNKS,)), one, sem((CHUNKS,)),
                one, sem((3, 2, CHUNKS)), one, sem((2,)), one, sem((steps,)),
                one, one, one, sem((CHUNKS,)),
                sem((6,)), sem((7,)), pltpu.SemaphoreType.REGULAR, sem((5,)),
                pltpu.VMEM((1, model_width), BF16), one,
            ],
            compiler_params=pltpu.CompilerParams(
                collective_id=0, has_side_effects=True, vmem_limit_bytes=44 * 1024 * 1024
            ),
            name="layer",
        )(*(pltpu.with_memory_space_constraint(a, pltpu.HBM) for a in (tokens, w_gate, w_up, w_down, expert_ids, gate_ints)))

    both = P(("node", "local"), None)
    weights = P("node", "local", None)
    return jax.shard_map(
        on_device, mesh=mesh,
        in_specs=(both, weights, weights, weights, both, both),
        out_specs=both, check_vma=False,
    )
```

```python
import functools

import jax
import jax.numpy as jnp
from jax import lax
from jax.experimental import pallas as pl
from jax.experimental.pallas import tpu as pltpu
from jax.sharding import PartitionSpec as P

CAP = 8
NX = 4
PARTS = (4, 4, 4, 4, 4, 4, 4)
CHUNKS = len(PARTS)
OTHER = 2
META = 128
BF16 = jnp.bfloat16
F32 = jnp.float32
MESH_ID = pl.DeviceIdType.MESH
NT = (((1,), (1,)), ((), ()))
scope = jax.named_scope


def ones(mask):
    return mask.astype(F32).astype(BF16)


def layer_kernel(
    nx, ny, nz,
    tok_ref, wg_ref, wu_ref, wd_ref, ids_ref, gates_ref,
    out_ref,
    tokv, idsv, gatesv, tsend, t1, t2, xbuf, wgu, wdn, zbuf, hbuf, pnear, rsend, rrecv,
    ysend, yrecv, fsend, frecv, ftok, ft1, ft2, fxs, fxr, fys, fyr, fzs, fin, a1, b1, c1, c2, e1, e2, gbuf,
    in_sem, wl_sem, ws_sem, wr_sem, s0, s1, r1, s2, r2, sa, ra, sx, rx, sp, rp, ss, s3, s4, r4,
    fs, fr, ready, so, outv, out_sem, gs, gr, gx,
):
    half = wgu.shape[-1]
    widths = [half * part // sum(PARTS) for part in PARTS]
    starts = [sum(widths[:q]) for q in range(CHUNKS + 1)]
    offs = [0] + [META + start for start in starts[1:]]
    lens = [META + widths[0]] + widths[1:]
    hz = nz // 2
    rows = CAP * 2
    ffl = wdn.shape[3]
    units = wdn.shape[1] * wdn.shape[2] * ffl
    n = lax.axis_index("node")
    l = lax.axis_index("local")
    x, y = lax.rem(n, nx), n // nx
    z, c = l // 2, lax.rem(l, 2)
    lead = c == 1

    def at_x(v, core=1):
        return (y * nx + v, z * 2 + core)

    def at_y(v, core):
        return (v * nx + x, z * 2 + core)

    up = (n, lax.rem(z + 1, nz) * 2 + 1)
    down = (n, lax.rem(z + nz - 1, nz) * 2 + 1)
    partner = (n, z * 2 + 1 - c)
    xs = [lax.rem(x + d, nx) for d in sorted(range(1, nx), key=lambda d: -min(d, nx - d))]
    ys = [lax.rem(y + d, ny) for d in sorted(range(1, ny), key=lambda d: -min(d, ny - d))]

    steps = hz - 1
    near = 2 * steps - 1
    opposite = near + 2

    def going_up(s):
        return 2 * s - 1

    def going_down(s):
        return 2 * s

    early = z < hz

    def across(core):
        return (n, lax.rem(z + hz, nz) * 2 + core)

    def push(src, dst, send, recv, device):
        pltpu.make_async_remote_copy(
            src_ref=src, dst_ref=dst, send_sem=send, recv_sem=recv,
            device_id=device, device_id_type=MESH_ID,
        ).start()

    def await_bytes(ref, sem):
        pltpu.make_async_copy(ref, ref, sem).wait()

    def signal(sem, device):
        pl.semaphore_signal(sem, 1, device_id=device, device_id_type=MESH_ID)

    def part(q):
        return pl.ds(offs[q], lens[q])

    def cols(q):
        return pl.ds(starts[q], widths[q])

    def data(q):
        return pl.ds(META + starts[q], widths[q])

    main, other = range(CHUNKS - OTHER), range(CHUNKS - OTHER, CHUNKS)
    split = starts[len(main)]
    main_part, main_cols = pl.ds(0, META + split), pl.ds(0, split)
    other_part = pl.ds(META + split, half - split)
    ring_order = list(main[:1]) + [q for pair in zip(other, main[1:]) for q in pair] + list(main[1 + OTHER :])
    back_order = [*main[:2], other[0], main[2], other[1], *main[3:]]

    def own(q):
        return pl.ds(starts[q] - split, widths[q])

    barrier = pltpu.get_barrier_semaphore()
    with scope("entry"):
        signal(barrier, partner)
        for v in ys:
            signal(barrier, at_y(v, 1))
            signal(barrier, at_y(v, 0))
        for v in xs:
            signal(barrier, at_x(v, 0))
            signal(barrier, at_x(v, 1))

        @pl.when(lead)
        def _():
            signal(barrier, up)
            signal(barrier, down)

        @pl.when(early)
        def _():
            signal(barrier, across(0))

            @pl.when(jnp.logical_not(lead))
            def _():
                signal(barrier, across(1))

        inputs = [
            pltpu.make_async_copy(tok_ref, tokv, in_sem.at[0]),
            pltpu.make_async_copy(ids_ref, idsv, in_sem.at[1]),
            pltpu.make_async_copy(gates_ref, gatesv, in_sem.at[2]),
        ]
        for copy in inputs:
            copy.start()
        for h in range(2):
            wcols = pl.ds(h * half, half)
            pltpu.make_async_copy(wg_ref.at[:, :, wcols], wgu.at[h, 0, 0], wl_sem.at[0]).start()
            pltpu.make_async_copy(wu_ref.at[:, :, wcols], wgu.at[h, 1, 0], wl_sem.at[0]).start()
            pltpu.make_async_copy(wd_ref.at[:, :, wcols], wdn.at[h, 0], wl_sem.at[1]).start()

        for copy in inputs:
            copy.wait()
        lane = lax.broadcasted_iota(jnp.int32, (2, META), 1)
        row = lax.broadcasted_iota(jnp.int32, (2, META), 0)
        gates = jnp.zeros((2, META), jnp.int32)
        for k in range(ids_ref.shape[1]):
            gates += jnp.where((lane == idsv[0, k]) & (row == 0), gatesv[0, k], 0)
        tsend[:, 0:META] = gates.astype(F32).astype(BF16)
        tok = tokv[...].astype(F32)
        tsend[:, META:] = jnp.concatenate([tok[:, :half], tok[:, half:]], axis=0).astype(BF16)

        @pl.when(lead)
        def _():
            t1[y * 2 + 1] = tsend[...]
            a1[x * 2 + 1] = tsend[:, other_part]

        @pl.when(jnp.logical_not(lead))
        def _():
            ftok[0] = tsend[...]

    with scope("bar"):
        count = 1 + 2 * (ny - 1) + 2 * (nx - 1) + 2 * c + (z // hz) * (2 - c)
        pl.semaphore_wait(barrier, count)

        @pl.when(jnp.logical_not(early))
        def _():
            signal(ready, across(0))

    with scope("ypush"):
        for q in other:
            for v in xs:
                push(tsend.at[:, part(q)], a1.at[x * 2 + c, :, own(q)], so.at[0], r1.at[q], at_x(v))

            @pl.when(jnp.logical_not(lead))
            def _():
                push(tsend.at[:, part(q)], a1.at[x * 2 + c, :, own(q)], s0, r1.at[q], partner)

        for q in main:
            for v in ys:
                push(tsend.at[:, part(q)], t1.at[y * 2 + c, :, part(q)], s1, r1.at[q], at_y(v, 1))

            @pl.when(jnp.logical_not(lead))
            def _():
                push(tsend.at[:, part(q)], t1.at[y * 2 + c, :, part(q)], s0, r1.at[q], partner)

        @pl.when(lead)
        def _():
            push(tsend, ftok.at[1], fs.at[0], fr.at[6], partner)

        for h in range(2):
            wcols = pl.ds(h * half, half)
            push(wg_ref.at[:, :, wcols], wgu.at[h, 0, 1], ws_sem.at[0], wr_sem.at[0], partner)
            push(wu_ref.at[:, :, wcols], wgu.at[h, 1, 1], ws_sem.at[0], wr_sem.at[0], partner)
            push(wd_ref.at[:, :, wcols], wdn.at[h, 1], ws_sem.at[1], wr_sem.at[1], partner)

    cells = nx * ny * 2

    def order(i):
        return ((i // 2) % ny) * nx + i // (2 * ny)

    def picker(field, col, side):
        i0 = lax.broadcasted_iota(jnp.int32, (cells, cells), 0)
        i1 = lax.broadcasted_iota(jnp.int32, (cells, cells), 1)
        same = ones(i0 // 2 == i1 // 2)
        own = ones(lax.broadcasted_iota(jnp.int32, (rows, META), 1) // 2 == n)
        meta = field[:, col, :, 0:META].reshape(cells, META)
        if side == 0:
            total = lax.dot_general(own, meta, NT, preferred_element_type=F32)
            hit = ones(total > 0)
            rank = jnp.dot(hit, ones(order(i0) < order(i1)), preferred_element_type=F32)
            hit = jnp.dot(hit, same, preferred_element_type=F32)
            shape = (rows, cells)
        else:
            total = lax.dot_general(meta, own, NT, preferred_element_type=F32)
            hit = ones(total > 0)
            rank = jnp.dot(ones(order(i1) < order(i0)), hit, preferred_element_type=F32)
            hit = jnp.dot(same, hit, preferred_element_type=F32)
            shape = (cells, rows)
        r = lax.broadcasted_iota(jnp.int32, shape, side)
        i = lax.broadcasted_iota(jnp.int32, shape, 1 - side)
        picks = ones((hit > 0) & (rank == (r // 2).astype(F32)) & (r % 2 == i % 2))
        if side == 1:
            return picks
        own_row = (r // CAP == col) & (rank == (r % CAP).astype(F32))
        gates = jnp.dot(ones((hit > 0) & own_row & (i % 2 == 0)), meta, preferred_element_type=F32)
        return picks, gates

    def weights_here():
        await_bytes(wgu.at[:, :, 0], wl_sem.at[0])
        await_bytes(wdn.at[:, 0], wl_sem.at[1])
        await_bytes(wgu.at[:, :, 1], wr_sem.at[0])
        await_bytes(wdn.at[:, 1], wr_sem.at[1])

    def gate_up(start, blocks, q):
        count = blocks * 2 * rows
        piece = xbuf[start : start + blocks, :, :, cols(q)].reshape(count, widths[q])
        for h in range(2):
            w = wgu[h, :, :, :, :, cols(q)].reshape(2 * units, widths[q])
            v = lax.dot_general(piece, w, NT, preferred_element_type=F32)
            for k in range(2):
                if q == 0:
                    zbuf[h, k, 0:count] = v[:, k * units : (k + 1) * units]
                else:
                    zbuf[h, k, 0:count] += v[:, k * units : (k + 1) * units]

    def activations(start, blocks):
        count = blocks * 2 * rows
        lane = lax.broadcasted_iota(jnp.int32, (META, units), 0)
        unit = lax.broadcasted_iota(jnp.int32, (META, units), 1)
        chosen = ones(lane == 2 * n + (unit // ffl) % 2)
        gate_rows = gbuf[start : start + blocks].reshape(count // 2, META)
        scale = jnp.dot(gate_rows, chosen, preferred_element_type=F32) / 8.0
        even, odd = pl.ds(0, count // 2, 2), pl.ds(1, count // 2, 2)
        gate_act = zbuf[0, 0, even, :] + zbuf[1, 0, odd, :]
        up_act = zbuf[0, 1, even, :] + zbuf[1, 1, odd, :]
        hidden = gate_act / (1.0 + jnp.exp(-gate_act)) * up_act * scale
        none = jnp.zeros_like(hidden)
        hbuf[0, even, :] = hidden
        hbuf[1, even, :] = none
        hbuf[0, odd, :] = none
        hbuf[1, odd, :] = hidden
        return jnp.concatenate([hbuf[0, 0:count], hbuf[1, 0:count]], axis=1).astype(BF16)

    def project(hidden, q):
        w = wdn[:, :, :, :, cols(q)].reshape(2 * units, widths[q])
        return jnp.dot(hidden, w, preferred_element_type=F32)

    def arrival(k):
        return k % 3

    def slot(direction, step):
        return direction * steps + step - 1

    @pl.when(jnp.logical_not(lead))
    def _():
        with scope("f_token"):
            @pl.when(early)
            def _():
                pl.semaphore_wait(ready, 2)

            await_bytes(ftok.at[1], fr.at[6])
            push(ftok, ft1.at[y], fs.at[0], fr.at[0], across(0))
        with scope("f_y"):
            await_bytes(ft1.at[y], fr.at[0])
            for v in ys:
                push(ft1.at[y], ft1.at[y], fs.at[1], fr.at[1], at_y(v, 0))
        with scope("f_x"):
            await_bytes(ft1.at[0 : ny - 1], fr.at[1])
            for v in range(ny):
                for col in range(2):
                    ft2[x, col, 2 * v : 2 * v + 2] = ft1[v, col]
            for v in xs:
                push(ft2.at[x], ft2.at[x], fs.at[2], fr.at[2], at_x(v, 0))
        with scope("s_wait"):
            weights_here()
        for batch, (start, blocks) in enumerate(((0, near - 2), (near - 2, 2))):
            with scope(f"s_wait{batch}"):
                await_bytes(xbuf.at[start : start + blocks], rx.at[batch])
                await_bytes(gbuf.at[start : start + blocks], gx.at[batch])
            with scope(f"s_comp{batch}"):
                for q in range(CHUNKS):
                    gate_up(start, blocks, q)
                hidden = activations(start, blocks)
                for q in range(CHUNKS):
                    v = project(hidden, q).astype(BF16).reshape(blocks, 2, rows, widths[q])
                    pnear[start : start + blocks, :, :, cols(q)] = v
        for b in range(near - 1, -1, -1):
            push(pnear.at[b], pnear.at[b], sp, rp.at[(b + 1) // 2], partner)
        with scope("f_pack"):
            await_bytes(ft2.at[0 : nx - 1], fr.at[2])
            picked = [picker(ft2, col, 0) for col in range(2)]
            gbuf[opposite] = (picked[0][1] + picked[1][1]).astype(BF16)
            for col in range(2):
                for q in range(CHUNKS):
                    field = ft2[:, col, :, data(q)].reshape(cells, widths[q])
                    rows_q = jnp.dot(picked[col][0], field, preferred_element_type=F32)
                    xbuf[opposite, col, :, cols(q)] = rows_q.astype(BF16)
            for q in range(CHUNKS):
                gate_up(opposite, 1, q)
            hidden = activations(opposite, 1)
        with scope("f_retx"):
            pickers = [picker(ft2, col, 1) for col in range(2)]
            for q in range(CHUNKS):
                v = project(hidden, q).astype(BF16).reshape(2, rows, widths[q])
                for col in range(2):
                    placed = jnp.dot(pickers[col], v[col], preferred_element_type=F32)
                    fxs[:, col, :, cols(q)] = placed.astype(BF16).reshape(nx, 2 * ny, widths[q])
            for v in xs:
                push(fxs.at[v], fxr.at[x], fs.at[3], fr.at[3], at_x(v, 0))
        with scope("f_rety"):
            await_bytes(fxr.at[0 : nx - 1], fr.at[3])
            for q in range(CHUNKS):
                total = fxs[x, :, :, cols(q)].astype(F32)
                for v in xs:
                    total += fxr[v, :, :, cols(q)].astype(F32)
                total = total.astype(BF16)
                for v in range(ny):
                    for col in range(2):
                        fys[v, col, :, cols(q)] = total[col, 2 * v : 2 * v + 2, :]
            for v in ys:
                push(fys.at[v], fyr.at[y], fs.at[4], fr.at[4], at_y(v, 0))
        with scope("f_retz"):
            await_bytes(fyr.at[0 : ny - 1], fr.at[4])
            for q in range(CHUNKS):
                total = fys[y, :, :, cols(q)].astype(F32)
                for v in ys:
                    total += fyr[v, :, :, cols(q)].astype(F32)
                fzs[:, :, cols(q)] = total.astype(BF16)
            for core in range(2):
                push(fzs.at[core], fin, fs.at[5], fr.at[5], across(core))

    def hop(s, q):
        for direction, b, later, device in (
            (0, going_up(s), going_up(s + 1), up),
            (1, going_down(s), going_down(s + 1), down),
        ):
            batch = 1 if s == steps - 1 else 0
            if q == ring_order[0]:
                await_bytes(gbuf.at[b], gr.at[arrival(s), direction])
                if s < steps:
                    push(gbuf.at[b], gbuf.at[later], gs.at[0], gr.at[arrival(s + 1), direction], device)
                    push(gbuf.at[b], gbuf.at[b], gs.at[1], gx.at[batch], partner)
            block = xbuf.at[b, :, :, cols(q)]
            await_bytes(block, ra.at[arrival(s), direction, q])
            if s < steps:
                push(block, xbuf.at[later, :, :, cols(q)], sa, ra.at[arrival(s + 1), direction, q], device)
                push(block, block, sx, rx.at[batch], partner)

    @pl.when(lead)
    def _():
        with scope("xstage"):
            for q in other:
                await_bytes(a1.at[0 : 2 * nx - 1, :, own(q)], r1.at[q])
                for v in ys:
                    push(a1.at[:, :, own(q)], b1.at[y, :, :, own(q)], so.at[1], r2.at[q], at_y(v, 1))
                b1[y, :, :, own(q)] = a1[:, :, own(q)]
            for q in main:
                await_bytes(t1.at[0 : 2 * ny - 1, :, part(q)], r1.at[q])
                for v in range(ny):
                    for col in range(2):
                        t2[x, col, 2 * v : 2 * v + 2, part(q)] = t1[2 * v + col, :, part(q)]
                for v in xs:
                    block = t2.at[x, :, :, part(q)]
                    push(block, block, s2, r2.at[q], at_x(v))

        with scope("pack"):
            pickers = None
            for q in ring_order:
                if q in main:
                    await_bytes(t2.at[0 : nx - 1, :, :, part(q)], r2.at[q])
                else:
                    await_bytes(b1.at[0 : ny - 1, :, :, own(q)], r2.at[q])
                    for v in range(ny):
                        for j in range(2 * nx):
                            t2[j // 2, j % 2, 2 * v : 2 * v + 2, part(q)] = b1[v, j, :, own(q)]
                if q == 0:
                    picked = [picker(t2, col, 0) for col in range(2)]
                    pickers = [p for p, _ in picked]
                    gbuf[0] = (picked[0][1] + picked[1][1]).astype(BF16)
                    push(gbuf.at[0], gbuf.at[going_up(1)], gs.at[0], gr.at[arrival(1), 0], up)
                    push(gbuf.at[0], gbuf.at[going_down(1)], gs.at[0], gr.at[arrival(1), 1], down)
                    push(gbuf.at[0], gbuf.at[0], gs.at[1], gx.at[0], partner)
                for col in range(2):
                    field = t2[:, col, :, data(q)].reshape(cells, widths[q])
                    rows_q = jnp.dot(pickers[col], field, preferred_element_type=F32)
                    xbuf[0, col, :, cols(q)] = rows_q.astype(BF16)
                block = xbuf.at[0, :, :, cols(q)]
                push(block, xbuf.at[going_up(1), :, :, cols(q)], sa, ra.at[arrival(1), 0, q], up)
                push(block, xbuf.at[going_down(1), :, :, cols(q)], sa, ra.at[arrival(1), 1, q], down)
                push(block, block, sx, rx.at[0], partner)
            weights_here()

        with scope("ring"):
            for s in range(1, steps + 1):
                for q in ring_order:
                    hop(s, q)
                    if s == steps:
                        gate_up(near, 2, q)
        with scope("act"):
            hidden = activations(near, 2)

        def onward(direction, s, q, value, device):
            i = slot(direction, s)
            if s > 1:
                await_bytes(rrecv.at[i - 1, :, :, cols(q)], ra.at[arrival(steps + s - 1), direction, q])
                value = value + rrecv[i - 1, :, :, cols(q)]
            rsend[i, :, :, cols(q)] = value
            push(rsend.at[i, :, :, cols(q)], rrecv.at[i, :, :, cols(q)], ss, ra.at[arrival(steps + s), direction, q], device)

        with scope("rs1"):
            for q in back_order:
                v = project(hidden, q).astype(BF16).reshape(2, 2, rows, widths[q])
                onward(0, 1, q, v[1], up)
                onward(1, 1, q, v[0], down)
        with scope("rs"):
            pickers = [picker(t2, col, 1) for col in range(2)]
            for s in range(2, steps + 1):
                at = steps + 1 - s
                await_bytes(pnear.at[0:2], rp.at[at])
                for q in back_order:
                    onward(0, s, q, pnear[going_down(at), :, :, cols(q)], up)
                    onward(1, s, q, pnear[going_up(at), :, :, cols(q)], down)

        with scope("retx"):
            await_bytes(pnear.at[0], rp.at[0])
            for q in back_order:
                one, two = slot(0, steps), slot(1, steps)
                await_bytes(rrecv.at[two, :, :, cols(q)], ra.at[arrival(2 * steps), 1, q])
                await_bytes(rrecv.at[one, :, :, cols(q)], ra.at[arrival(2 * steps), 0, q])
                total = pnear[0, :, :, cols(q)].astype(F32) + rrecv[one, :, :, cols(q)].astype(F32)
                total = (total + rrecv[two, :, :, cols(q)].astype(F32)).astype(BF16)
                for col in range(2):
                    placed = jnp.dot(pickers[col], total[col], preferred_element_type=F32).astype(BF16)
                    if q in main:
                        ysend[:, col, :, cols(q)] = placed.reshape(nx, 2 * ny, widths[q])
                    else:
                        for i in range(nx * ny):
                            c1[i % ny, 2 * (i // ny) + col, :, own(q)] = placed[2 * i : 2 * i + 2, :]
                if q in main:
                    for turn in range(2):
                        for v in xs:
                            @pl.when(v == 0 if turn == 0 else v > 0)
                            def _():
                                push(ysend.at[v, :, :, cols(q)], yrecv.at[x, :, :, cols(q)], s3, r1.at[q], at_x(v))
                else:
                    for v in ys:
                        push(c1.at[v, :, :, own(q)], c2.at[y, :, :, own(q)], so.at[2], r1.at[q], at_y(v, 1))
        with scope("rety"):
            for q in main:
                await_bytes(yrecv.at[0 : nx - 1, :, :, cols(q)], r1.at[q])
                total = ysend[x, :, :, cols(q)].astype(F32)
                for v in xs:
                    total += yrecv[v, :, :, cols(q)].astype(F32)
                total = total.astype(BF16)
                for v in range(ny):
                    for col in range(2):
                        fsend[v, col, :, cols(q)] = total[col, 2 * v : 2 * v + 2, :]
                for turn in range(2):
                    for v in ys:
                        @pl.when(v == 0 if turn == 0 else v > 0)
                        def _():
                            for col in (1, 0):
                                push(fsend.at[v, col, :, cols(q)], frecv.at[y, :, cols(q)], s4, r4.at[q], at_y(v, col))
                push(fsend.at[y, 0, :, cols(q)], frecv.at[y, :, cols(q)], s0, r4.at[q], partner)
                frecv[y, :, cols(q)] = fsend[y, 1, :, cols(q)]
            for q in other:
                await_bytes(c2.at[0 : ny - 1, :, :, own(q)], r1.at[q])
                total = c1[y, :, :, own(q)].astype(F32)
                for v in ys:
                    total += c2[v, :, :, own(q)].astype(F32)
                e1[:, :, own(q)] = total.astype(BF16)
                for v in xs:
                    for col in range(2):
                        push(e1.at[2 * v + col, :, own(q)], e2.at[x, :, own(q)], so.at[3], r4.at[q], at_x(v, col))
                push(e1.at[2 * x, :, own(q)], e2.at[x, :, own(q)], so.at[4], r4.at[q], partner)
                e2[x, :, own(q)] = e1[2 * x + 1, :, own(q)]

    with scope("final"):
        await_bytes(fin, fr.at[5])
        for q in range(CHUNKS):
            parts, mine, count = (frecv, cols(q), ny) if q in main else (e2, own(q), nx)

            @pl.when(lead)
            def _():
                await_bytes(parts.at[0 : count - 1, :, mine], r4.at[q])

            @pl.when(jnp.logical_not(lead))
            def _():
                await_bytes(parts.at[:, :, mine], r4.at[q])

            total = fin[:, cols(q)].astype(F32)
            for v in range(count):
                total += parts[v, :, mine].astype(F32)
            total = total.astype(BF16)
            outv[0:1, cols(q)] = total[0:1, :]
            outv[0:1, pl.ds(half + starts[q], widths[q])] = total[1:2, :]

    result = pltpu.make_async_copy(outv, out_ref, out_sem)
    result.start()

    with scope("drain"):
        await_bytes(t1.at[0 : ny - 1, :, main_part], s1)
        await_bytes(a1.at[0 : nx - 1], so.at[0])
        await_bytes(wgu.at[:, :, 1], ws_sem.at[0])
        await_bytes(wdn.at[:, 1], ws_sem.at[1])

        @pl.when(jnp.logical_not(lead))
        def _():
            await_bytes(tsend, s0)
            await_bytes(pnear, sp)
            await_bytes(ftok, fs.at[0])
            await_bytes(ft1.at[0 : ny - 1], fs.at[1])
            await_bytes(ft2.at[0 : nx - 1], fs.at[2])
            await_bytes(fxs.at[0 : nx - 1], fs.at[3])
            await_bytes(fys.at[0 : ny - 1], fs.at[4])
            await_bytes(fzs, fs.at[5])

        @pl.when(lead)
        def _():
            await_bytes(t2.at[0 : nx - 1, :, :, main_part], s2)
            await_bytes(b1.at[0 : ny - 1], so.at[1])
            await_bytes(c2.at[0 : ny - 1], so.at[2])
            await_bytes(e1.at[0 : 2 * (nx - 1)], so.at[3])
            await_bytes(e1.at[0], so.at[4])
            await_bytes(xbuf.at[0 : 2 * steps], sa)
            await_bytes(xbuf.at[0:near], sx)
            await_bytes(gbuf.at[0 : 2 * steps], gs.at[0])
            await_bytes(gbuf.at[0:near], gs.at[1])
            await_bytes(rsend, ss)
            await_bytes(yrecv.at[0 : nx - 1, :, :, main_cols], s3)
            await_bytes(fsend.at[0 : ny - 1, :, :, main_cols], s4)
            await_bytes(frecv.at[0, :, main_cols], s0)
            await_bytes(tsend, fs.at[0])

        result.wait()


def solution(mesh):
    nodes, locals_ = mesh.shape["node"], mesh.shape["local"]
    nx = min(NX, nodes)
    ny, nz = nodes // nx, locals_ // 2
    hz = nz // 2
    steps = hz - 1
    near = 2 * steps - 1

    def on_device(tokens, w_gate, w_up, w_down, expert_ids, gate_ints):
        model_width = tokens.shape[1]
        half = model_width // 2
        exp_node, ffl = w_gate.shape[0], w_gate.shape[1]
        units = 2 * exp_node * ffl
        rows = 2 * CAP
        lanes = half * sum(PARTS[-OTHER:]) // sum(PARTS)
        sem = pltpu.SemaphoreType.DMA
        one = sem(())
        any_space = pl.BlockSpec(memory_space=pl.ANY)
        vmem = pl.BlockSpec(memory_space=pltpu.VMEM)
        return pl.pallas_call(
            functools.partial(layer_kernel, nx, ny, nz),
            out_shape=jax.ShapeDtypeStruct((1, model_width), BF16),
            in_specs=[any_space] * 6,
            out_specs=any_space,
            scratch_shapes=[
                pltpu.VMEM((1, model_width), BF16),
                pltpu.SMEM(expert_ids.shape, jnp.int32),
                pltpu.SMEM(gate_ints.shape, jnp.int32),
                pltpu.VMEM((2, META + half), BF16),
                pltpu.VMEM((2 * ny, 2, META + half), BF16),
                pltpu.VMEM((nx, 2, 2 * ny, META + half), BF16),
                pltpu.VMEM((nz, 2, rows, half), BF16),
                pltpu.VMEM((2, 2, 2, exp_node, ffl, half), BF16),
                pltpu.VMEM((2, 2, exp_node, ffl, half), BF16),
                pltpu.VMEM((2, 2, near * 2 * rows, units), F32),
                pltpu.VMEM((2, near * 2 * rows, units), F32),
                pltpu.VMEM((near, 2, rows, half), BF16),
                pltpu.VMEM((2 * steps, 2, rows, half), BF16),
                pltpu.VMEM((2 * steps, 2, rows, half), BF16),
                pltpu.VMEM((nx, 2, 2 * ny, half), BF16),
                pltpu.VMEM((nx, 2, 2 * ny, half), BF16),
                pltpu.VMEM((ny, 2, 2, half), BF16),
                pltpu.VMEM((ny, 2, half), BF16),
                pltpu.VMEM((2, 2, META + half), BF16),
                pltpu.VMEM((ny, 2, 2, META + half), BF16),
                pltpu.VMEM((nx, 2, 2 * ny, META + half), BF16),
                pltpu.VMEM((nx, 2, 2 * ny, half), BF16),
                pltpu.VMEM((nx, 2, 2 * ny, half), BF16),
                pltpu.VMEM((ny, 2, 2, half), BF16),
                pltpu.VMEM((ny, 2, 2, half), BF16),
                pltpu.VMEM((2, 2, half), BF16),
                pltpu.VMEM((2, half), BF16),
                pltpu.VMEM((2 * nx, 2, lanes), BF16),
                pltpu.VMEM((ny, 2 * nx, 2, lanes), BF16),
                pltpu.VMEM((ny, 2 * nx, 2, lanes), BF16),
                pltpu.VMEM((ny, 2 * nx, 2, lanes), BF16),
                pltpu.VMEM((2 * nx, 2, lanes), BF16),
                pltpu.VMEM((nx, 2, lanes), BF16),
                pltpu.VMEM((nz, rows, META), BF16),
                sem((3,)), sem((2,)), sem((2,)), sem((2,)),
                one, one, sem((CHUNKS,)), one, sem((CHUNKS,)),
                one, sem((3, 2, CHUNKS)), one, sem((2,)), one, sem((steps,)),
                one, one, one, sem((CHUNKS,)),
                sem((6,)), sem((7,)), pltpu.SemaphoreType.REGULAR, sem((5,)),
                pltpu.VMEM((1, model_width), BF16), one,
                sem((2,)), sem((3, 2)), sem((2,)),
            ],
            compiler_params=pltpu.CompilerParams(
                collective_id=0, has_side_effects=True, vmem_limit_bytes=44 * 1024 * 1024
            ),
            name="layer",
        )(*(pltpu.with_memory_space_constraint(a, pltpu.HBM) for a in (tokens, w_gate, w_up, w_down, expert_ids, gate_ints)))

    both = P(("node", "local"), None)
    weights = P("node", "local", None)
    return jax.shard_map(
        on_device, mesh=mesh,
        in_specs=(both, weights, weights, weights, both, both),
        out_specs=both, check_vma=False,
    )
```

```python
import functools

import jax
import jax.numpy as jnp
from jax import lax
from jax.experimental import pallas as pl
from jax.experimental.pallas import tpu as pltpu
from jax.sharding import PartitionSpec as P

CAP = 8
NX = 4
PARTS = (4, 4, 4, 4, 4, 4, 4)
CHUNKS = len(PARTS)
OTHER = 2
META = 128
BF16 = jnp.bfloat16
F32 = jnp.float32
MESH_ID = pl.DeviceIdType.MESH
NT = (((1,), (1,)), ((), ()))
scope = jax.named_scope


def ones(mask):
    return mask.astype(F32).astype(BF16)


def layer_kernel(
    nx, ny, nz,
    tok_ref, wg_ref, wu_ref, wd_ref, ids_ref, gates_ref,
    out_ref,
    tokv, idsv, gatesv, tsend, t1, t2, xbuf, wgu, wdn, zbuf, hbuf, pnear, rsend, rrecv,
    ysend, yrecv, fsend, frecv, ftok, ft1, ft2, fxs, fxr, fys, fyr, fzs, fin, a1, b1, c1, c2, e1, e2, gbuf,
    in_sem, wl_sem, ws_sem, wr_sem, s0, s1, r1, s2, r2, sa, ra, sx, rx, sp, rp, ss, s3, s4, r4,
    fs, fr, ready, so, outv, out_sem, gs, gr, gx,
):
    half = wgu.shape[-1]
    widths = [half * part // sum(PARTS) for part in PARTS]
    starts = [sum(widths[:q]) for q in range(CHUNKS + 1)]
    offs = [0] + [META + start for start in starts[1:]]
    lens = [META + widths[0]] + widths[1:]
    hz = nz // 2
    rows = CAP * 2
    ffl = wdn.shape[3]
    units = wdn.shape[1] * wdn.shape[2] * ffl
    n = lax.axis_index("node")
    l = lax.axis_index("local")
    x, y = lax.rem(n, nx), n // nx
    z, c = l // 2, lax.rem(l, 2)
    lead = c == 1

    def at_x(v, core=1):
        return (y * nx + v, z * 2 + core)

    def at_y(v, core):
        return (v * nx + x, z * 2 + core)

    up = (n, lax.rem(z + 1, nz) * 2 + 1)
    down = (n, lax.rem(z + nz - 1, nz) * 2 + 1)
    partner = (n, z * 2 + 1 - c)
    xs = [lax.rem(x + d, nx) for d in sorted(range(1, nx), key=lambda d: -min(d, nx - d))]
    ys = [lax.rem(y + d, ny) for d in sorted(range(1, ny), key=lambda d: -min(d, ny - d))]

    steps = hz - 1
    near = 2 * steps - 1
    opposite = near + 2

    def going_up(s):
        return 2 * s - 1

    def going_down(s):
        return 2 * s

    early = z < hz

    def across(core):
        return (n, lax.rem(z + hz, nz) * 2 + core)

    def push(src, dst, send, recv, device):
        pltpu.make_async_remote_copy(
            src_ref=src, dst_ref=dst, send_sem=send, recv_sem=recv,
            device_id=device, device_id_type=MESH_ID,
        ).start()

    def await_bytes(ref, sem):
        pltpu.make_async_copy(ref, ref, sem).wait()

    def signal(sem, device):
        pl.semaphore_signal(sem, 1, device_id=device, device_id_type=MESH_ID)

    def part(q):
        return pl.ds(offs[q], lens[q])

    def cols(q):
        return pl.ds(starts[q], widths[q])

    def data(q):
        return pl.ds(META + starts[q], widths[q])

    main, other = range(CHUNKS - OTHER), range(CHUNKS - OTHER, CHUNKS)
    split = starts[len(main)]
    main_part, main_cols = pl.ds(0, META + split), pl.ds(0, split)
    other_part = pl.ds(META + split, half - split)
    ring_order = list(main[:1]) + [q for pair in zip(other, main[1:]) for q in pair] + list(main[1 + OTHER :])
    back_order = [*main[:2], other[0], main[2], other[1], *main[3:]]

    def own(q):
        return pl.ds(starts[q] - split, widths[q])

    barrier = pltpu.get_barrier_semaphore()
    with scope("entry"):
        signal(barrier, partner)
        for v in ys:
            signal(barrier, at_y(v, 1))
            signal(barrier, at_y(v, 0))
        for v in xs:
            signal(barrier, at_x(v, 0))
            signal(barrier, at_x(v, 1))

        @pl.when(lead)
        def _():
            signal(barrier, up)
            signal(barrier, down)

        @pl.when(early)
        def _():
            signal(barrier, across(0))

            @pl.when(jnp.logical_not(lead))
            def _():
                signal(barrier, across(1))

        inputs = [
            pltpu.make_async_copy(tok_ref, tokv, in_sem.at[0]),
            pltpu.make_async_copy(ids_ref, idsv, in_sem.at[1]),
            pltpu.make_async_copy(gates_ref, gatesv, in_sem.at[2]),
        ]
        for copy in inputs:
            copy.start()
        for h in range(2):
            wcols = pl.ds(h * half, half)
            pltpu.make_async_copy(wg_ref.at[:, :, wcols], wgu.at[h, 0, 0], wl_sem.at[0]).start()
            pltpu.make_async_copy(wu_ref.at[:, :, wcols], wgu.at[h, 1, 0], wl_sem.at[0]).start()
            pltpu.make_async_copy(wd_ref.at[:, :, wcols], wdn.at[h, 0], wl_sem.at[1]).start()

        for copy in inputs:
            copy.wait()
        lane = lax.broadcasted_iota(jnp.int32, (2, META), 1)
        row = lax.broadcasted_iota(jnp.int32, (2, META), 0)
        gates = jnp.zeros((2, META), jnp.int32)
        for k in range(ids_ref.shape[1]):
            gates += jnp.where((lane == idsv[0, k]) & (row == 0), gatesv[0, k], 0)
        tsend[:, 0:META] = gates.astype(F32).astype(BF16)
        tok = tokv[...].astype(F32)
        tsend[:, META:] = jnp.concatenate([tok[:, :half], tok[:, half:]], axis=0).astype(BF16)

        @pl.when(lead)
        def _():
            t1[y * 2 + 1] = tsend[...]
            a1[x * 2 + 1] = tsend[:, other_part]

        @pl.when(jnp.logical_not(lead))
        def _():
            ftok[0] = tsend[...]

    with scope("bar"):
        count = 1 + 2 * (ny - 1) + 2 * (nx - 1) + 2 * c + (z // hz) * (2 - c)
        pl.semaphore_wait(barrier, count)

        @pl.when(jnp.logical_not(early))
        def _():
            signal(ready, across(0))

    with scope("ypush"):
        for q in other:
            for v in xs:
                push(tsend.at[:, part(q)], a1.at[x * 2 + c, :, own(q)], so.at[0], r1.at[q], at_x(v))

            @pl.when(jnp.logical_not(lead))
            def _():
                push(tsend.at[:, part(q)], a1.at[x * 2 + c, :, own(q)], s0, r1.at[q], partner)

        for q in main:
            for v in ys:
                push(tsend.at[:, part(q)], t1.at[y * 2 + c, :, part(q)], s1, r1.at[q], at_y(v, 1))

            @pl.when(jnp.logical_not(lead))
            def _():
                push(tsend.at[:, part(q)], t1.at[y * 2 + c, :, part(q)], s0, r1.at[q], partner)

        @pl.when(lead)
        def _():
            push(tsend, ftok.at[1], fs.at[0], fr.at[6], partner)

        for h in range(2):
            wcols = pl.ds(h * half, half)
            push(wg_ref.at[:, :, wcols], wgu.at[h, 0, 1], ws_sem.at[0], wr_sem.at[0], partner)
            push(wu_ref.at[:, :, wcols], wgu.at[h, 1, 1], ws_sem.at[0], wr_sem.at[0], partner)
            push(wd_ref.at[:, :, wcols], wdn.at[h, 1], ws_sem.at[1], wr_sem.at[1], partner)

    cells = nx * ny * 2

    def order(i):
        return ((i // 2) % ny) * nx + i // (2 * ny)

    def picker(field, col, side):
        i0 = lax.broadcasted_iota(jnp.int32, (cells, cells), 0)
        i1 = lax.broadcasted_iota(jnp.int32, (cells, cells), 1)
        same = ones(i0 // 2 == i1 // 2)
        own = ones(lax.broadcasted_iota(jnp.int32, (rows, META), 1) // 2 == n)
        meta = field[:, col, :, 0:META].reshape(cells, META)
        if side == 0:
            total = lax.dot_general(own, meta, NT, preferred_element_type=F32)
            hit = ones(total > 0)
            rank = jnp.dot(hit, ones(order(i0) < order(i1)), preferred_element_type=F32)
            hit = jnp.dot(hit, same, preferred_element_type=F32)
            shape = (rows, cells)
        else:
            total = lax.dot_general(meta, own, NT, preferred_element_type=F32)
            hit = ones(total > 0)
            rank = jnp.dot(ones(order(i1) < order(i0)), hit, preferred_element_type=F32)
            hit = jnp.dot(same, hit, preferred_element_type=F32)
            shape = (cells, rows)
        r = lax.broadcasted_iota(jnp.int32, shape, side)
        i = lax.broadcasted_iota(jnp.int32, shape, 1 - side)
        picks = ones((hit > 0) & (rank == (r // 2).astype(F32)) & (r % 2 == i % 2))
        if side == 1:
            return picks
        own_row = (r // CAP == col) & (rank == (r % CAP).astype(F32))
        gates = jnp.dot(ones((hit > 0) & own_row & (i % 2 == 0)), meta, preferred_element_type=F32)
        return picks, gates

    def weights_here():
        await_bytes(wgu.at[:, :, 0], wl_sem.at[0])
        await_bytes(wdn.at[:, 0], wl_sem.at[1])
        await_bytes(wgu.at[:, :, 1], wr_sem.at[0])
        await_bytes(wdn.at[:, 1], wr_sem.at[1])

    def gate_up(start, blocks, q):
        count = blocks * 2 * rows
        piece = xbuf[start : start + blocks, :, :, cols(q)].reshape(count, widths[q])
        for h in range(2):
            w = wgu[h, :, :, :, :, cols(q)].reshape(2 * units, widths[q])
            v = lax.dot_general(piece, w, NT, preferred_element_type=F32)
            for k in range(2):
                if q == 0:
                    zbuf[h, k, 0:count] = v[:, k * units : (k + 1) * units]
                else:
                    zbuf[h, k, 0:count] += v[:, k * units : (k + 1) * units]

    def activations(start, blocks):
        count = blocks * 2 * rows
        lane = lax.broadcasted_iota(jnp.int32, (META, units), 0)
        unit = lax.broadcasted_iota(jnp.int32, (META, units), 1)
        chosen = ones(lane == 2 * n + (unit // ffl) % 2)
        gate_rows = gbuf[start : start + blocks].reshape(count // 2, META)
        scale = jnp.dot(gate_rows, chosen, preferred_element_type=F32) / 8.0
        even, odd = pl.ds(0, count // 2, 2), pl.ds(1, count // 2, 2)
        gate_act = zbuf[0, 0, even, :] + zbuf[1, 0, odd, :]
        up_act = zbuf[0, 1, even, :] + zbuf[1, 1, odd, :]
        hidden = gate_act / (1.0 + jnp.exp(-gate_act)) * up_act * scale
        none = jnp.zeros_like(hidden)
        hbuf[0, even, :] = hidden
        hbuf[1, even, :] = none
        hbuf[0, odd, :] = none
        hbuf[1, odd, :] = hidden
        return jnp.concatenate([hbuf[0, 0:count], hbuf[1, 0:count]], axis=1).astype(BF16)

    def project(hidden, q):
        w = wdn[:, :, :, :, cols(q)].reshape(2 * units, widths[q])
        return jnp.dot(hidden, w, preferred_element_type=F32)

    def arrival(k):
        return k % 3

    def slot(direction, step):
        return direction * steps + step - 1

    @pl.when(jnp.logical_not(lead))
    def _():
        with scope("f_token"):
            @pl.when(early)
            def _():
                pl.semaphore_wait(ready, 2)

            await_bytes(ftok.at[1], fr.at[6])
            push(ftok, ft1.at[y], fs.at[0], fr.at[0], across(0))
        with scope("f_y"):
            await_bytes(ft1.at[y], fr.at[0])
            for v in ys:
                push(ft1.at[y], ft1.at[y], fs.at[1], fr.at[1], at_y(v, 0))
        with scope("f_x"):
            await_bytes(ft1.at[0 : ny - 1], fr.at[1])
            for v in range(ny):
                for col in range(2):
                    ft2[x, col, 2 * v : 2 * v + 2] = ft1[v, col]
            for v in xs:
                push(ft2.at[x], ft2.at[x], fs.at[2], fr.at[2], at_x(v, 0))
        with scope("s_wait"):
            weights_here()
        for batch, (start, blocks) in enumerate(((0, near - 2), (near - 2, 2))):
            with scope(f"s_wait{batch}"):
                await_bytes(xbuf.at[start : start + blocks], rx.at[batch])
                await_bytes(gbuf.at[start : start + blocks], gx.at[batch])
            with scope(f"s_comp{batch}"):
                for q in range(CHUNKS):
                    gate_up(start, blocks, q)
                hidden = activations(start, blocks)
                for q in range(CHUNKS):
                    v = project(hidden, q).astype(BF16).reshape(blocks, 2, rows, widths[q])
                    pnear[start : start + blocks, :, :, cols(q)] = v
        for b in range(near - 1, -1, -1):
            push(pnear.at[b], pnear.at[b], sp, rp.at[(b + 1) // 2], partner)
        with scope("f_pack"):
            await_bytes(ft2.at[0 : nx - 1], fr.at[2])
            picked = [picker(ft2, col, 0) for col in range(2)]
            gbuf[opposite] = (picked[0][1] + picked[1][1]).astype(BF16)
            for col in range(2):
                for q in range(CHUNKS):
                    field = ft2[:, col, :, data(q)].reshape(cells, widths[q])
                    rows_q = jnp.dot(picked[col][0], field, preferred_element_type=F32)
                    xbuf[opposite, col, :, cols(q)] = rows_q.astype(BF16)
            for q in range(CHUNKS):
                gate_up(opposite, 1, q)
            hidden = activations(opposite, 1)
        with scope("f_retx"):
            pickers = [picker(ft2, col, 1) for col in range(2)]
            for q in range(CHUNKS):
                v = project(hidden, q).astype(BF16).reshape(2, rows, widths[q])
                for col in range(2):
                    placed = jnp.dot(pickers[col], v[col], preferred_element_type=F32)
                    fxs[:, col, :, cols(q)] = placed.astype(BF16).reshape(nx, 2 * ny, widths[q])
            for v in xs:
                push(fxs.at[v], fxr.at[x], fs.at[3], fr.at[3], at_x(v, 0))
        with scope("f_rety"):
            await_bytes(fxr.at[0 : nx - 1], fr.at[3])
            for q in range(CHUNKS):
                total = fxs[x, :, :, cols(q)].astype(F32)
                for v in xs:
                    total += fxr[v, :, :, cols(q)].astype(F32)
                total = total.astype(BF16)
                for v in range(ny):
                    for col in range(2):
                        fys[v, col, :, cols(q)] = total[col, 2 * v : 2 * v + 2, :]
            for v in ys:
                push(fys.at[v], fyr.at[y], fs.at[4], fr.at[4], at_y(v, 0))
        with scope("f_retz"):
            await_bytes(fyr.at[0 : ny - 1], fr.at[4])
            for q in range(CHUNKS):
                total = fys[y, :, :, cols(q)].astype(F32)
                for v in ys:
                    total += fyr[v, :, :, cols(q)].astype(F32)
                fzs[:, :, cols(q)] = total.astype(BF16)
            for core in range(2):
                push(fzs.at[core], fin, fs.at[5], fr.at[5], across(core))

    def hop(s, q):
        for direction, b, later, device in (
            (0, going_up(s), going_up(s + 1), up),
            (1, going_down(s), going_down(s + 1), down),
        ):
            batch = 1 if s == steps - 1 else 0
            if q == ring_order[0]:
                await_bytes(gbuf.at[b], gr.at[arrival(s), direction])
                if s < steps:
                    push(gbuf.at[b], gbuf.at[later], gs.at[0], gr.at[arrival(s + 1), direction], device)
                    push(gbuf.at[b], gbuf.at[b], gs.at[1], gx.at[batch], partner)
            block = xbuf.at[b, :, :, cols(q)]
            await_bytes(block, ra.at[arrival(s), direction, q])
            if s < steps:
                push(block, xbuf.at[later, :, :, cols(q)], sa, ra.at[arrival(s + 1), direction, q], device)
                push(block, block, sx, rx.at[batch], partner)

    @pl.when(lead)
    def _():
        with scope("xstage"):
            for q in other:
                await_bytes(a1.at[0 : 2 * nx - 1, :, own(q)], r1.at[q])
                for v in ys:
                    push(a1.at[:, :, own(q)], b1.at[y, :, :, own(q)], so.at[1], r2.at[q], at_y(v, 1))
                b1[y, :, :, own(q)] = a1[:, :, own(q)]
            for q in main:
                await_bytes(t1.at[0 : 2 * ny - 1, :, part(q)], r1.at[q])
                for v in range(ny):
                    for col in range(2):
                        t2[x, col, 2 * v : 2 * v + 2, part(q)] = t1[2 * v + col, :, part(q)]
                for v in xs:
                    block = t2.at[x, :, :, part(q)]
                    push(block, block, s2, r2.at[q], at_x(v))

        with scope("pack"):
            pickers = None
            for q in ring_order:
                if q in main:
                    await_bytes(t2.at[0 : nx - 1, :, :, part(q)], r2.at[q])
                else:
                    await_bytes(b1.at[0 : ny - 1, :, :, own(q)], r2.at[q])
                    for v in range(ny):
                        for j in range(2 * nx):
                            t2[j // 2, j % 2, 2 * v : 2 * v + 2, part(q)] = b1[v, j, :, own(q)]
                if q == 0:
                    picked = [picker(t2, col, 0) for col in range(2)]
                    pickers = [p for p, _ in picked]
                for col in range(2):
                    field = t2[:, col, :, data(q)].reshape(cells, widths[q])
                    rows_q = jnp.dot(pickers[col], field, preferred_element_type=F32)
                    xbuf[0, col, :, cols(q)] = rows_q.astype(BF16)
                block = xbuf.at[0, :, :, cols(q)]
                push(block, xbuf.at[going_up(1), :, :, cols(q)], sa, ra.at[arrival(1), 0, q], up)
                push(block, xbuf.at[going_down(1), :, :, cols(q)], sa, ra.at[arrival(1), 1, q], down)
                push(block, block, sx, rx.at[0], partner)
                if q == 0:
                    gbuf[0] = (picked[0][1] + picked[1][1]).astype(BF16)
                    push(gbuf.at[0], gbuf.at[going_up(1)], gs.at[0], gr.at[arrival(1), 0], up)
                    push(gbuf.at[0], gbuf.at[going_down(1)], gs.at[0], gr.at[arrival(1), 1], down)
                    push(gbuf.at[0], gbuf.at[0], gs.at[1], gx.at[0], partner)
            weights_here()

        with scope("ring"):
            for s in range(1, steps + 1):
                for q in ring_order:
                    hop(s, q)
                    if s == steps:
                        gate_up(near, 2, q)
        with scope("act"):
            hidden = activations(near, 2)

        def onward(direction, s, q, value, device):
            i = slot(direction, s)
            if s > 1:
                await_bytes(rrecv.at[i - 1, :, :, cols(q)], ra.at[arrival(steps + s - 1), direction, q])
                value = value + rrecv[i - 1, :, :, cols(q)]
            rsend[i, :, :, cols(q)] = value
            push(rsend.at[i, :, :, cols(q)], rrecv.at[i, :, :, cols(q)], ss, ra.at[arrival(steps + s), direction, q], device)

        with scope("rs1"):
            for q in back_order:
                v = project(hidden, q).astype(BF16).reshape(2, 2, rows, widths[q])
                onward(0, 1, q, v[1], up)
                onward(1, 1, q, v[0], down)
        with scope("rs"):
            pickers = [picker(t2, col, 1) for col in range(2)]
            for s in range(2, steps + 1):
                at = steps + 1 - s
                await_bytes(pnear.at[0:2], rp.at[at])
                for q in back_order:
                    onward(0, s, q, pnear[going_down(at), :, :, cols(q)], up)
                    onward(1, s, q, pnear[going_up(at), :, :, cols(q)], down)

        with scope("retx"):
            await_bytes(pnear.at[0], rp.at[0])
            for q in back_order:
                one, two = slot(0, steps), slot(1, steps)
                await_bytes(rrecv.at[two, :, :, cols(q)], ra.at[arrival(2 * steps), 1, q])
                await_bytes(rrecv.at[one, :, :, cols(q)], ra.at[arrival(2 * steps), 0, q])
                total = pnear[0, :, :, cols(q)].astype(F32) + rrecv[one, :, :, cols(q)].astype(F32)
                total = (total + rrecv[two, :, :, cols(q)].astype(F32)).astype(BF16)
                for col in range(2):
                    placed = jnp.dot(pickers[col], total[col], preferred_element_type=F32).astype(BF16)
                    if q in main:
                        ysend[:, col, :, cols(q)] = placed.reshape(nx, 2 * ny, widths[q])
                    else:
                        for i in range(nx * ny):
                            c1[i % ny, 2 * (i // ny) + col, :, own(q)] = placed[2 * i : 2 * i + 2, :]
                if q in main:
                    for turn in range(2):
                        for v in xs:
                            @pl.when(v == 0 if turn == 0 else v > 0)
                            def _():
                                push(ysend.at[v, :, :, cols(q)], yrecv.at[x, :, :, cols(q)], s3, r1.at[q], at_x(v))
                else:
                    for v in ys:
                        push(c1.at[v, :, :, own(q)], c2.at[y, :, :, own(q)], so.at[2], r1.at[q], at_y(v, 1))
        with scope("rety"):
            for q in main:
                await_bytes(yrecv.at[0 : nx - 1, :, :, cols(q)], r1.at[q])
                total = ysend[x, :, :, cols(q)].astype(F32)
                for v in xs:
                    total += yrecv[v, :, :, cols(q)].astype(F32)
                total = total.astype(BF16)
                for v in range(ny):
                    for col in range(2):
                        fsend[v, col, :, cols(q)] = total[col, 2 * v : 2 * v + 2, :]
                for turn in range(2):
                    for v in ys:
                        @pl.when(v == 0 if turn == 0 else v > 0)
                        def _():
                            for col in (1, 0):
                                push(fsend.at[v, col, :, cols(q)], frecv.at[y, :, cols(q)], s4, r4.at[q], at_y(v, col))
                push(fsend.at[y, 0, :, cols(q)], frecv.at[y, :, cols(q)], s0, r4.at[q], partner)
                frecv[y, :, cols(q)] = fsend[y, 1, :, cols(q)]
            for q in other:
                await_bytes(c2.at[0 : ny - 1, :, :, own(q)], r1.at[q])
                total = c1[y, :, :, own(q)].astype(F32)
                for v in ys:
                    total += c2[v, :, :, own(q)].astype(F32)
                e1[:, :, own(q)] = total.astype(BF16)
                for v in xs:
                    for col in range(2):
                        push(e1.at[2 * v + col, :, own(q)], e2.at[x, :, own(q)], so.at[3], r4.at[q], at_x(v, col))
                push(e1.at[2 * x, :, own(q)], e2.at[x, :, own(q)], so.at[4], r4.at[q], partner)
                e2[x, :, own(q)] = e1[2 * x + 1, :, own(q)]

    with scope("final"):
        await_bytes(fin, fr.at[5])
        for q in [*main[:-1], *other, main[-1]]:
            parts, mine, count = (frecv, cols(q), ny) if q in main else (e2, own(q), nx)

            @pl.when(lead)
            def _():
                await_bytes(parts.at[0 : count - 1, :, mine], r4.at[q])

            @pl.when(jnp.logical_not(lead))
            def _():
                await_bytes(parts.at[:, :, mine], r4.at[q])

            total = fin[:, cols(q)].astype(F32)
            for v in range(count):
                total += parts[v, :, mine].astype(F32)
            total = total.astype(BF16)
            outv[0:1, cols(q)] = total[0:1, :]
            outv[0:1, pl.ds(half + starts[q], widths[q])] = total[1:2, :]

    result = pltpu.make_async_copy(outv, out_ref, out_sem)
    result.start()

    with scope("drain"):
        await_bytes(t1.at[0 : ny - 1, :, main_part], s1)
        await_bytes(a1.at[0 : nx - 1], so.at[0])
        await_bytes(wgu.at[:, :, 1], ws_sem.at[0])
        await_bytes(wdn.at[:, 1], ws_sem.at[1])

        @pl.when(jnp.logical_not(lead))
        def _():
            await_bytes(tsend, s0)
            await_bytes(pnear, sp)
            await_bytes(ftok, fs.at[0])
            await_bytes(ft1.at[0 : ny - 1], fs.at[1])
            await_bytes(ft2.at[0 : nx - 1], fs.at[2])
            await_bytes(fxs.at[0 : nx - 1], fs.at[3])
            await_bytes(fys.at[0 : ny - 1], fs.at[4])
            await_bytes(fzs, fs.at[5])

        @pl.when(lead)
        def _():
            await_bytes(t2.at[0 : nx - 1, :, :, main_part], s2)
            await_bytes(b1.at[0 : ny - 1], so.at[1])
            await_bytes(c2.at[0 : ny - 1], so.at[2])
            await_bytes(e1.at[0 : 2 * (nx - 1)], so.at[3])
            await_bytes(e1.at[0], so.at[4])
            await_bytes(xbuf.at[0 : 2 * steps], sa)
            await_bytes(xbuf.at[0:near], sx)
            await_bytes(gbuf.at[0 : 2 * steps], gs.at[0])
            await_bytes(gbuf.at[0:near], gs.at[1])
            await_bytes(rsend, ss)
            await_bytes(yrecv.at[0 : nx - 1, :, :, main_cols], s3)
            await_bytes(fsend.at[0 : ny - 1, :, :, main_cols], s4)
            await_bytes(frecv.at[0, :, main_cols], s0)
            await_bytes(tsend, fs.at[0])

        result.wait()


def solution(mesh):
    nodes, locals_ = mesh.shape["node"], mesh.shape["local"]
    nx = min(NX, nodes)
    ny, nz = nodes // nx, locals_ // 2
    hz = nz // 2
    steps = hz - 1
    near = 2 * steps - 1

    def on_device(tokens, w_gate, w_up, w_down, expert_ids, gate_ints):
        model_width = tokens.shape[1]
        half = model_width // 2
        exp_node, ffl = w_gate.shape[0], w_gate.shape[1]
        units = 2 * exp_node * ffl
        rows = 2 * CAP
        lanes = half * sum(PARTS[-OTHER:]) // sum(PARTS)
        sem = pltpu.SemaphoreType.DMA
        one = sem(())
        any_space = pl.BlockSpec(memory_space=pl.ANY)
        vmem = pl.BlockSpec(memory_space=pltpu.VMEM)
        return pl.pallas_call(
            functools.partial(layer_kernel, nx, ny, nz),
            out_shape=jax.ShapeDtypeStruct((1, model_width), BF16),
            in_specs=[any_space] * 6,
            out_specs=any_space,
            scratch_shapes=[
                pltpu.VMEM((1, model_width), BF16),
                pltpu.SMEM(expert_ids.shape, jnp.int32),
                pltpu.SMEM(gate_ints.shape, jnp.int32),
                pltpu.VMEM((2, META + half), BF16),
                pltpu.VMEM((2 * ny, 2, META + half), BF16),
                pltpu.VMEM((nx, 2, 2 * ny, META + half), BF16),
                pltpu.VMEM((nz, 2, rows, half), BF16),
                pltpu.VMEM((2, 2, 2, exp_node, ffl, half), BF16),
                pltpu.VMEM((2, 2, exp_node, ffl, half), BF16),
                pltpu.VMEM((2, 2, near * 2 * rows, units), F32),
                pltpu.VMEM((2, near * 2 * rows, units), F32),
                pltpu.VMEM((near, 2, rows, half), BF16),
                pltpu.VMEM((2 * steps, 2, rows, half), BF16),
                pltpu.VMEM((2 * steps, 2, rows, half), BF16),
                pltpu.VMEM((nx, 2, 2 * ny, half), BF16),
                pltpu.VMEM((nx, 2, 2 * ny, half), BF16),
                pltpu.VMEM((ny, 2, 2, half), BF16),
                pltpu.VMEM((ny, 2, half), BF16),
                pltpu.VMEM((2, 2, META + half), BF16),
                pltpu.VMEM((ny, 2, 2, META + half), BF16),
                pltpu.VMEM((nx, 2, 2 * ny, META + half), BF16),
                pltpu.VMEM((nx, 2, 2 * ny, half), BF16),
                pltpu.VMEM((nx, 2, 2 * ny, half), BF16),
                pltpu.VMEM((ny, 2, 2, half), BF16),
                pltpu.VMEM((ny, 2, 2, half), BF16),
                pltpu.VMEM((2, 2, half), BF16),
                pltpu.VMEM((2, half), BF16),
                pltpu.VMEM((2 * nx, 2, lanes), BF16),
                pltpu.VMEM((ny, 2 * nx, 2, lanes), BF16),
                pltpu.VMEM((ny, 2 * nx, 2, lanes), BF16),
                pltpu.VMEM((ny, 2 * nx, 2, lanes), BF16),
                pltpu.VMEM((2 * nx, 2, lanes), BF16),
                pltpu.VMEM((nx, 2, lanes), BF16),
                pltpu.VMEM((nz, rows, META), BF16),
                sem((3,)), sem((2,)), sem((2,)), sem((2,)),
                one, one, sem((CHUNKS,)), one, sem((CHUNKS,)),
                one, sem((3, 2, CHUNKS)), one, sem((2,)), one, sem((steps,)),
                one, one, one, sem((CHUNKS,)),
                sem((6,)), sem((7,)), pltpu.SemaphoreType.REGULAR, sem((5,)),
                pltpu.VMEM((1, model_width), BF16), one,
                sem((2,)), sem((3, 2)), sem((2,)),
            ],
            compiler_params=pltpu.CompilerParams(
                collective_id=0, has_side_effects=True, vmem_limit_bytes=44 * 1024 * 1024
            ),
            name="layer",
        )(*(pltpu.with_memory_space_constraint(a, pltpu.HBM) for a in (tokens, w_gate, w_up, w_down, expert_ids, gate_ints)))

    both = P(("node", "local"), None)
    weights = P("node", "local", None)
    return jax.shard_map(
        on_device, mesh=mesh,
        in_specs=(both, weights, weights, weights, both, both),
        out_specs=both, check_vma=False,
    )
```
